256 devices in a mesh: seq: 32 (over y, x, core), tp: 8 (over z).
Axes of the slice: x: 4, y: 4, z: 8, core: 2. Of those that a mesh axis runs over, the one named last changes fastest.
Arguments:
- hidden_in: bfloat16 [2, 16384, 2560], P(None, 'seq'), may hold values from -6 to 6
- gate_proj: bfloat16 [2560, 5120], P(None, 'tp'), may hold values from -0.125 to 0.125
- value_proj: bfloat16 [2560, 5120], P(None, 'tp'), may hold values from -0.125 to 0.125
- bc_proj: bfloat16 [2560, 256], P(None, 'tp'), may hold values from -0.125 to 0.125
- step_proj: bfloat16 [2560, 80], P(None, 'tp'), may hold values from -0.125 to 0.125
- value_conv: float32 [4, 5120], P(None, 'tp'), may hold values from -3 to 3
- bc_conv: float32 [4, 256], replicated, may hold values from -3 to 3
- step_bias: float32 [80], P('tp'), may hold values from -1.5 to 0
- log_rate: float32 [80], P('tp'), as said below
- norm_gain: float32 [5120], P('tp'), may hold values from 0.25 to 1.75
Outputs:
- mixer_out: bfloat16 [2, 16384, 5120], P(None, 'seq', 'tp')
The draws below stay inside these ranges and needn't reach their ends.
Inputs may be any that keep to these rules, and one draw needn't show every extreme that they name: log_rate lies between -1.5 - ln(16384) and 1.0 - ln(16384).
All inputs are finite; a program needn't handle non-finite values.
Results may differ from the reference program's by a relative error of at most 0.0095.
Values may be sent and summed in bfloat16 or wider, within the bound.
A program may use at most 128 MiB of HBM per device.

```python
import math
import jax
import jax.numpy as jnp
from jax import lax

D = 2560
DI = 5120
HEADS = 80
HEAD_DIM = 64
STATE = 128
CONV = 4
BATCH = 2
BLOCK = 64
SEQ_LEN = 16384


def draw_log_rate(key, part):
    shift = math.log(SEQ_LEN)
    return jax.random.uniform(key, (HEADS,), jnp.float32, -1.5 - shift, 1.0 - shift)


def level_of(own_key, dims, cuts, smallest, top_value):
    def one(axis_at, blocks):
        draws = jax.random.uniform(jax.random.fold_in(jax.random.fold_in(own_key, 6), axis_at), (blocks,), jnp.float32, smallest / len(cuts), top_value / len(cuts))
        return jnp.repeat(jnp.exp(draws), dims[axis_at] // blocks).reshape((-1,) + (1,) * (len(dims) - axis_at - 1))

    level = one(*cuts[0])
    for cut in cuts[1:]:
        level = level * one(*cut)
    return level


def noise(rng, extent, deviation, reach, shards=(), kind=jnp.bfloat16):
    entries = deviation * jax.random.normal(rng, extent, jnp.float32)
    if shards:
        entries = entries * level_of(rng, extent, shards, -0.22, 0.18)
    return jnp.clip(entries, -reach, reach).astype(kind)


def setup_inputs(seed: int = 0) -> dict:
    streams_of = jax.random.split(jax.random.key(seed), 11)
    hidden_in = noise(streams_of[0], (BATCH, SEQ_LEN, D), 1.0, 6.0, ((1, 32),))
    gate_proj = noise(streams_of[1], (D, DI), D ** -0.5, 0.125, ((1, 8),))
    value_proj = noise(streams_of[2], (D, DI), D ** -0.5, 0.125, ((1, 8),))
    bc_proj = noise(streams_of[3], (D, 2 * STATE), D ** -0.5, 0.125, ((1, 8),))
    step_proj = noise(streams_of[4], (D, HEADS), D ** -0.5, 0.125, ((1, 8),))
    value_conv = noise(streams_of[5], (CONV, DI), CONV ** -0.5, 3.0, ((1, 8),), jnp.float32)
    bc_conv = noise(streams_of[6], (CONV, 2 * STATE), CONV ** -0.5, 3.0, (), jnp.float32)
    step_bias = jnp.clip(-1.5 + 1.5 * jax.random.uniform(streams_of[7], (HEADS,), jnp.float32) ** level_of(streams_of[7], (HEADS,), ((0, 8),), -0.2, 0.2), -1.5, 0.0)
    log_rate = draw_log_rate(jax.random.fold_in(streams_of[10], 71), 0)
    norm_gain = jnp.clip(1.0 + 0.15 * jax.random.normal(streams_of[9], (DI,), jnp.float32), 0.25, 1.75)
    return {"hidden_in": hidden_in, "gate_proj": gate_proj, "value_proj": value_proj, "bc_proj": bc_proj, "step_proj": step_proj, "value_conv": value_conv, "bc_conv": bc_conv, "step_bias": step_bias, "log_rate": log_rate, "norm_gain": norm_gain}


epsilon = 1e-05

def conv_silu(padded, kernel, length):
    running = jnp.zeros((padded.shape[0], length, padded.shape[2]), jnp.float32)
    for tap_index in range(kernel.shape[0]):
        running = running + kernel[tap_index] * padded[:, tap_index:tap_index + length, :]
    return jax.nn.silu(running)

def block_step(carried, inputs):
    values, log_decay, step_sizes, b_rows, c_rows = inputs
    length = log_decay.shape[1]
    cumulative = jnp.cumsum(log_decay, axis=1)
    log_gap = cumulative[:, :, None, :] - cumulative[:, None, :, :]
    causal = jnp.arange(length)[:, None] >= jnp.arange(length)[None, :]
    weights_in = jnp.exp(jnp.where(causal[None, :, :, None], log_gap, -jnp.inf))
    scores = jnp.einsum('bin,bjn->bij', c_rows, b_rows, precision=lax.Precision.HIGHEST)
    mixing = scores[:, :, :, None] * weights_in * step_sizes[:, None, :, :]
    within = jnp.einsum('bijh,bjhp->bihp', mixing, values, precision=lax.Precision.HIGHEST)
    earlier = jnp.einsum('bin,bhpn->bihp', c_rows, carried, precision=lax.Precision.HIGHEST)
    earlier = earlier * jnp.exp(cumulative)[..., None]
    remain = jnp.exp(cumulative[:, -1:, :] - cumulative) * step_sizes
    added_state = jnp.einsum('bjh,bjhp,bjn->bhpn', remain, values, b_rows, precision=lax.Precision.HIGHEST)
    updated = jnp.exp(cumulative[:, -1, :])[:, :, None, None] * carried + added_state
    return (updated, within + earlier)

def to_blocks(series, batch_size, blocks):
    return jnp.moveaxis(series.reshape((batch_size, blocks, BLOCK) + series.shape[2:]), 1, 0)

def reference(hidden_in, gate_proj, value_proj, bc_proj, step_proj, value_conv, bc_conv, step_bias, log_rate, norm_gain):
    flat_rows = hidden_in.reshape(-1, D)
    gate_pre = jnp.dot(flat_rows, gate_proj, preferred_element_type=jnp.float32).astype(jnp.bfloat16)
    value_pre = jnp.dot(flat_rows, value_proj, preferred_element_type=jnp.float32).astype(jnp.bfloat16)
    bc_pre = jnp.dot(flat_rows, bc_proj, preferred_element_type=jnp.float32).astype(jnp.bfloat16)
    step_pre = jnp.dot(flat_rows, step_proj, preferred_element_type=jnp.float32)
    value_pad = jnp.pad(value_pre.reshape(BATCH, SEQ_LEN, DI).astype(jnp.float32), ((0, 0), (CONV - 1, 0), (0, 0)))
    bc_pad = jnp.pad(bc_pre.reshape(BATCH, SEQ_LEN, 2 * STATE).astype(jnp.float32), ((0, 0), (CONV - 1, 0), (0, 0)))
    values = conv_silu(value_pad, value_conv, SEQ_LEN).reshape(BATCH, SEQ_LEN, HEADS, HEAD_DIM)
    bc_rows = conv_silu(bc_pad, bc_conv, SEQ_LEN)
    b_rows = bc_rows[..., :STATE]
    c_rows = bc_rows[..., STATE:]
    step_sizes = jax.nn.softplus(step_pre.reshape(BATCH, SEQ_LEN, HEADS) + step_bias)
    log_decay = -step_sizes * jnp.exp(log_rate)
    blocks = SEQ_LEN // BLOCK
    initial = jnp.zeros((BATCH, HEADS, HEAD_DIM, STATE), jnp.float32)
    final_state, outputs = lax.scan(block_step, initial, (to_blocks(values, BATCH, blocks), to_blocks(log_decay, BATCH, blocks), to_blocks(step_sizes, BATCH, blocks), to_blocks(b_rows, BATCH, blocks), to_blocks(c_rows, BATCH, blocks)))
    mixed_out = jnp.moveaxis(outputs, 0, 1).reshape(BATCH, SEQ_LEN, DI)
    gated_out = mixed_out * jax.nn.silu(gate_pre.reshape(BATCH, SEQ_LEN, DI).astype(jnp.float32))
    scale_sq = lax.optimization_barrier(jnp.sum(gated_out * gated_out, axis=-1, keepdims=True)) / DI
    return (gated_out * lax.rsqrt(scale_sq + epsilon) * norm_gain).astype(jnp.bfloat16)
```

```python
import jax
import jax.numpy as jnp
from jax import lax
from jax.experimental import pallas as pl
from jax.experimental.pallas import tpu as pltpu
from jax.sharding import PartitionSpec as P

DI = 5120
HEAD_DIM = 64
STATE = 128
CONV = 4
BLOCK = 128
LANES = 128
PAD = 16
HALO = 8
TILE = 256
MESH = pl.DeviceIdType.MESH

epsilon = 1e-05
F32 = jnp.float32
BF16 = jnp.bfloat16


def silu(x):
    return x * (1.0 / (1.0 + jnp.exp(-x)))


def halves(x):
    high = x.astype(BF16)
    low = (x - high.astype(F32)).astype(BF16)
    return jnp.concatenate([high, low], axis=1)


def dot_nt(a, b):
    return lax.dot_general(a, b, (((1,), (1,)), ((), ())), preferred_element_type=F32)


def mixer_kernel(
    hidden_ref, value_ref, gate_ref, small_ref, conv_ref, bc_conv_ref,
    bias_ref, rate_ref, expand_ref,
    gated_ref, scale_ref,
    rows, weights, small_pre, bc_wide, fin, fout, ends, logs, pair_logs, chip_logs,
    all_logs, early, late, pre, gates, scaled, right, other,
    local, pair, sent, got, prefix, owned, owned_pair, entering, sums, others,
    load_sem, halo_sem, log_sem, log_send, log_recv, early_send, early_recv,
    late_send, late_recv, pair_sem, out_send, out_recv, back_send, back_recv,
    swap_sem, sum_send, sum_recv,
):
    batch, length, _ = hidden_ref.shape
    width = value_ref.shape[1]
    blocks = length // BLOCK
    total_blocks = batch * blocks
    narrow = early.shape[1]
    late_len = late.shape[2] // batch
    early_len = early.shape[2] // batch
    me = lax.axis_index("tp")
    ring = lax.axis_size("tp")
    place = lax.axis_index("seq")
    devices = lax.axis_size("seq")
    chips = devices // 2
    core = lax.rem(place, 2)
    chip = place // 2
    partner = place + 1 - 2 * core
    after = lax.rem(place + 1, devices)
    before = lax.rem(place + devices - 1, devices)
    half = STATE // 2
    mine = pl.ds(pl.multiple_of(core * half, half), half)

    def chip_at(away):
        return lax.rem(chip + away, chips)

    def tp_at(away):
        return lax.rem(me + away, ring)

    def remote(source, target, send, recv, **device):
        return pltpu.make_async_remote_copy(
            src_ref=source, dst_ref=target, send_sem=send, recv_sem=recv,
            device_id=device, device_id_type=MESH,
        )

    chunk = length // 2
    loads = []
    for b in range(batch):
        for part in range(2):
            loads.append(pltpu.make_async_copy(
                hidden_ref.at[b, pl.ds(part * chunk, chunk)],
                rows.at[b, pl.ds(PAD + part * chunk, chunk)], load_sem.at[2 * b + part],
            ))
    gate_load = pltpu.make_async_copy(
        gate_ref, weights.at[:, pl.ds(width, width)], load_sem.at[2 * batch]
    )
    value_load = pltpu.make_async_copy(
        value_ref, weights.at[:, pl.ds(0, width)], load_sem.at[2 * batch + 1]
    )
    for load in loads:
        load.start()
    gate_load.start()
    value_load.start()

    barrier = pltpu.get_barrier_semaphore()
    for device in (after, before, partner):
        pl.semaphore_signal(barrier, inc=1, device_id={"seq": device}, device_id_type=MESH)
    for away in range(1, ring):
        pl.semaphore_signal(
            barrier, inc=1, device_id={"tp": tp_at(away)}, device_id_type=MESH
        )
    for away in range(1, chips):
        pl.semaphore_signal(
            barrier, inc=1, device_id={"seq": 2 * chip_at(away) + core}, device_id_type=MESH
        )

    for b in range(batch):
        rows[b, 0:HALO, :] = jnp.zeros((HALO, rows.shape[2]), BF16)
        small_pre[b, 0:LANES, :] = jnp.zeros((LANES, LANES), F32)
    for b in range(batch):
        for part in range(2):
            loads[2 * b + part].wait()
            at = slice(part * chunk, (part + 1) * chunk)
            small_pre[b, LANES + at.start : LANES + at.stop, :] = dot_nt(
                rows[b, PAD + at.start : PAD + at.stop, :], small_ref[...]
            )
    pl.semaphore_wait(barrier, 3 + (ring - 1) + (chips - 1))

    halo = remote(
        rows.at[:, pl.ds(PAD + length - HALO, HALO)], rows.at[:, pl.ds(PAD - HALO, HALO)],
        halo_sem.at[0], halo_sem.at[1], seq=after,
    )
    halo.start()

    taps = bc_conv_ref[pl.ds(pl.multiple_of(me * narrow, narrow), narrow), :]

    def bc_conv(x):
        total = taps[:, CONV - 1 : CONV] * x
        for k in range(1, CONV):
            total = total + taps[:, CONV - 1 - k : CONV - k] * pltpu.roll(x, k, 1)
        return silu(total).astype(BF16)

    def transpose_bc(b, piece):
        at = slice(piece * LANES, (piece + 1) * LANES)
        flipped = jnp.transpose(small_pre[b, at, :])[0:narrow, :]
        bc_wide[b, :, at] = flipped.astype(BF16).astype(F32)

    for b in range(batch):
        for piece in range(1, 1 + length // LANES):
            transpose_bc(b, piece)
        done = bc_conv(bc_wide[b, :, LANES : LANES + length])
        early[me, :, b * early_len : (b + 1) * early_len] = done[:, late_len:]

    def ring_copies(slots, send, recv, clockwise, step):
        index = step if clockwise else ring // 2 + step
        source = tp_at(ring - step) if clockwise else tp_at(step)
        target = tp_at(1) if clockwise else tp_at(ring - 1)
        return remote(
            slots.at[source], slots.at[source], send.at[index], recv.at[index], tp=target
        )

    early_steps = (ring // 2, ring - 1 - ring // 2)
    late_steps = (ring - 1 - ring // 2, ring // 2)

    def ring_start(slots, send, recv, steps, step):
        for clockwise in (True, False):
            if step < steps[0 if clockwise else 1]:
                ring_copies(slots, send, recv, clockwise, step).start()

    def ring_next(slots, send, recv, steps, step):
        for clockwise in (True, False):
            if step < steps[0 if clockwise else 1]:
                ring_copies(slots, send, recv, clockwise, step).wait_recv()
        ring_start(slots, send, recv, steps, step + 1)

    def ring_finish(slots, send, recv, steps):
        for clockwise in (True, False):
            for step in range(steps[0 if clockwise else 1]):
                ring_copies(slots, send, recv, clockwise, step).wait_send()

    early_ring = (early, early_send, early_recv, early_steps)
    late_ring = (late, late_send, late_recv, late_steps)
    ring_start(*early_ring, 0)

    row = lax.broadcasted_iota(jnp.int32, (BLOCK, BLOCK), 0)
    col = lax.broadcasted_iota(jnp.int32, (BLOCK, BLOCK), 1)
    triangle = jnp.where(row >= col, 1.0, 0.0).astype(F32)
    ms, mos, totals = [], [], []
    for b in range(batch):
        offset = jnp.zeros((1, LANES), F32)
        for k in range(blocks):
            step_pre = small_pre[b, LANES + k * BLOCK : LANES + (k + 1) * BLOCK, :] + bias_ref[...]
            steps = jnp.maximum(step_pre, 0.0) + jnp.log1p(jnp.exp(-jnp.abs(step_pre)))
            cumulative = jnp.dot(
                triangle, -steps * rate_ref[...],
                precision=lax.Precision.HIGHEST, preferred_element_type=F32,
            )
            last = cumulative[BLOCK - 1 : BLOCK, :]
            mid = 0.5 * last
            fin[b * blocks + k] = halves(jnp.exp(mid - cumulative) * steps)
            fout[b * blocks + k] = halves(jnp.exp(cumulative - mid))
            ms.append(mid)
            mos.append(mid + offset)
            offset = offset + last
        totals.append(offset)
    table = jnp.exp(jnp.concatenate(ms + mos, axis=0))
    ends[...] = jnp.dot(halves(table), expand_ref[...], preferred_element_type=F32)
    logs[...] = jnp.concatenate(totals + [jnp.zeros((8 - batch, LANES), F32)], axis=0)
    pair_log = remote(logs, pair_logs, log_sem.at[0], log_sem.at[1], seq=partner)
    pair_log.start()

    def log_copies(away):
        return remote(
            chip_logs, all_logs.at[chip], log_send.at[away - 1], log_recv.at[away - 1],
            seq=2 * chip_at(away) + core,
        )

    def gate_part(b, product):
        return silu(product.astype(BF16).astype(F32))

    def tile_of(index):
        cut = slice(index * TILE, (index + 1) * TILE)

        @pl.loop(0, batch)
        def _(b):
            if cut.start >= width:
                product = jnp.dot(
                    rows[b, PAD : PAD + length, :], weights[:, cut], preferred_element_type=F32
                )
                gates[b, :, cut.start - width : cut.stop - width] = gate_part(b, product)
            else:
                product = jnp.dot(rows[b], weights[:, cut], preferred_element_type=F32)
                inner = min(TILE, width - cut.start)
                pre[b, :, cut.start : cut.start + inner] = (
                    product[:, :inner].astype(BF16).astype(F32)
                )
                if inner < TILE:
                    gates[b, :, 0 : TILE - inner] = gate_part(b, product[PAD:, inner:])

    tiles = 2 * width // TILE
    value_tiles = -(-width // TILE)
    gate_load.wait()
    tile_of(tiles - 1)

    halo.wait()

    @pl.when(place == 0)
    def _():
        for b in range(batch):
            rows[b, 0:PAD, :] = jnp.zeros((PAD, rows.shape[2]), BF16)

    for b in range(batch):
        small_pre[b, LANES - PAD : LANES, :] = dot_nt(rows[b, 0:PAD, :], small_ref[...])
        transpose_bc(b, 0)
        done = bc_conv(bc_wide[b, :, 0 : LANES + late_len])
        late[me, :, b * late_len : (b + 1) * late_len] = done[:, LANES:]
    ring_start(*late_ring, 0)
    pair_log.wait()
    chip_logs[...] = logs[...] + pair_logs[...]
    all_logs[chip] = logs[...] + pair_logs[...]
    for away in range(1, chips):
        log_copies(away).start()

    for index in range(value_tiles, tiles - 1):
        tile_of(index)
    ring_next(*early_ring, 0)
    value_load.wait()
    tile_of(0)
    ring_next(*late_ring, 0)
    tile_of(1)
    ring_next(*early_ring, 1)
    ring_next(*late_ring, 1)
    for index in range(2, value_tiles):
        tile_of(index)
    ring_next(*early_ring, 2)
    ring_next(*late_ring, 2)

    for b in range(batch):
        for k in range(blocks):
            base = PAD + k * BLOCK - CONV + 1
            wide = jnp.dot(fin[b * blocks + k], expand_ref[...], preferred_element_type=F32)
            for start in range(0, width, LANES):
                cut = slice(start, start + LANES)
                x = conv_ref[0:1, cut] * pre[b, base : base + BLOCK, cut]
                for tap in range(1, CONV):
                    x = x + conv_ref[tap : tap + 1, cut] * pre[
                        b, base + tap : base + tap + BLOCK, cut
                    ]
                right[b * blocks + k, STATE:, cut] = (silu(x) * wide[:, cut]).astype(BF16)

    ring_next(*early_ring, 3)
    ring_next(*late_ring, 3)

    def bc_block(b, k, first):
        at = k * BLOCK
        if at < late_len:
            part = late[first : first + ring // 2, :, b * late_len + at : b * late_len + at + BLOCK]
        else:
            at += b * early_len - late_len
            part = early[first : first + ring // 2, :, at : at + BLOCK]
        return part.reshape(STATE, BLOCK)

    for b in range(batch):
        held = jnp.zeros((STATE, width), F32)
        for k in range(blocks):
            g = b * blocks + k
            e = ends[g : g + 1, :]
            ahead = e * held
            right[g, :STATE, :] = ahead.astype(BF16)
            added = jnp.dot(
                bc_block(b, k, 0), right[g, STATE:, :], preferred_element_type=F32
            )
            held = e * (ahead + added)
        local[b] = held.astype(BF16)

    pair_copy = remote(local, pair, pair_sem.at[0], pair_sem.at[1], seq=partner)
    pair_copy.start()
    for away in range(1, chips):
        log_copies(away).wait()
    own_end = jnp.exp(logs[...])
    pair_end = jnp.exp(pair_logs[...])
    wide_ends = jnp.dot(
        halves(jnp.concatenate([own_end, pair_end], axis=0)), expand_ref[...],
        preferred_element_type=F32,
    )
    low = chip < chips // batch
    spans = jnp.concatenate(
        [jnp.where(low, all_logs[i, 0:1, :], all_logs[i, 1:2, :]) for i in range(chips)], axis=0
    )
    spans = jnp.dot(halves(jnp.exp(spans)), expand_ref[...], preferred_element_type=F32)

    def out_copies(away):
        peer = chip_at(away)
        return remote(
            sent.at[peer], got.at[chip], out_send.at[away - 1], out_recv.at[away - 1],
            seq=2 * peer + core,
        )

    def back_copies(away):
        peer = chip_at(away)
        return remote(
            prefix.at[peer], owned.at[chip], back_send.at[away - 1], back_recv.at[away - 1],
            seq=2 * peer + core,
        )

    pair_copy.wait()
    groups = chips // batch
    for b in range(batch):
        own = local[b, mine, :].astype(F32)
        theirs = pair[b, mine, :].astype(F32)
        first = jnp.where(core == 0, own, theirs)
        second = jnp.where(core == 0, theirs, own)
        later = jnp.where(core == 0, wide_ends[8 + b : 9 + b, :], wide_ends[b : b + 1, :])
        both = (later * first + second).reshape(groups, half // groups, width)
        sent[b * groups : (b + 1) * groups] = both.astype(BF16)
    got[chip] = sent[chip]
    for away in range(1, chips):
        out_copies(away).start()

    def left_of(b, k):
        b_flat = bc_block(b, k, 0)
        c_rows = jnp.transpose(bc_block(b, k, ring // 2).astype(F32)).astype(BF16)
        return b_flat, c_rows

    for b in range(batch):
        for k in range(blocks):
            g = b * blocks + k
            at = slice(k * BLOCK, (k + 1) * BLOCK)
            b_flat, c_rows = left_of(b, k)
            scores = jnp.dot(c_rows, b_flat, preferred_element_type=F32)
            mixing = jnp.where(row >= col, scores, 0.0).astype(BF16)
            left = jnp.concatenate([c_rows, mixing], axis=1)
            scaled[g] = c_rows
            wide = jnp.dot(fout[g], expand_ref[...], preferred_element_type=F32)
            y = jnp.dot(left, right[g], preferred_element_type=F32)
            weighted = wide * gates[b, at, :]
            gated_ref[b, at, :] = y * weighted
            other[b, at, :] = weighted * ends[total_blocks + g : total_blocks + g + 1, :]

    for away in range(1, chips):
        out_copies(away).wait()
    running = jnp.zeros((half // groups, width), F32)
    for i in range(chips):
        prefix[i] = running.astype(BF16)
        if i + 1 < chips:
            running = spans[i : i + 1, :] * running + got[i].astype(F32)
    owned[chip] = prefix[chip]
    for away in range(1, chips):
        back_copies(away).start()
    ring_finish(*early_ring)
    ring_finish(*late_ring)
    for away in range(1, chips):
        back_copies(away).wait()
    swap = remote(owned, owned_pair, swap_sem.at[0], swap_sem.at[1], seq=partner)
    swap.start()
    swap.wait()

    for b in range(batch):
        at = slice(b * groups, (b + 1) * groups)
        own = owned[at].astype(F32).reshape(half, width)
        theirs = owned_pair[at].astype(F32).reshape(half, width)
        span = wide_ends[8 + b : 9 + b, :]
        for c in range(2):
            cut = slice(c * half, (c + 1) * half)
            full = jnp.where(core == c, own, theirs)
            moved = span * full + pair[b, cut, :].astype(F32)
            entering[b, cut, :] = jnp.where(core == 0, full, moved).astype(BF16)

    for b in range(batch):
        for k in range(blocks):
            g = b * blocks + k
            at = slice(k * BLOCK, (k + 1) * BLOCK)
            extra = jnp.dot(scaled[g], entering[b], preferred_element_type=F32)
            total = jnp.zeros((BLOCK, LANES), F32)
            for start in range(0, width, LANES):
                cut = slice(start, start + LANES)
                gated = gated_ref[b, at, cut] + other[b, at, cut] * extra[:, cut]
                gated_ref[b, at, cut] = gated
                total = total + gated * gated
            sums[g : g + 1, :] = jnp.sum(jnp.transpose(total), axis=0, keepdims=True)

    def sum_copies(away):
        return remote(
            sums, others.at[away - 1], sum_send.at[away - 1], sum_recv.at[away - 1],
            tp=tp_at(away),
        )

    for away in range(1, ring):
        sum_copies(away).start()
    for away in range(1, ring):
        sum_copies(away).wait()
    whole_sq = sums[...]
    for away in range(1, ring):
        whole_sq = whole_sq + others[away - 1]
    scale_ref[...] = lax.rsqrt(whole_sq / DI + epsilon)


def norm_kernel(gated_ref, scale_ref, gain_ref, out_ref):
    width = gated_ref.shape[2]
    step = pl.program_id(0)
    count = gated_ref.shape[1] // BLOCK
    for k in range(count):
        at = slice(k * BLOCK, (k + 1) * BLOCK)
        line = scale_ref[pl.ds(step * count + k, 1), :]
        column = jnp.transpose(jnp.broadcast_to(line, (BLOCK, LANES)))
        for start in range(0, width, LANES):
            cut = slice(start, start + LANES)
            out_ref[0, at, cut] = (
                gated_ref[0, at, cut] * column * gain_ref[:, cut]
            ).astype(BF16)


def per_device(
    hidden_in, gate_proj, value_proj, bc_proj, step_proj,
    value_conv, bc_conv, step_bias, log_rate, norm_gain,
):
    batch, length, model_width = hidden_in.shape
    heads = step_proj.shape[1]
    width = value_proj.shape[1]
    narrow = bc_proj.shape[1]
    blocks = length // BLOCK
    tp = lax.axis_size("tp")
    chips = lax.axis_size("seq") // 2
    total_blocks = batch * blocks
    half = STATE // 2
    groups = chips // batch
    late_len = BLOCK
    early_len = length - late_len

    tail = LANES - narrow - heads
    small = jnp.concatenate(
        [bc_proj.T, step_proj.T, jnp.zeros((tail, model_width), BF16)], axis=0
    )
    bias = jnp.pad(step_bias, (narrow, tail)).reshape(1, LANES)
    rate = jnp.pad(jnp.exp(log_rate), (narrow, tail)).reshape(1, LANES)
    lanes = lax.broadcasted_iota(jnp.int32, (2 * LANES, width), 1) // HEAD_DIM
    owner = lax.broadcasted_iota(jnp.int32, (2 * LANES, width), 0) % LANES - narrow
    expand = (lanes == owner).astype(BF16)

    hbm = pl.BlockSpec(memory_space=pltpu.HBM)
    vmem = pl.BlockSpec(memory_space=pltpu.VMEM)
    dma = pltpu.SemaphoreType.DMA
    gated, scale = pl.pallas_call(
        mixer_kernel,
        out_shape=(
            jax.ShapeDtypeStruct((batch, length, width), F32),
            jax.ShapeDtypeStruct((total_blocks, LANES), F32),
        ),
        in_specs=[hbm] * 3 + [vmem] * 6,
        out_specs=[vmem, vmem],
        scratch_shapes=[
            pltpu.VMEM((batch, PAD + length, model_width), BF16),
            pltpu.VMEM((model_width, 2 * width), BF16),
            pltpu.VMEM((batch, LANES + length, LANES), F32),
            pltpu.VMEM((batch, narrow, LANES + length), F32),
            pltpu.VMEM((total_blocks, BLOCK, 2 * LANES), BF16),
            pltpu.VMEM((total_blocks, BLOCK, 2 * LANES), BF16),
            pltpu.VMEM((2 * total_blocks, width), F32),
            pltpu.VMEM((8, LANES), F32),
            pltpu.VMEM((8, LANES), F32),
            pltpu.VMEM((8, LANES), F32),
            pltpu.VMEM((chips, 8, LANES), F32),
            pltpu.VMEM((tp, narrow, batch * early_len), BF16),
            pltpu.VMEM((tp, narrow, batch * late_len), BF16),
            pltpu.VMEM((batch, PAD + length, width), F32),
            pltpu.VMEM((batch, length, width), F32),
            pltpu.VMEM((total_blocks, BLOCK, STATE), BF16),
            pltpu.VMEM((total_blocks, STATE + BLOCK, width), BF16),
            pltpu.VMEM((batch, length, width), F32),
            pltpu.VMEM((batch, STATE, width), BF16),
            pltpu.VMEM((batch, STATE, width), BF16),
            pltpu.VMEM((chips, half // groups, width), BF16),
            pltpu.VMEM((chips, half // groups, width), BF16),
            pltpu.VMEM((chips, half // groups, width), BF16),
            pltpu.VMEM((chips, half // groups, width), BF16),
            pltpu.VMEM((chips, half // groups, width), BF16),
            pltpu.VMEM((batch, STATE, width), BF16),
            pltpu.VMEM((total_blocks, LANES), F32),
            pltpu.VMEM((tp - 1, total_blocks, LANES), F32),
            dma((2 * batch + 2,)),
            dma((2,)),
            dma((2,)),
            dma((chips - 1,)),
            dma((chips - 1,)),
            dma((tp,)),
            dma((tp,)),
            dma((tp,)),
            dma((tp,)),
            dma((2,)),
            dma((chips - 1,)),
            dma((chips - 1,)),
            dma((chips - 1,)),
            dma((chips - 1,)),
            dma((2,)),
            dma((tp - 1,)),
            dma((tp - 1,)),
        ],
        compiler_params=pltpu.CompilerParams(
            vmem_limit_bytes=48 << 20, collective_id=0, has_side_effects=True
        ),
        name="mixer",
    )(
        hidden_in, value_proj, gate_proj, small, value_conv, bc_conv.T, bias, rate, expand,
    )

    part = 2 * BLOCK
    steps = length // part
    return pl.pallas_call(
        norm_kernel,
        grid=(batch * steps,),
        out_shape=jax.ShapeDtypeStruct((batch, length, width), BF16),
        in_specs=[
            pl.BlockSpec((1, part, width), lambda s: (s // steps, s % steps, 0)),
            pl.BlockSpec((total_blocks, LANES), lambda s: (0, 0)),
            pl.BlockSpec((1, width), lambda s: (0, 0)),
        ],
        out_specs=pl.BlockSpec((1, part, width), lambda s: (s // steps, s % steps, 0)),
        compiler_params=pltpu.CompilerParams(vmem_limit_bytes=12 << 20),
        name="norm",
    )(gated, scale, norm_gain.reshape(1, width))


def solution(mesh):
    return jax.shard_map(
        per_device,
        mesh=mesh,
        in_specs=(
            P(None, "seq", None),
            P(None, "tp"),
            P(None, "tp"),
            P(None, "tp"),
            P(None, "tp"),
            P(None, "tp"),
            P(),
            P("tp"),
            P("tp"),
            P("tp"),
        ),
        out_specs=P(None, "seq", "tp"),
        check_vma=False,
    )
```

```python
import jax
import jax.numpy as jnp
from jax import lax
from jax.experimental import pallas as pl
from jax.experimental.pallas import tpu as pltpu
from jax.sharding import PartitionSpec as P

DI = 5120
HEAD_DIM = 64
STATE = 128
CONV = 4
BLOCK = 128
LANES = 128
PAD = 16
HALO = 8
TILE = 256
MESH = pl.DeviceIdType.MESH

epsilon = 1e-05
F32 = jnp.float32
BF16 = jnp.bfloat16


def silu(x):
    return x * (1.0 / (1.0 + jnp.exp(-x)))


def halves(x):
    high = x.astype(BF16)
    low = (x - high.astype(F32)).astype(BF16)
    return jnp.concatenate([high, low], axis=1)


def dot_nt(a, b):
    return lax.dot_general(a, b, (((1,), (1,)), ((), ())), preferred_element_type=F32)


def mixer_kernel(
    hidden_ref, value_ref, gate_ref, bc_in, step_in, conv_in, bc_conv_in,
    bias_in, rate_in, gain_in,
    gated_ref, scale_ref,
    small_ref, step_cols, conv_ref, bc_taps, bc_square, bc_conv_ref,
    bias_small, rate_small, bias_ref, rate_ref, gain_ref, expand_ref, rows, weights, small_pre, bc_wide, fin, fout, ends, logs, pair_logs, chip_logs,
    all_logs, early, late, pre, gates, scaled, right, other,
    local, pair, sent, got, prefix, owned, owned_pair, entering, sums, others,
    load_sem, small_sem, halo_sem, log_sem, log_send, log_recv, early_send, early_recv,
    late_send, late_recv, pair_sem, out_send, out_recv, back_send, back_recv,
    swap_sem, sum_send, sum_recv,
):
    batch, length, _ = hidden_ref.shape
    width = value_ref.shape[1]
    blocks = length // BLOCK
    total_blocks = batch * blocks
    narrow = early.shape[1]
    late_len = late.shape[2] // batch
    early_len = early.shape[2] // batch
    me = lax.axis_index("tp")
    ring = lax.axis_size("tp")
    place = lax.axis_index("seq")
    devices = lax.axis_size("seq")
    chips = devices // 2
    core = lax.rem(place, 2)
    chip = place // 2
    partner = place + 1 - 2 * core
    after = lax.rem(place + 1, devices)
    before = lax.rem(place + devices - 1, devices)
    half = STATE // 2
    mine = pl.ds(pl.multiple_of(core * half, half), half)

    def chip_at(away):
        return lax.rem(chip + away, chips)

    def tp_at(away):
        return lax.rem(me + away, ring)

    def remote(source, target, send, recv, **device):
        return pltpu.make_async_remote_copy(
            src_ref=source, dst_ref=target, send_sem=send, recv_sem=recv,
            device_id=device, device_id_type=MESH,
        )

    little = [
        pltpu.make_async_copy(source, target, small_sem.at[i])
        for i, (source, target) in enumerate((
            (bc_in, small_ref.at[pl.ds(narrow, narrow)]), (step_in, step_cols),
            (bc_conv_in, bc_taps), (bias_in, bias_small), (rate_in, rate_small),
            (conv_in, conv_ref), (gain_in, gain_ref),
        ))
    ]
    for load in little:
        load.start()
    chunk = length // 2
    loads = []
    for b in range(batch):
        for part in range(2):
            loads.append(pltpu.make_async_copy(
                hidden_ref.at[b, pl.ds(part * chunk, chunk)],
                rows.at[b, pl.ds(PAD + part * chunk, chunk)], load_sem.at[2 * b + part],
            ))
    gate_load = pltpu.make_async_copy(
        gate_ref, weights.at[:, pl.ds(width, width)], load_sem.at[2 * batch]
    )
    value_load = pltpu.make_async_copy(
        value_ref, weights.at[:, pl.ds(0, width)], load_sem.at[2 * batch + 1]
    )
    for load in loads:
        load.start()
    gate_load.start()
    value_load.start()

    barrier = pltpu.get_barrier_semaphore()
    for device in (after, before, partner):
        pl.semaphore_signal(barrier, inc=1, device_id={"seq": device}, device_id_type=MESH)
    for away in range(1, ring):
        pl.semaphore_signal(
            barrier, inc=1, device_id={"tp": tp_at(away)}, device_id_type=MESH
        )
    for away in range(1, chips):
        pl.semaphore_signal(
            barrier, inc=1, device_id={"seq": 2 * chip_at(away) + core}, device_id_type=MESH
        )

    for b in range(batch):
        rows[b, 0:HALO, :] = jnp.zeros((HALO, rows.shape[2]), BF16)
        small_pre[b, 0:LANES, :] = jnp.zeros((LANES, LANES), F32)
    heads = step_cols.shape[0]
    small_ref[0:narrow, :] = jnp.zeros((narrow, small_ref.shape[1]), BF16)
    small_ref[2 * narrow :, :] = jnp.zeros((LANES - 2 * narrow, small_ref.shape[1]), BF16)
    bias_ref[...] = jnp.zeros_like(bias_ref)
    rate_ref[...] = jnp.zeros_like(rate_ref)
    bc_square[...] = jnp.zeros_like(bc_square)
    lane = lax.broadcasted_iota(jnp.int32, expand_ref.shape, 1) // HEAD_DIM
    owner = lax.rem(lax.broadcasted_iota(jnp.int32, expand_ref.shape, 0), LANES)
    expand_ref[...] = jnp.where(lane == owner, 1.0, 0.0).astype(BF16)
    for load in little:
        load.wait()
    small_ref[0:heads, :] = step_cols[...]
    bias_ref[:, 0:heads] = bias_small[...]
    rate_ref[:, 0:heads] = jnp.exp(rate_small[...])
    for part in range(2):
        cut = slice(part * LANES, (part + 1) * LANES)
        bc_square[0:CONV, :] = bc_taps[:, cut]
        bc_conv_ref[cut, :] = jnp.transpose(bc_square[...])
    for b in range(batch):
        for part in range(2):
            loads[2 * b + part].wait()
            at = slice(part * chunk, (part + 1) * chunk)
            small_pre[b, LANES + at.start : LANES + at.stop, :] = dot_nt(
                rows[b, PAD + at.start : PAD + at.stop, :], small_ref[...]
            )
    pl.semaphore_wait(barrier, 3 + (ring - 1) + (chips - 1))

    halo = remote(
        rows.at[:, pl.ds(PAD + length - HALO, HALO)], rows.at[:, pl.ds(PAD - HALO, HALO)],
        halo_sem.at[0], halo_sem.at[1], seq=after,
    )
    halo.start()

    taps = bc_conv_ref[pl.ds(pl.multiple_of(me * narrow, narrow), narrow), :]

    def bc_conv(x):
        total = taps[:, CONV - 1 : CONV] * x
        for k in range(1, CONV):
            total = total + taps[:, CONV - 1 - k : CONV - k] * pltpu.roll(x, k, 1)
        return silu(total).astype(BF16)

    def transpose_bc(b, piece):
        at = slice(piece * LANES, (piece + 1) * LANES)
        flipped = jnp.transpose(small_pre[b, at, :])[narrow : 2 * narrow, :]
        bc_wide[b, :, at] = flipped.astype(BF16).astype(F32)

    for b in range(batch):
        for piece in range(1, 1 + length // LANES):
            transpose_bc(b, piece)
        done = bc_conv(bc_wide[b, :, LANES : LANES + length])
        early[me, :, b * early_len : (b + 1) * early_len] = done[:, late_len:]

    def ring_copies(slots, send, recv, clockwise, step):
        index = step if clockwise else ring // 2 + step
        source = tp_at(ring - step) if clockwise else tp_at(step)
        target = tp_at(1) if clockwise else tp_at(ring - 1)
        return remote(
            slots.at[source], slots.at[source], send.at[index], recv.at[index], tp=target
        )

    early_steps = (ring // 2, ring - 1 - ring // 2)
    late_steps = (ring - 1 - ring // 2, ring // 2)

    def ring_start(slots, send, recv, steps, step):
        for clockwise in (True, False):
            if step < steps[0 if clockwise else 1]:
                ring_copies(slots, send, recv, clockwise, step).start()

    def ring_next(slots, send, recv, steps, step):
        for clockwise in (True, False):
            if step < steps[0 if clockwise else 1]:
                ring_copies(slots, send, recv, clockwise, step).wait_recv()
        ring_start(slots, send, recv, steps, step + 1)

    def ring_finish(slots, send, recv, steps):
        for clockwise in (True, False):
            for step in range(steps[0 if clockwise else 1]):
                ring_copies(slots, send, recv, clockwise, step).wait_send()

    early_ring = (early, early_send, early_recv, early_steps)
    late_ring = (late, late_send, late_recv, late_steps)
    ring_start(*early_ring, 0)

    row = lax.broadcasted_iota(jnp.int32, (BLOCK, BLOCK), 0)
    col = lax.broadcasted_iota(jnp.int32, (BLOCK, BLOCK), 1)
    triangle = jnp.where(row >= col, 1.0, 0.0).astype(F32)
    ms, mos, totals = [], [], []
    for b in range(batch):
        offset = jnp.zeros((1, LANES), F32)
        for k in range(blocks):
            step_pre = small_pre[b, LANES + k * BLOCK : LANES + (k + 1) * BLOCK, :] + bias_ref[...]
            steps = jnp.maximum(step_pre, 0.0) + jnp.log1p(jnp.exp(-jnp.abs(step_pre)))
            cumulative = jnp.dot(
                triangle, -steps * rate_ref[...],
                precision=lax.Precision.HIGHEST, preferred_element_type=F32,
            )
            last = cumulative[BLOCK - 1 : BLOCK, :]
            mid = 0.5 * last
            fin[b * blocks + k] = halves(jnp.exp(mid - cumulative) * steps)
            fout[b * blocks + k] = halves(jnp.exp(cumulative - mid))
            ms.append(mid)
            mos.append(mid + offset)
            offset = offset + last
        totals.append(offset)
    table = jnp.exp(jnp.concatenate(ms + mos, axis=0))
    ends[...] = jnp.dot(halves(table), expand_ref[...], preferred_element_type=F32)
    logs[...] = jnp.concatenate(totals + [jnp.zeros((8 - batch, LANES), F32)], axis=0)
    pair_log = remote(logs, pair_logs, log_sem.at[0], log_sem.at[1], seq=partner)
    pair_log.start()

    def log_copies(away):
        return remote(
            chip_logs, all_logs.at[chip], log_send.at[away - 1], log_recv.at[away - 1],
            seq=2 * chip_at(away) + core,
        )

    def gate_part(b, product):
        return silu(product.astype(BF16).astype(F32))

    def tile_of(index):
        cut = slice(index * TILE, (index + 1) * TILE)

        @pl.loop(0, batch)
        def _(b):
            if cut.start >= width:
                product = jnp.dot(
                    rows[b, PAD : PAD + length, :], weights[:, cut], preferred_element_type=F32
                )
                gates[b, :, cut.start - width : cut.stop - width] = gate_part(b, product)
            else:
                product = jnp.dot(rows[b], weights[:, cut], preferred_element_type=F32)
                inner = min(TILE, width - cut.start)
                pre[b, :, cut.start : cut.start + inner] = (
                    product[:, :inner].astype(BF16).astype(F32)
                )
                if inner < TILE:
                    gates[b, :, 0 : TILE - inner] = gate_part(b, product[PAD:, inner:])

    tiles = 2 * width // TILE
    value_tiles = -(-width // TILE)
    gate_load.wait()
    tile_of(tiles - 1)

    halo.wait()

    @pl.when(place == 0)
    def _():
        for b in range(batch):
            rows[b, 0:PAD, :] = jnp.zeros((PAD, rows.shape[2]), BF16)

    for b in range(batch):
        small_pre[b, LANES - PAD : LANES, :] = dot_nt(rows[b, 0:PAD, :], small_ref[...])
        transpose_bc(b, 0)
        done = bc_conv(bc_wide[b, :, 0 : LANES + late_len])
        late[me, :, b * late_len : (b + 1) * late_len] = done[:, LANES:]
    ring_start(*late_ring, 0)
    pair_log.wait()
    chip_logs[...] = logs[...] + pair_logs[...]
    all_logs[chip] = logs[...] + pair_logs[...]
    for away in range(1, chips):
        log_copies(away).start()

    for index in range(value_tiles, tiles - 1):
        tile_of(index)
    ring_next(*early_ring, 0)
    value_load.wait()
    tile_of(0)
    ring_next(*late_ring, 0)
    tile_of(1)
    ring_next(*early_ring, 1)
    ring_next(*late_ring, 1)
    for index in range(2, value_tiles):
        tile_of(index)
    ring_next(*early_ring, 2)
    ring_next(*late_ring, 2)

    for b in range(batch):
        for k in range(blocks):
            base = PAD + k * BLOCK - CONV + 1
            wide = jnp.dot(fin[b * blocks + k], expand_ref[...], preferred_element_type=F32)
            for start in range(0, width, LANES):
                cut = slice(start, start + LANES)
                x = conv_ref[0:1, cut] * pre[b, base : base + BLOCK, cut]
                for tap in range(1, CONV):
                    x = x + conv_ref[tap : tap + 1, cut] * pre[
                        b, base + tap : base + tap + BLOCK, cut
                    ]
                right[b * blocks + k, STATE:, cut] = (silu(x) * wide[:, cut]).astype(BF16)

    ring_next(*early_ring, 3)
    ring_next(*late_ring, 3)

    def bc_block(b, k, first):
        at = k * BLOCK
        if at < late_len:
            part = late[first : first + ring // 2, :, b * late_len + at : b * late_len + at + BLOCK]
        else:
            at += b * early_len - late_len
            part = early[first : first + ring // 2, :, at : at + BLOCK]
        return part.reshape(STATE, BLOCK)

    for b in range(batch):
        held = jnp.zeros((STATE, width), F32)
        for k in range(blocks):
            g = b * blocks + k
            e = ends[g : g + 1, :]
            ahead = e * held
            right[g, :STATE, :] = ahead.astype(BF16)
            added = jnp.dot(
                bc_block(b, k, 0), right[g, STATE:, :], preferred_element_type=F32
            )
            held = e * (ahead + added)
        local[b] = held.astype(BF16)

    pair_copy = remote(local, pair, pair_sem.at[0], pair_sem.at[1], seq=partner)
    pair_copy.start()
    for away in range(1, chips):
        log_copies(away).wait()
    own_end = jnp.exp(logs[...])
    pair_end = jnp.exp(pair_logs[...])
    wide_ends = jnp.dot(
        halves(jnp.concatenate([own_end, pair_end], axis=0)), expand_ref[...],
        preferred_element_type=F32,
    )
    low = chip < chips // batch
    spans = jnp.concatenate(
        [jnp.where(low, all_logs[i, 0:1, :], all_logs[i, 1:2, :]) for i in range(chips)], axis=0
    )
    spans = jnp.dot(halves(jnp.exp(spans)), expand_ref[...], preferred_element_type=F32)

    def out_copies(away):
        peer = chip_at(away)
        return remote(
            sent.at[peer], got.at[chip], out_send.at[away - 1], out_recv.at[away - 1],
            seq=2 * peer + core,
        )

    def back_copies(away):
        peer = chip_at(away)
        return remote(
            prefix.at[peer], owned.at[chip], back_send.at[away - 1], back_recv.at[away - 1],
            seq=2 * peer + core,
        )

    pair_copy.wait()
    groups = chips // batch
    for b in range(batch):
        own = local[b, mine, :].astype(F32)
        theirs = pair[b, mine, :].astype(F32)
        first = jnp.where(core == 0, own, theirs)
        second = jnp.where(core == 0, theirs, own)
        later = jnp.where(core == 0, wide_ends[8 + b : 9 + b, :], wide_ends[b : b + 1, :])
        both = (later * first + second).reshape(groups, half // groups, width)
        sent[b * groups : (b + 1) * groups] = both.astype(BF16)
    got[chip] = sent[chip]
    for away in range(1, chips):
        out_copies(away).start()

    def left_of(b, k):
        b_flat = bc_block(b, k, 0)
        c_rows = jnp.transpose(bc_block(b, k, ring // 2).astype(F32)).astype(BF16)
        return b_flat, c_rows

    for b in range(batch):
        for k in range(blocks):
            g = b * blocks + k
            at = slice(k * BLOCK, (k + 1) * BLOCK)
            b_flat, c_rows = left_of(b, k)
            scores = jnp.dot(c_rows, b_flat, preferred_element_type=F32)
            mixing = jnp.where(row >= col, scores, 0.0).astype(BF16)
            left = jnp.concatenate([c_rows, mixing], axis=1)
            scaled[g] = c_rows
            wide = jnp.dot(fout[g], expand_ref[...], preferred_element_type=F32)
            y = jnp.dot(left, right[g], preferred_element_type=F32)
            weighted = wide * gates[b, at, :]
            gated_ref[b, at, :] = y * weighted
            other[b, at, :] = weighted * ends[total_blocks + g : total_blocks + g + 1, :]

    for away in range(1, chips):
        out_copies(away).wait()
    running = jnp.zeros((half // groups, width), F32)
    for i in range(chips):
        prefix[i] = running.astype(BF16)
        if i + 1 < chips:
            running = spans[i : i + 1, :] * running + got[i].astype(F32)
    owned[chip] = prefix[chip]
    for away in range(1, chips):
        back_copies(away).start()
    ring_finish(*early_ring)
    ring_finish(*late_ring)
    for away in range(1, chips):
        back_copies(away).wait()
    swap = remote(owned, owned_pair, swap_sem.at[0], swap_sem.at[1], seq=partner)
    swap.start()
    swap.wait()

    for b in range(batch):
        at = slice(b * groups, (b + 1) * groups)
        own = owned[at].astype(F32).reshape(half, width)
        theirs = owned_pair[at].astype(F32).reshape(half, width)
        span = wide_ends[8 + b : 9 + b, :]
        for c in range(2):
            cut = slice(c * half, (c + 1) * half)
            full = jnp.where(core == c, own, theirs)
            moved = span * full + pair[b, cut, :].astype(F32)
            entering[b, cut, :] = jnp.where(core == 0, full, moved).astype(BF16)

    for b in range(batch):
        for k in range(blocks):
            g = b * blocks + k
            at = slice(k * BLOCK, (k + 1) * BLOCK)
            extra = jnp.dot(scaled[g], entering[b], preferred_element_type=F32)
            total = jnp.zeros((BLOCK, LANES), F32)
            for start in range(0, width, LANES):
                cut = slice(start, start + LANES)
                gated = gated_ref[b, at, cut] + other[b, at, cut] * extra[:, cut]
                gated_ref[b, at, cut] = gated * gain_ref[start // LANES : start // LANES + 1, :]
                total = total + gated * gated
            sums[g : g + 1, :] = jnp.sum(jnp.transpose(total), axis=0, keepdims=True)

    def sum_copies(away):
        return remote(
            sums, others.at[away - 1], sum_send.at[away - 1], sum_recv.at[away - 1],
            tp=tp_at(away),
        )

    for away in range(1, ring):
        sum_copies(away).start()
    for away in range(1, ring):
        sum_copies(away).wait()
    whole_sq = sums[...]
    for away in range(1, ring):
        whole_sq = whole_sq + others[away - 1]
    scale_ref[...] = lax.rsqrt(whole_sq / DI + epsilon)


def norm_kernel(gated_ref, scale_ref, out_ref):
    width = gated_ref.shape[2]
    step = pl.program_id(0)
    count = gated_ref.shape[1] // BLOCK
    for k in range(count):
        at = slice(k * BLOCK, (k + 1) * BLOCK)
        line = scale_ref[pl.ds(step * count + k, 1), :]
        column = jnp.transpose(jnp.broadcast_to(line, (BLOCK, LANES)))
        for start in range(0, width, LANES):
            cut = slice(start, start + LANES)
            out_ref[0, at, cut] = (gated_ref[0, at, cut] * column).astype(BF16)


def per_device(
    hidden_in, gate_proj, value_proj, bc_proj, step_proj,
    value_conv, bc_conv, step_bias, log_rate, norm_gain,
):
    batch, length, model_width = hidden_in.shape
    heads = step_proj.shape[1]
    width = value_proj.shape[1]
    narrow = bc_proj.shape[1]
    blocks = length // BLOCK
    tp = lax.axis_size("tp")
    chips = lax.axis_size("seq") // 2
    total_blocks = batch * blocks
    half = STATE // 2
    groups = chips // batch
    late_len = BLOCK
    early_len = length - late_len

    hbm = pl.BlockSpec(memory_space=pltpu.HBM)
    vmem = pl.BlockSpec(memory_space=pltpu.VMEM)
    dma = pltpu.SemaphoreType.DMA
    gated, scale = pl.pallas_call(
        mixer_kernel,
        out_shape=(
            jax.ShapeDtypeStruct((batch, length, width), F32),
            jax.ShapeDtypeStruct((total_blocks, LANES), F32),
        ),
        in_specs=[hbm] * 10,
        out_specs=[vmem, vmem],
        scratch_shapes=[
            pltpu.VMEM((LANES, model_width), BF16),
            pltpu.VMEM((heads, model_width), BF16),
            pltpu.VMEM((CONV, width), F32),
            pltpu.VMEM((CONV, 2 * STATE), F32),
            pltpu.VMEM((LANES, LANES), F32),
            pltpu.VMEM((2 * STATE, LANES), F32),
            pltpu.VMEM((1, heads), F32),
            pltpu.VMEM((1, heads), F32),
            pltpu.VMEM((1, LANES), F32),
            pltpu.VMEM((1, LANES), F32),
            pltpu.VMEM((width // LANES, LANES), F32),
            pltpu.VMEM((2 * LANES, width), BF16),
            pltpu.VMEM((batch, PAD + length, model_width), BF16),
            pltpu.VMEM((model_width, 2 * width), BF16),
            pltpu.VMEM((batch, LANES + length, LANES), F32),
            pltpu.VMEM((batch, narrow, LANES + length), F32),
            pltpu.VMEM((total_blocks, BLOCK, 2 * LANES), BF16),
            pltpu.VMEM((total_blocks, BLOCK, 2 * LANES), BF16),
            pltpu.VMEM((2 * total_blocks, width), F32),
            pltpu.VMEM((8, LANES), F32),
            pltpu.VMEM((8, LANES), F32),
            pltpu.VMEM((8, LANES), F32),
            pltpu.VMEM((chips, 8, LANES), F32),
            pltpu.VMEM((tp, narrow, batch * early_len), BF16),
            pltpu.VMEM((tp, narrow, batch * late_len), BF16),
            pltpu.VMEM((batch, PAD + length, width), F32),
            pltpu.VMEM((batch, length, width), F32),
            pltpu.VMEM((total_blocks, BLOCK, STATE), BF16),
            pltpu.VMEM((total_blocks, STATE + BLOCK, width), BF16),
            pltpu.VMEM((batch, length, width), F32),
            pltpu.VMEM((batch, STATE, width), BF16),
            pltpu.VMEM((batch, STATE, width), BF16),
            pltpu.VMEM((chips, half // groups, width), BF16),
            pltpu.VMEM((chips, half // groups, width), BF16),
            pltpu.VMEM((chips, half // groups, width), BF16),
            pltpu.VMEM((chips, half // groups, width), BF16),
            pltpu.VMEM((chips, half // groups, width), BF16),
            pltpu.VMEM((batch, STATE, width), BF16),
            pltpu.VMEM((total_blocks, LANES), F32),
            pltpu.VMEM((tp - 1, total_blocks, LANES), F32),
            dma((2 * batch + 2,)),
            dma((7,)),
            dma((2,)),
            dma((2,)),
            dma((chips - 1,)),
            dma((chips - 1,)),
            dma((tp,)),
            dma((tp,)),
            dma((tp,)),
            dma((tp,)),
            dma((2,)),
            dma((chips - 1,)),
            dma((chips - 1,)),
            dma((chips - 1,)),
            dma((chips - 1,)),
            dma((2,)),
            dma((tp - 1,)),
            dma((tp - 1,)),
        ],
        compiler_params=pltpu.CompilerParams(
            vmem_limit_bytes=48 << 20, collective_id=0, has_side_effects=True
        ),
        name="mixer",
    )(*(pltpu.with_memory_space_constraint(x, pltpu.HBM) for x in (
        hidden_in, value_proj, gate_proj, bc_proj.T, step_proj.T, value_conv, bc_conv,
        step_bias.reshape(1, heads), log_rate.reshape(1, heads),
        norm_gain.reshape(width // LANES, LANES),
    )))

    part = 2 * BLOCK
    steps = length // part
    return pl.pallas_call(
        norm_kernel,
        grid=(batch * steps,),
        out_shape=jax.ShapeDtypeStruct((batch, length, width), BF16),
        in_specs=[
            pl.BlockSpec((1, part, width), lambda s: (s // steps, s % steps, 0)),
            pl.BlockSpec((total_blocks, LANES), lambda s: (0, 0)),
        ],
        out_specs=pl.BlockSpec((1, part, width), lambda s: (s // steps, s % steps, 0)),
        compiler_params=pltpu.CompilerParams(vmem_limit_bytes=12 << 20),
        name="norm",
    )(gated, scale)


def solution(mesh):
    return jax.shard_map(
        per_device,
        mesh=mesh,
        in_specs=(
            P(None, "seq", None),
            P(None, "tp"),
            P(None, "tp"),
            P(None, "tp"),
            P(None, "tp"),
            P(None, "tp"),
            P(),
            P("tp"),
            P("tp"),
            P("tp"),
        ),
        out_specs=P(None, "seq", "tp"),
        check_vma=False,
    )
```

```python
import jax
import jax.numpy as jnp
from jax import lax
from jax.experimental import pallas as pl
from jax.experimental.pallas import tpu as pltpu
from jax.sharding import PartitionSpec as P

DI = 5120
HEAD_DIM = 64
STATE = 128
CONV = 4
BLOCK = 128
LANES = 128
PAD = 16
HALO = 8
TILE = 256
SIDE = 4
MESH = pl.DeviceIdType.MESH

epsilon = 1e-05
F32 = jnp.float32
BF16 = jnp.bfloat16


def silu(x):
    return x * (1.0 / (1.0 + jnp.exp(-x)))


def halves(x):
    high = x.astype(BF16)
    low = (x - high.astype(F32)).astype(BF16)
    return jnp.concatenate([high, low], axis=1)


def dot_nt(a, b):
    return lax.dot_general(a, b, (((1,), (1,)), ((), ())), preferred_element_type=F32)


def mixer_kernel(
    hidden_ref, value_ref, gate_ref, bc_in, step_in, conv_in, bc_conv_in,
    bias_in, rate_in, gain_in,
    gated_ref, scale_ref,
    small_ref, step_cols, conv_ref, bc_taps, bc_square, bc_conv_ref,
    bias_small, rate_small, bias_ref, rate_ref, gain_ref, expand_ref, rows, weights, small_pre, bc_wide, fin, fout, ends, logs, pair_logs, chip_logs,
    all_logs, far, near, first_slots, pre, gates, left, right, other,
    local, pair, sent, got, prefix, owned, owned_pair, entering, sums, others,
    load_sem, small_sem, halo_sem, log_sem, log_send, log_recv, ring_send,
    far_recv, near_recv, first_recv, pair_sem, out_send, out_recv, back_send, back_recv,
    swap_sem, sum_send, sum_recv,
):
    batch, length, _ = hidden_ref.shape
    width = value_ref.shape[1]
    blocks = length // BLOCK
    total_blocks = batch * blocks
    narrow = bc_in.shape[0]
    me = lax.axis_index("tp")
    ring = lax.axis_size("tp")
    place = lax.axis_index("seq")
    devices = lax.axis_size("seq")
    chips = devices // 2
    core = lax.rem(place, 2)
    chip = place // 2
    partner = place + 1 - 2 * core
    after = lax.rem(place + 1, devices)
    before = lax.rem(place + devices - 1, devices)
    half = STATE // 2
    mine = pl.ds(pl.multiple_of(core * half, half), half)

    across = SIDE
    along = chips // SIDE

    def chip_at(move):
        dy, dx = move
        return (
            lax.rem(chip // across + dy, along) * across
            + lax.rem(lax.rem(chip, across) + dx, across)
        )

    def hops(away, count):
        return min(away, count - away)

    moves = sorted(
        [(dy, dx) for dy in range(along) for dx in range(across) if dy or dx],
        key=lambda move: -(hops(move[0], along) + hops(move[1], across)),
    )
    turns = sorted(range(1, lax.axis_size("tp")), key=lambda away: -hops(away, lax.axis_size("tp")))

    def wait_bytes(ref, count, semaphore):
        part = ref.at[pl.ds(0, count)]
        pltpu.make_async_copy(part, part, semaphore).wait()

    def tp_at(away):
        return lax.rem(me + away, ring)

    def remote(source, target, send, recv, **device):
        return pltpu.make_async_remote_copy(
            src_ref=source, dst_ref=target, send_sem=send, recv_sem=recv,
            device_id=device, device_id_type=MESH,
        )

    little = [
        pltpu.make_async_copy(source, target, small_sem.at[i])
        for i, (source, target) in enumerate((
            (bc_in, small_ref.at[pl.ds(narrow, narrow)]), (step_in, step_cols),
            (bc_conv_in, bc_taps), (bias_in, bias_small), (rate_in, rate_small),
            (conv_in, conv_ref), (gain_in, gain_ref),
        ))
    ]
    for load in little:
        load.start()
    chunk = length // 2
    loads = []
    for b in range(batch):
        for part in range(2):
            loads.append(pltpu.make_async_copy(
                hidden_ref.at[b, pl.ds(part * chunk, chunk)],
                rows.at[b, pl.ds(PAD + part * chunk, chunk)], load_sem.at[2 * b + part],
            ))
    gate_load = pltpu.make_async_copy(
        gate_ref, weights.at[:, pl.ds(width, width)], load_sem.at[2 * batch]
    )
    value_load = pltpu.make_async_copy(
        value_ref, weights.at[:, pl.ds(0, width)], load_sem.at[2 * batch + 1]
    )
    order = [2 * b + part for part in (1, 0) for b in range(batch)]
    for i in order:
        loads[i].start()

    barrier = pltpu.get_barrier_semaphore()
    for device in (after, before, partner):
        pl.semaphore_signal(barrier, inc=1, device_id={"seq": device}, device_id_type=MESH)
    for away in range(1, ring):
        pl.semaphore_signal(
            barrier, inc=1, device_id={"tp": tp_at(away)}, device_id_type=MESH
        )
    for move in moves:
        pl.semaphore_signal(
            barrier, inc=1, device_id={"seq": 2 * chip_at(move) + core}, device_id_type=MESH
        )

    for b in range(batch):
        rows[b, 0:HALO, :] = jnp.zeros((HALO, rows.shape[2]), BF16)
        small_pre[b, 0:LANES, :] = jnp.zeros((LANES, LANES), F32)
    heads = step_cols.shape[0]
    small_ref[0:narrow, :] = jnp.zeros((narrow, small_ref.shape[1]), BF16)
    small_ref[2 * narrow :, :] = jnp.zeros((LANES - 2 * narrow, small_ref.shape[1]), BF16)
    bias_ref[...] = jnp.zeros_like(bias_ref)
    rate_ref[...] = jnp.zeros_like(rate_ref)
    bc_square[...] = jnp.zeros_like(bc_square)
    lane = lax.broadcasted_iota(jnp.int32, expand_ref.shape, 1) // HEAD_DIM
    owner = lax.rem(lax.broadcasted_iota(jnp.int32, expand_ref.shape, 0), LANES)
    expand_ref[...] = jnp.where(lane == owner, 1.0, 0.0).astype(BF16)
    for load in little[:2]:
        load.wait()
    small_ref[0:heads, :] = step_cols[...]

    def small_product(part, b):
        loads[2 * b + part].wait()
        start = part * chunk
        small_pre[b, LANES + start : LANES + start + chunk, :] = dot_nt(
            rows[b, PAD + start : PAD + start + chunk, :], small_ref[...]
        )

    for b in range(batch):
        small_product(1, b)
    pl.semaphore_wait(barrier, 3 + (ring - 1) + (chips - 1))
    halo = remote(
        rows.at[:, pl.ds(PAD + length - HALO, HALO)], rows.at[:, pl.ds(PAD - HALO, HALO)],
        halo_sem.at[0], halo_sem.at[1], seq=after,
    )
    halo.start()
    value_load.start()
    for b in range(batch):
        small_product(0, b)
    for load in little[2:]:
        load.wait()
    bias_ref[:, 0:heads] = bias_small[...]
    rate_ref[:, 0:heads] = jnp.exp(rate_small[...])
    for part in range(2):
        cut = slice(part * LANES, (part + 1) * LANES)
        bc_square[0:CONV, :] = bc_taps[:, cut]
        bc_conv_ref[cut, :] = jnp.transpose(bc_square[...])
    taps = bc_conv_ref[pl.ds(pl.multiple_of(me * narrow, narrow), narrow), :]

    def bc_conv(x):
        total = taps[:, CONV - 1 : CONV] * x
        for k in range(1, CONV):
            total = total + taps[:, CONV - 1 - k : CONV - k] * pltpu.roll(x, k, 1)
        return silu(total).astype(BF16)

    def transpose_bc(b, piece):
        at = slice(piece * LANES, (piece + 1) * LANES)
        flipped = jnp.transpose(small_pre[b, at, :])[narrow : 2 * narrow, :]
        bc_wide[b, :, at] = flipped.astype(BF16).astype(F32)

    chunks = (
        (far, far_recv, blocks // 2, blocks, 1),
        (near, near_recv, 1, blocks // 2, -1),
        (first_slots, first_recv, 0, 1, -1),
    )

    def convolve(which):
        slots, _, low, high, _ = chunks[which]
        size = (high - low) * BLOCK
        for b in range(batch):
            done = bc_conv(bc_wide[b, :, low * LANES : (high + 1) * LANES])
            slots[me, :, b * size : (b + 1) * size] = done[:, LANES:]

    def ring_copy(which, source, steps, arrival):
        slots, recv = chunks[which][:2]
        source = tp_at(source % ring)
        return remote(
            slots.at[source], slots.at[source], ring_send.at[which], recv.at[arrival],
            tp=tp_at(steps % ring),
        )

    def ring_two(which):
        for way in (1, -1):
            ring_copy(which, 0, 2 * way, 0 if way == 1 else 1).start()

    def ring_one(which):
        for way in (1, -1):
            ring_copy(which, 0, way, 2).start()

    def ring_relay(which):
        for way in (1, -1):
            ring_copy(which, 0, 2 * way, 0 if way == 1 else 1).wait_recv()
            if chunks[which][4] == way:
                ring_copy(which, -2 * way, 2 * way, 2).start()
            ring_copy(which, -2 * way, way, 2).start()

    def ring_finish(which):
        slots, recv = chunks[which][:2]
        wait_bytes(slots, ring - 3, recv.at[2])

    def ring_sent(which):
        wait_bytes(chunks[which][0], ring - 1, ring_send.at[which])

    for b in range(batch):
        for piece in range(1, 1 + length // LANES):
            transpose_bc(b, piece)
    for which in range(2):
        convolve(which)
        ring_two(which)

    halo.wait()

    @pl.when(place == 0)
    def _():
        for b in range(batch):
            rows[b, 0:PAD, :] = jnp.zeros((PAD, rows.shape[2]), BF16)

    for b in range(batch):
        small_pre[b, LANES - PAD : LANES, :] = dot_nt(rows[b, 0:PAD, :], small_ref[...])
        transpose_bc(b, 0)
    convolve(2)
    ring_two(2)
    for which in range(3):
        ring_one(which)

    def gate_part(b, product):
        return silu(product.astype(BF16).astype(F32))

    def tile_of(index):
        cut = slice(index * TILE, (index + 1) * TILE)

        @pl.loop(0, batch)
        def _(b):
            if cut.start >= width:
                product = jnp.dot(
                    rows[b, PAD : PAD + length, :], weights[:, cut], preferred_element_type=F32
                )
                gates[b, :, cut.start - width : cut.stop - width] = gate_part(b, product)
            else:
                product = jnp.dot(rows[b], weights[:, cut], preferred_element_type=F32)
                inner = min(TILE, width - cut.start)
                pre[b, :, cut.start : cut.start + inner] = (
                    product[:, :inner].astype(BF16).astype(F32)
                )
                if inner < TILE:
                    gates[b, :, 0 : TILE - inner] = gate_part(b, product[PAD:, inner:])

    tiles = 2 * width // TILE
    value_tiles = -(-width // TILE)
    gate_load.start()
    value_load.wait()
    tile_of(0)

    row = lax.broadcasted_iota(jnp.int32, (BLOCK, BLOCK), 0)
    col = lax.broadcasted_iota(jnp.int32, (BLOCK, BLOCK), 1)
    triangle = jnp.where(row >= col, 1.0, 0.0).astype(F32)
    ms, mos, totals = [], [], []
    for b in range(batch):
        offset = jnp.zeros((1, LANES), F32)
        for k in range(blocks):
            step_pre = small_pre[b, LANES + k * BLOCK : LANES + (k + 1) * BLOCK, :] + bias_ref[...]
            steps = jnp.maximum(step_pre, 0.0) + jnp.log1p(jnp.exp(-jnp.abs(step_pre)))
            cumulative = jnp.dot(
                triangle, -steps * rate_ref[...],
                precision=lax.Precision.HIGHEST, preferred_element_type=F32,
            )
            last = cumulative[BLOCK - 1 : BLOCK, :]
            mid = 0.5 * last
            fin[b * blocks + k] = halves(jnp.exp(mid - cumulative) * steps)
            fout[b * blocks + k] = halves(jnp.exp(cumulative - mid))
            ms.append(mid)
            mos.append(mid + offset)
            offset = offset + last
        totals.append(offset)
    table = jnp.exp(jnp.concatenate(ms + mos, axis=0))
    ends[...] = jnp.dot(halves(table), expand_ref[...], preferred_element_type=F32)
    logs[...] = jnp.concatenate(totals + [jnp.zeros((8 - batch, LANES), F32)], axis=0)
    pair_log = remote(logs, pair_logs, log_sem.at[0], log_sem.at[1], seq=partner)
    pair_log.start()

    tile_of(1)
    for which in range(3):
        ring_relay(which)

    pair_log.wait()
    chip_logs[...] = logs[...] + pair_logs[...]
    all_logs[chip] = logs[...] + pair_logs[...]
    for move in moves:
        remote(
            chip_logs, all_logs.at[chip], log_send.at[0], log_recv.at[0],
            seq=2 * chip_at(move) + core,
        ).start()

    gate_load.wait()
    tile_of(2)

    def values_of(g):
        b, k = divmod(g, blocks)
        base = PAD + k * BLOCK - CONV + 1
        wide = jnp.dot(fin[g], expand_ref[...], preferred_element_type=F32)
        for start in range(0, width, LANES):
            cut = slice(start, start + LANES)
            x = conv_ref[0:1, cut] * pre[b, base : base + BLOCK, cut]
            for tap in range(1, CONV):
                x = x + conv_ref[tap : tap + 1, cut] * pre[
                    b, base + tap : base + tap + BLOCK, cut
                ]
            right[g, STATE:, cut] = (silu(x) * wide[:, cut]).astype(BF16)

    for g in range(total_blocks):
        values_of(g)
    for which in range(3):
        ring_finish(which)

    def bc_block(b, k, first):
        slots, _, low, high, _ = next(c for c in chunks if c[2] <= k < c[3])
        at = (b * (high - low) + k - low) * BLOCK
        return slots[first : first + ring // 2, :, at : at + BLOCK].reshape(STATE, BLOCK)

    for b in range(batch):
        held = jnp.zeros((STATE, width), F32)
        for k in range(blocks):
            g = b * blocks + k
            e = ends[g : g + 1, :]
            ahead = e * held
            right[g, :STATE, :] = ahead.astype(BF16)
            added = jnp.dot(
                bc_block(b, k, 0), right[g, STATE:, :], preferred_element_type=F32
            )
            held = e * (ahead + added)
        local[b] = held.astype(BF16)

    pair_copy = remote(local, pair, pair_sem.at[0], pair_sem.at[1], seq=partner)
    pair_copy.start()
    for g in range(total_blocks):
        b, k = divmod(g, blocks)
        b_flat = bc_block(b, k, 0)
        c_rows = jnp.transpose(bc_block(b, k, ring // 2).astype(F32)).astype(BF16)
        scores = jnp.dot(c_rows, b_flat, preferred_element_type=F32)
        left[g, :, :STATE] = c_rows
        left[g, :, STATE:] = jnp.where(row >= col, scores, 0.0).astype(BF16)
    wait_bytes(all_logs, chips - 1, log_send.at[0])
    wait_bytes(all_logs, chips - 1, log_recv.at[0])
    own_end = jnp.exp(logs[...])
    pair_end = jnp.exp(pair_logs[...])
    wide_ends = jnp.dot(
        halves(jnp.concatenate([own_end, pair_end], axis=0)), expand_ref[...],
        preferred_element_type=F32,
    )
    low = chip < chips // batch
    spans = jnp.concatenate(
        [jnp.where(low, all_logs[i, 0:1, :], all_logs[i, 1:2, :]) for i in range(chips)], axis=0
    )
    spans = jnp.dot(halves(jnp.exp(spans)), expand_ref[...], preferred_element_type=F32)

    pair_copy.wait()
    groups = chips // batch
    for b in range(batch):
        own = local[b, mine, :].astype(F32)
        theirs = pair[b, mine, :].astype(F32)
        first = jnp.where(core == 0, own, theirs)
        second = jnp.where(core == 0, theirs, own)
        later = jnp.where(core == 0, wide_ends[8 + b : 9 + b, :], wide_ends[b : b + 1, :])
        both = (later * first + second).reshape(groups, half // groups, width)
        sent[b * groups : (b + 1) * groups] = both.astype(BF16)
    got[chip] = sent[chip]
    for move in moves:
        peer = chip_at(move)
        remote(
            sent.at[peer], got.at[chip], out_send.at[0], out_recv.at[0], seq=2 * peer + core
        ).start()
    for index in range(value_tiles, tiles):
        tile_of(index)

    wait_bytes(got, chips - 1, out_send.at[0])
    wait_bytes(got, chips - 1, out_recv.at[0])
    running = jnp.zeros((half // groups, width), F32)
    for i in range(chips):
        prefix[i] = running.astype(BF16)
        if i + 1 < chips:
            running = spans[i : i + 1, :] * running + got[i].astype(F32)
    owned[chip] = prefix[chip]
    for move in moves:
        peer = chip_at(move)
        remote(
            prefix.at[peer], owned.at[chip], back_send.at[0], back_recv.at[0],
            seq=2 * peer + core,
        ).start()

    for g in range(total_blocks):
        b, k = divmod(g, blocks)
        at = slice(k * BLOCK, (k + 1) * BLOCK)
        wide = jnp.dot(fout[g], expand_ref[...], preferred_element_type=F32)
        y = jnp.dot(left[g], right[g], preferred_element_type=F32)
        weighted = wide * gates[b, at, :]
        gated_ref[b, at, :] = y * weighted
        other[b, at, :] = weighted * ends[total_blocks + g : total_blocks + g + 1, :]
    for which in range(3):
        ring_sent(which)
    wait_bytes(owned, chips - 1, back_send.at[0])
    wait_bytes(owned, chips - 1, back_recv.at[0])
    swap = remote(owned, owned_pair, swap_sem.at[0], swap_sem.at[1], seq=partner)
    swap.start()
    swap.wait()

    for b in range(batch):
        at = slice(b * groups, (b + 1) * groups)
        own = owned[at].astype(F32).reshape(half, width)
        theirs = owned_pair[at].astype(F32).reshape(half, width)
        span = wide_ends[8 + b : 9 + b, :]
        for c in range(2):
            cut = slice(c * half, (c + 1) * half)
            full = jnp.where(core == c, own, theirs)
            moved = span * full + pair[b, cut, :].astype(F32)
            entering[b, cut, :] = jnp.where(core == 0, full, moved).astype(BF16)

    for b in range(batch):
        for k in range(blocks):
            g = b * blocks + k
            at = slice(k * BLOCK, (k + 1) * BLOCK)
            extra = jnp.dot(left[g, :, :STATE], entering[b], preferred_element_type=F32)
            total = jnp.zeros((BLOCK, LANES), F32)
            for start in range(0, width, LANES):
                cut = slice(start, start + LANES)
                gated = gated_ref[b, at, cut] + other[b, at, cut] * extra[:, cut]
                gated_ref[b, at, cut] = gated * gain_ref[start // LANES : start // LANES + 1, :]
                total = total + gated * gated
            sums[g : g + 1, :] = jnp.sum(jnp.transpose(total), axis=0, keepdims=True)

    for away in turns:
        remote(sums, others.at[me], sum_send.at[0], sum_recv.at[0], tp=tp_at(away)).start()
    others[me] = sums[...]
    wait_bytes(others, ring - 1, sum_send.at[0])
    wait_bytes(others, ring - 1, sum_recv.at[0])
    whole_sq = others[0]
    for k in range(1, ring):
        whole_sq = whole_sq + others[k]
    scale_ref[...] = lax.rsqrt(whole_sq / DI + epsilon)


def norm_kernel(gated_ref, scale_ref, out_ref, done, sems):
    batch, length, width = gated_ref.shape
    copies = []
    for b in range(batch):
        for k in range(length // BLOCK):
            g = b * (length // BLOCK) + k
            at = slice(k * BLOCK, (k + 1) * BLOCK)
            column = jnp.transpose(jnp.broadcast_to(scale_ref[g : g + 1, :], (BLOCK, LANES)))
            for start in range(0, width, LANES):
                cut = slice(start, start + LANES)
                done[b, at, cut] = (gated_ref[b, at, cut] * column).astype(BF16)
            copies.append(pltpu.make_async_copy(
                done.at[b, pl.ds(k * BLOCK, BLOCK)], out_ref.at[b, pl.ds(k * BLOCK, BLOCK)],
                sems.at[g],
            ))
            copies[-1].start()
    for copy in copies:
        copy.wait()


def per_device(
    hidden_in, gate_proj, value_proj, bc_proj, step_proj,
    value_conv, bc_conv, step_bias, log_rate, norm_gain,
):
    batch, length, model_width = hidden_in.shape
    heads = step_proj.shape[1]
    width = value_proj.shape[1]
    narrow = bc_proj.shape[1]
    blocks = length // BLOCK
    tp = lax.axis_size("tp")
    chips = lax.axis_size("seq") // 2
    total_blocks = batch * blocks
    half = STATE // 2
    groups = chips // batch

    hbm = pl.BlockSpec(memory_space=pltpu.HBM)
    vmem = pl.BlockSpec(memory_space=pltpu.VMEM)
    dma = pltpu.SemaphoreType.DMA
    gated, scale = pl.pallas_call(
        mixer_kernel,
        out_shape=(
            jax.ShapeDtypeStruct((batch, length, width), F32),
            jax.ShapeDtypeStruct((total_blocks, LANES), F32),
        ),
        in_specs=[hbm] * 10,
        out_specs=[vmem, vmem],
        scratch_shapes=[
            pltpu.VMEM((LANES, model_width), BF16),
            pltpu.VMEM((heads, model_width), BF16),
            pltpu.VMEM((CONV, width), F32),
            pltpu.VMEM((CONV, 2 * STATE), F32),
            pltpu.VMEM((LANES, LANES), F32),
            pltpu.VMEM((2 * STATE, LANES), F32),
            pltpu.VMEM((1, heads), F32),
            pltpu.VMEM((1, heads), F32),
            pltpu.VMEM((1, LANES), F32),
            pltpu.VMEM((1, LANES), F32),
            pltpu.VMEM((width // LANES, LANES), F32),
            pltpu.VMEM((2 * LANES, width), BF16),
            pltpu.VMEM((batch, PAD + length, model_width), BF16),
            pltpu.VMEM((model_width, 2 * width), BF16),
            pltpu.VMEM((batch, LANES + length, LANES), F32),
            pltpu.VMEM((batch, narrow, LANES + length), F32),
            pltpu.VMEM((total_blocks, BLOCK, 2 * LANES), BF16),
            pltpu.VMEM((total_blocks, BLOCK, 2 * LANES), BF16),
            pltpu.VMEM((2 * total_blocks, width), F32),
            pltpu.VMEM((8, LANES), F32),
            pltpu.VMEM((8, LANES), F32),
            pltpu.VMEM((8, LANES), F32),
            pltpu.VMEM((chips, 8, LANES), F32),
            pltpu.VMEM((tp, narrow, batch * (blocks - blocks // 2) * BLOCK), BF16),
            pltpu.VMEM((tp, narrow, batch * (blocks // 2 - 1) * BLOCK), BF16),
            pltpu.VMEM((tp, narrow, batch * BLOCK), BF16),
            pltpu.VMEM((batch, PAD + length, width), F32),
            pltpu.VMEM((batch, length, width), F32),
            pltpu.VMEM((total_blocks, BLOCK, STATE + BLOCK), BF16),
            pltpu.VMEM((total_blocks, STATE + BLOCK, width), BF16),
            pltpu.VMEM((batch, length, width), F32),
            pltpu.VMEM((batch, STATE, width), BF16),
            pltpu.VMEM((batch, STATE, width), BF16),
            pltpu.VMEM((chips, half // groups, width), BF16),
            pltpu.VMEM((chips, half // groups, width), BF16),
            pltpu.VMEM((chips, half // groups, width), BF16),
            pltpu.VMEM((chips, half // groups, width), BF16),
            pltpu.VMEM((chips, half // groups, width), BF16),
            pltpu.VMEM((batch, STATE, width), BF16),
            pltpu.VMEM((total_blocks, LANES), F32),
            pltpu.VMEM((tp, total_blocks, LANES), F32),
            dma((2 * batch + 2,)),
            dma((7,)),
            dma((2,)),
            dma((2,)),
            dma((1,)),
            dma((1,)),
            dma((3,)),
            dma((3,)),
            dma((3,)),
            dma((3,)),
            dma((2,)),
            dma((1,)),
            dma((1,)),
            dma((1,)),
            dma((1,)),
            dma((2,)),
            dma((1,)),
            dma((1,)),
        ],
        compiler_params=pltpu.CompilerParams(
            vmem_limit_bytes=48 << 20, collective_id=0, has_side_effects=True
        ),
        name="mixer",
    )(*(pltpu.with_memory_space_constraint(x, pltpu.HBM) for x in (
        hidden_in, value_proj, gate_proj, bc_proj.T, step_proj.T, value_conv, bc_conv,
        step_bias.reshape(1, heads), log_rate.reshape(1, heads),
        norm_gain.reshape(width // LANES, LANES),
    )))

    return pl.pallas_call(
        norm_kernel,
        out_shape=jax.ShapeDtypeStruct((batch, length, width), BF16),
        in_specs=[vmem, vmem],
        out_specs=hbm,
        scratch_shapes=[pltpu.VMEM((batch, length, width), BF16), dma((total_blocks,))],
        compiler_params=pltpu.CompilerParams(vmem_limit_bytes=8 << 20),
        name="norm",
    )(gated, scale)


def solution(mesh):
    return jax.shard_map(
        per_device,
        mesh=mesh,
        in_specs=(
            P(None, "seq", None),
            P(None, "tp"),
            P(None, "tp"),
            P(None, "tp"),
            P(None, "tp"),
            P(None, "tp"),
            P(),
            P("tp"),
            P("tp"),
            P("tp"),
        ),
        out_specs=P(None, "seq", "tp"),
        check_vma=False,
    )
```

```python
import jax
import jax.numpy as jnp
from jax import lax
from jax.experimental import pallas as pl
from jax.experimental.pallas import tpu as pltpu
from jax.sharding import PartitionSpec as P

DI = 5120
HEAD_DIM = 64
STATE = 128
CONV = 4
BLOCK = 128
LANES = 128
PAD = 16
HALO = 8
TILE = 256
SIDE = 4
GREETED = (1, 2, 6, 7)
MESH = pl.DeviceIdType.MESH

epsilon = 1e-05
F32 = jnp.float32
BF16 = jnp.bfloat16


def silu(x):
    halved = 0.5 * x
    return halved + halved * jnp.tanh(halved)


def halves(x):
    high = x.astype(BF16)
    low = (x - high.astype(F32)).astype(BF16)
    return jnp.concatenate([high, low], axis=1)


def thirds(x):
    terms = []
    for _ in range(3):
        terms.append(x.astype(BF16))
        x = x - terms[-1].astype(F32)
    return jnp.concatenate(terms, axis=0)


def mixer_kernel(
    hidden_ref, value_ref, gate_ref, bc_in, step_in, conv_in, bc_conv_in,
    bias_in, rate_in, gain_in,
    gated_ref, scale_ref,
    small_ref, first_weights, step_cols, conv_ref, bc_taps, bc_square, bc_conv_ref,
    bias_small, rate_small, bias_ref, rate_ref, gain_ref, expand_ref, rows, weights, small_pre, bc_wide, fin, fout, ends, logs, pair_logs, chip_logs,
    all_logs, far, near, first_slots, pre, gates, left, right, other,
    local, pair, sent, got, prefix, owned, owned_pair, entering, sums, others,
    load_sem, small_sem, halo_sem, log_sem, log_send, log_recv, ring_send,
    far_recv, near_recv, first_recv, pair_sem, out_send, out_recv, back_send, back_recv,
    swap_sem, sum_send, sum_recv,
):
    batch, length, _ = hidden_ref.shape
    width = value_ref.shape[1]
    blocks = length // BLOCK
    total_blocks = batch * blocks
    narrow = bc_in.shape[0]
    me = lax.axis_index("tp")
    ring = lax.axis_size("tp")
    place = lax.axis_index("seq")
    devices = lax.axis_size("seq")
    chips = devices // 2
    core = lax.rem(place, 2)
    chip = place // 2
    partner = place + 1 - 2 * core
    after = lax.rem(place + 1, devices)
    before = lax.rem(place + devices - 1, devices)
    half = STATE // 2
    mine = pl.ds(pl.multiple_of(core * half, half), half)
    theirs_at = pl.ds(pl.multiple_of(half - core * half, half), half)

    across = SIDE
    along = chips // SIDE

    def chip_at(move):
        dy, dx = move
        return (
            lax.rem(chip // across + dy, along) * across
            + lax.rem(lax.rem(chip, across) + dx, across)
        )

    def hops(away, count):
        return min(away, count - away)

    moves = sorted(
        [(dy, dx) for dy in range(along) for dx in range(across) if dy or dx],
        key=lambda move: -(hops(move[0], along) + hops(move[1], across)),
    )
    turns = sorted(range(1, lax.axis_size("tp")), key=lambda away: -hops(away, lax.axis_size("tp")))

    def wait_bytes(ref, count, semaphore):
        part = ref.at[pl.ds(0, count)]
        pltpu.make_async_copy(part, part, semaphore).wait()

    def tp_at(away):
        return lax.rem(me + away, ring)

    def remote(source, target, send, recv, **device):
        return pltpu.make_async_remote_copy(
            src_ref=source, dst_ref=target, send_sem=send, recv_sem=recv,
            device_id=device, device_id_type=MESH,
        )

    little = [
        pltpu.make_async_copy(source, target, small_sem.at[i])
        for i, (source, target) in enumerate((
            (bc_in, small_ref.at[pl.ds(narrow, narrow)]), (step_in, step_cols),
            (bc_conv_in, bc_taps), (bias_in, bias_small), (rate_in, rate_small),
            (conv_in, conv_ref), (gain_in, gain_ref),
        ))
    ]
    for load in little:
        load.start()
    chunk = length // 2
    loads = []
    for b in range(batch):
        for part in range(2):
            loads.append(pltpu.make_async_copy(
                hidden_ref.at[b, pl.ds(part * chunk, chunk)],
                rows.at[b, pl.ds(PAD + part * chunk, chunk)], load_sem.at[2 * b + part],
            ))
    body = width - LANES
    gate_load = pltpu.make_async_copy(
        gate_ref, weights.at[:, pl.ds(body, width)], load_sem.at[2 * batch]
    )
    value_load = pltpu.make_async_copy(
        value_ref.at[:, pl.ds(0, body)], weights.at[:, pl.ds(0, body)],
        load_sem.at[2 * batch + 1],
    )
    tail_load = pltpu.make_async_copy(
        value_ref.at[:, pl.ds(body, LANES)], first_weights.at[:, pl.ds(LANES, LANES)],
        load_sem.at[2 * batch + 2],
    )
    tail_load.start()
    order = [2 * b + part for part in (1, 0) for b in range(batch)]
    for i in order:
        loads[i].start()

    barrier = pltpu.get_barrier_semaphore()
    for device in (after, before, partner):
        pl.semaphore_signal(barrier, inc=1, device_id={"seq": device}, device_id_type=MESH)
    for away in GREETED:
        pl.semaphore_signal(
            barrier, inc=1, device_id={"tp": tp_at(away)}, device_id_type=MESH
        )
    for move in moves:
        pl.semaphore_signal(
            barrier, inc=1, device_id={"seq": 2 * chip_at(move) + core}, device_id_type=MESH
        )

    for b in range(batch):
        rows[b, 0:HALO, :] = jnp.zeros((HALO, rows.shape[2]), BF16)
        small_pre[b, 0:LANES, :] = jnp.zeros((LANES, LANES), F32)
    heads = step_cols.shape[0]
    small_ref[0:narrow, :] = jnp.zeros((narrow, small_ref.shape[1]), BF16)
    small_ref[2 * narrow :, :] = jnp.zeros((LANES - 2 * narrow, small_ref.shape[1]), BF16)
    bias_ref[...] = jnp.zeros_like(bias_ref)
    rate_ref[...] = jnp.zeros_like(rate_ref)
    bc_square[...] = jnp.zeros_like(bc_square)
    lane = lax.broadcasted_iota(jnp.int32, expand_ref.shape, 1) // HEAD_DIM
    owner = lax.rem(lax.broadcasted_iota(jnp.int32, expand_ref.shape, 0), LANES)
    expand_ref[...] = jnp.where(lane == owner, 1.0, 0.0).astype(BF16)
    for load in little[:2]:
        load.wait()
    small_ref[0:heads, :] = step_cols[...]

    for at in range(0, small_ref.shape[1], LANES):
        first_weights[at : at + LANES, :LANES] = jnp.transpose(small_ref[:, at : at + LANES])

    def first_products(product, b, small_at, value_at):
        small_pre[b, small_at, :] = product[:, :LANES]
        pre[b, value_at, body:] = product[:, LANES:].astype(BF16).astype(F32)

    tail_load.wait()

    @pl.loop(0, 2 * batch)
    def _(i):
        part = 1 - i // batch
        b = lax.rem(i, batch)
        start = pl.multiple_of(part * chunk, chunk)
        pltpu.make_async_copy(
            hidden_ref.at[b, pl.ds(start, chunk)], rows.at[b, pl.ds(PAD + start, chunk)],
            load_sem.at[2 * b + part],
        ).wait()
        product = jnp.dot(
            rows[b, pl.ds(PAD + start, chunk), :], first_weights[...], preferred_element_type=F32
        )
        first_products(product, b, pl.ds(LANES + start, chunk), pl.ds(PAD + start, chunk))

    pl.semaphore_wait(barrier, 3 + len(GREETED) + (chips - 1))
    halo = remote(
        rows.at[:, pl.ds(PAD + length - HALO, HALO)], rows.at[:, pl.ds(PAD - HALO, HALO)],
        halo_sem.at[0], halo_sem.at[1], seq=after,
    )
    @pl.when(place < devices - 1)
    def _():
        halo.start()

    value_load.start()
    for load in little[2:]:
        load.wait()
    bias_ref[:, 0:heads] = bias_small[...]
    rate_ref[:, 0:heads] = jnp.exp(rate_small[...])
    for part in range(2):
        cut = slice(part * LANES, (part + 1) * LANES)
        bc_square[0:CONV, :] = bc_taps[:, cut]
        bc_conv_ref[cut, :] = jnp.transpose(bc_square[...])
    taps = bc_conv_ref[pl.ds(pl.multiple_of(me * narrow, narrow), narrow), :]

    def bc_conv(x):
        total = taps[:, CONV - 1 : CONV] * x
        for k in range(1, CONV):
            total = total + taps[:, CONV - 1 - k : CONV - k] * pltpu.roll(x, k, 1)
        return silu(total).astype(BF16)

    def transpose_bc(b, piece):
        at = slice(piece * LANES, (piece + 1) * LANES)
        flipped = jnp.transpose(small_pre[b, at, :])[narrow : 2 * narrow, :]
        bc_wide[b, :, at] = flipped.astype(BF16).astype(F32)

    chunks = (
        (far, far_recv, blocks // 2, blocks, 1),
        (near, near_recv, 1, blocks // 2, -1),
        (first_slots, first_recv, 0, 1, -1),
    )
    b_way = jnp.where(jnp.logical_and(me >= 2, me < 2 + ring // 2), 1, -1)

    def convolve(which):
        slots, _, low, high, _ = chunks[which]
        size = (high - low) * BLOCK
        for b in range(batch):
            done = bc_conv(bc_wide[b, :, low * LANES : (high + 1) * LANES])
            slots[me, :, b * size : (b + 1) * size] = done[:, LANES:]

    def ring_copy(which, source, target):
        slots, recv = chunks[which][:2]
        return remote(
            slots.at[source], slots.at[source], ring_send.at[which], recv.at[source], tp=target
        )

    def ring_own(which, steps):
        for away in (steps, ring - steps):
            ring_copy(which, me, tp_at(away)).start()

    def ring_relay(which, way):
        source = tp_at(ring - 2 * way)
        ring_copy(which, source, tp_at(1)).wait_recv()

        @pl.when(way == chunks[which][4])
        def _():
            ring_copy(which, source, tp_at(ring + 2 * way)).start()

        ring_copy(which, source, tp_at(ring + way)).start()

    def ring_finish(which, first, way):
        passed = tp_at(ring - 2 * way)
        for source in range(first, first + ring // 2):
            @pl.when(jnp.logical_and(me != source, passed != source))
            def _():
                ring_copy(which, source, tp_at(1)).wait_recv()

    def ring_sent(which):
        wait_bytes(chunks[which][0], ring - 1, ring_send.at[which])

    for b in range(batch):
        for piece in range(1, 1 + length // LANES):
            transpose_bc(b, piece)
    for which in range(2):
        convolve(which)
        ring_own(which, 2)
    for which in range(2):
        ring_own(which, 1)

    row = lax.broadcasted_iota(jnp.int32, (BLOCK, BLOCK), 0)
    col = lax.broadcasted_iota(jnp.int32, (BLOCK, BLOCK), 1)
    triangle = jnp.where(row >= col, 1.0, 0.0).astype(BF16)
    triangle = jnp.concatenate([triangle] * 3, axis=1)
    ms, mos, totals = [], [], []
    for b in range(batch):
        offset = jnp.zeros((1, LANES), F32)
        for k in range(blocks):
            step_pre = small_pre[b, LANES + k * BLOCK : LANES + (k + 1) * BLOCK, :] + bias_ref[...]
            steps = jnp.maximum(step_pre, 0.0) + jnp.log1p(jnp.exp(-jnp.abs(step_pre)))
            cumulative = jnp.dot(
                triangle, thirds(-steps * rate_ref[...]), preferred_element_type=F32
            )
            last = cumulative[BLOCK - 1 : BLOCK, :]
            mid = 0.5 * last
            fin[b * blocks + k] = halves(jnp.exp(mid - cumulative) * steps)
            fout[b * blocks + k] = halves(jnp.exp(cumulative - mid))
            ms.append(mid)
            mos.append(mid + offset)
            offset = offset + last
        totals.append(offset)
    table = jnp.exp(jnp.concatenate(ms + mos, axis=0))
    ends[...] = jnp.dot(halves(table), expand_ref[...], preferred_element_type=F32)
    logs[...] = jnp.concatenate(totals + [jnp.zeros((8 - batch, LANES), F32)], axis=0)
    pair_log = remote(logs, pair_logs, log_sem.at[0], log_sem.at[1], seq=partner)
    pair_log.start()

    @pl.when(place < devices - 1)
    def _():
        halo.wait_send()

    @pl.when(place > 0)
    def _():
        halo.wait_recv()

    @pl.when(place == 0)
    def _():
        for b in range(batch):
            rows[b, 0:PAD, :] = jnp.zeros((PAD, rows.shape[2]), BF16)

    product = jnp.dot(
        jnp.concatenate([rows[b, 0:PAD, :] for b in range(batch)], axis=0), first_weights[...],
        preferred_element_type=F32,
    )
    for b in range(batch):
        first_products(
            product[b * PAD : (b + 1) * PAD], b, slice(LANES - PAD, LANES), slice(0, PAD)
        )
        transpose_bc(b, 0)
    convolve(2)
    ring_own(2, 2)
    ring_own(2, 1)

    def gate_part(b, product):
        return silu(product.astype(BF16).astype(F32))

    def tile_of(start, size):
        cut = slice(start, start + size)

        @pl.loop(0, batch)
        def _(b):
            if start >= body:
                product = jnp.dot(
                    rows[b, PAD : PAD + length, :], weights[:, cut], preferred_element_type=F32
                )
                gates[b, :, start - body : start - body + size] = gate_part(b, product)
            else:
                product = jnp.dot(rows[b], weights[:, cut], preferred_element_type=F32)
                pre[b, :, cut] = product.astype(BF16).astype(F32)

    value_tiles = [(at, TILE) for at in range(0, body, TILE)]
    gate_tiles = [
        (at, min(TILE, body + width - at)) for at in range(body, body + width, TILE)
    ]
    gate_load.start()
    value_load.wait()
    tile_of(*value_tiles[0])

    pair_log.wait()
    chip_logs[...] = logs[...] + pair_logs[...]
    all_logs[chip] = logs[...] + pair_logs[...]
    for move in moves:
        remote(
            chip_logs, all_logs.at[chip], log_send.at[0], log_recv.at[0],
            seq=2 * chip_at(move) + core,
        ).start()
    for which in range(2):
        ring_relay(which, b_way)
    for start, size in value_tiles[1:]:
        tile_of(start, size)
    ring_relay(2, b_way)

    def values_of(g):
        b, k = divmod(g, blocks)
        base = PAD + k * BLOCK - HALO
        wide = jnp.dot(fin[g], expand_ref[...], preferred_element_type=F32)
        for start in range(0, width, LANES):
            cut = slice(start, start + LANES)
            window = pre[b, base : base + HALO + BLOCK, cut]
            x = conv_ref[0:1, cut] * window
            for tap in range(1, CONV):
                x = pltpu.roll(x, 1, 0) + conv_ref[tap : tap + 1, cut] * window
            right[g, STATE:, cut] = (silu(x[HALO:]) * wide[:, cut]).astype(BF16)

    for g in range(total_blocks):
        values_of(g)
    for which in range(3):
        ring_finish(which, 0, b_way)

    def bc_block(b, k, first):
        slots, _, low, high, _ = next(c for c in chunks if c[2] <= k < c[3])
        at = (b * (high - low) + k - low) * BLOCK
        return slots[first : first + ring // 2, :, at : at + BLOCK].reshape(STATE, BLOCK)

    for b in range(batch):
        held = jnp.zeros((STATE, width), F32)
        for k in range(blocks):
            g = b * blocks + k
            e = ends[g : g + 1, :]
            ahead = e * held
            right[g, :STATE, :] = ahead.astype(BF16)
            added = jnp.dot(
                bc_block(b, k, 0), right[g, STATE:, :], preferred_element_type=F32
            )
            held = e * (ahead + added)
        local[b] = held.astype(BF16)

    def pair_copy(at, index):
        return remote(
            local.at[:, at], pair.at[:, at], pair_sem.at[index], pair_sem.at[index + 1],
            seq=partner,
        )

    pair_copy(theirs_at, 0).start()
    pair_copy(mine, 2).start()
    for which in range(3):
        ring_relay(which, -b_way)
    wait_bytes(all_logs, chips - 1, log_send.at[0])
    wait_bytes(all_logs, chips - 1, log_recv.at[0])
    own_end = jnp.exp(logs[...])
    pair_end = jnp.exp(pair_logs[...])
    wide_ends = jnp.dot(
        halves(jnp.concatenate([own_end, pair_end], axis=0)), expand_ref[...],
        preferred_element_type=F32,
    )
    low = chip < chips // batch
    spans = jnp.concatenate(
        [jnp.where(low, all_logs[i, 0:1, :], all_logs[i, 1:2, :]) for i in range(chips)], axis=0
    )
    spans = jnp.dot(halves(jnp.exp(spans)), expand_ref[...], preferred_element_type=F32)

    pair_copy(theirs_at, 0).wait()
    groups = chips // batch
    for b in range(batch):
        own = local[b, mine, :].astype(F32)
        theirs = pair[b, mine, :].astype(F32)
        first = jnp.where(core == 0, own, theirs)
        second = jnp.where(core == 0, theirs, own)
        later = jnp.where(core == 0, wide_ends[8 + b : 9 + b, :], wide_ends[b : b + 1, :])
        both = (later * first + second).reshape(groups, half // groups, width)
        sent[b * groups : (b + 1) * groups] = both.astype(BF16)
    got[chip] = sent[chip]
    for move in moves:
        peer = chip_at(move)
        remote(
            sent.at[peer], got.at[chip], out_send.at[0], out_recv.at[0], seq=2 * peer + core
        ).start()
    gate_load.wait()
    for start, size in gate_tiles[:2]:
        tile_of(start, size)

    wait_bytes(got, chips - 1, out_send.at[0])
    wait_bytes(got, chips - 1, out_recv.at[0])
    running = jnp.zeros((half // groups, width), F32)
    for i in range(chips):
        prefix[i] = running.astype(BF16)
        if i + 1 < chips:
            running = spans[i : i + 1, :] * running + got[i].astype(F32)
    owned[chip] = prefix[chip]
    for move in moves:
        peer = chip_at(move)
        remote(
            prefix.at[peer], owned.at[chip], back_send.at[0], back_recv.at[0],
            seq=2 * peer + core,
        ).start()

    for start, size in gate_tiles[2:]:
        tile_of(start, size)
    for which in range(3):
        ring_finish(which, ring // 2, -b_way)
    for g in range(total_blocks):
        b, k = divmod(g, blocks)
        b_flat = bc_block(b, k, 0)
        c_rows = jnp.transpose(bc_block(b, k, ring // 2).astype(F32)).astype(BF16)
        scores = jnp.dot(c_rows, b_flat, preferred_element_type=F32)
        left[g, :, :STATE] = c_rows
        left[g, :, STATE:] = jnp.where(row >= col, scores, 0.0).astype(BF16)
    for g in range(total_blocks):
        b, k = divmod(g, blocks)
        at = slice(k * BLOCK, (k + 1) * BLOCK)
        wide = jnp.dot(fout[g], expand_ref[...], preferred_element_type=F32)
        y = jnp.dot(left[g], right[g], preferred_element_type=F32)
        weighted = wide * gates[b, at, :]
        gated_ref[b, at, :] = y * weighted
        other[b, at, :] = weighted * ends[total_blocks + g : total_blocks + g + 1, :]
    for which in range(3):
        ring_sent(which)
    wait_bytes(owned, chips - 1, back_send.at[0])
    wait_bytes(owned, chips - 1, back_recv.at[0])
    swap = remote(owned, owned_pair, swap_sem.at[0], swap_sem.at[1], seq=partner)
    swap.start()
    pair_copy(mine, 2).wait()
    swap.wait()

    for b in range(batch):
        at = slice(b * groups, (b + 1) * groups)
        own = owned[at].astype(F32).reshape(half, width)
        theirs = owned_pair[at].astype(F32).reshape(half, width)
        span = wide_ends[8 + b : 9 + b, :]
        for c in range(2):
            cut = slice(c * half, (c + 1) * half)
            full = jnp.where(core == c, own, theirs)
            moved = span * full + pair[b, cut, :].astype(F32)
            entering[b, cut, :] = jnp.where(core == 0, full, moved).astype(BF16)

    for b in range(batch):
        for k in range(blocks):
            g = b * blocks + k
            at = slice(k * BLOCK, (k + 1) * BLOCK)
            extra = jnp.dot(left[g, :, :STATE], entering[b], preferred_element_type=F32)
            total = jnp.zeros((BLOCK, LANES), F32)
            for start in range(0, width, LANES):
                cut = slice(start, start + LANES)
                gated = gated_ref[b, at, cut] + other[b, at, cut] * extra[:, cut]
                gated_ref[b, at, cut] = gated * gain_ref[start // LANES : start // LANES + 1, :]
                total = total + gated * gated
            sums[g : g + 1, :] = jnp.sum(jnp.transpose(total), axis=0, keepdims=True)

    for away in turns:
        remote(sums, others.at[me], sum_send.at[0], sum_recv.at[0], tp=tp_at(away)).start()
    others[me] = sums[...]
    wait_bytes(others, ring - 1, sum_send.at[0])
    wait_bytes(others, ring - 1, sum_recv.at[0])
    whole_sq = others[0]
    for k in range(1, ring):
        whole_sq = whole_sq + others[k]
    scale_ref[...] = lax.rsqrt(whole_sq / DI + epsilon)


def norm_kernel(gated_ref, scale_ref, out_ref, done, sems):
    batch, length, width = gated_ref.shape
    copies = []
    for b in range(batch):
        for k in range(length // BLOCK):
            g = b * (length // BLOCK) + k
            at = slice(k * BLOCK, (k + 1) * BLOCK)
            column = jnp.transpose(jnp.broadcast_to(scale_ref[g : g + 1, :], (BLOCK, LANES)))
            for start in range(0, width, LANES):
                cut = slice(start, start + LANES)
                done[b, at, cut] = (gated_ref[b, at, cut] * column).astype(BF16)
            copies.append(pltpu.make_async_copy(
                done.at[b, pl.ds(k * BLOCK, BLOCK)], out_ref.at[b, pl.ds(k * BLOCK, BLOCK)],
                sems.at[g],
            ))
            copies[-1].start()
    for copy in copies:
        copy.wait()


def per_device(
    hidden_in, gate_proj, value_proj, bc_proj, step_proj,
    value_conv, bc_conv, step_bias, log_rate, norm_gain,
):
    batch, length, model_width = hidden_in.shape
    heads = step_proj.shape[1]
    width = value_proj.shape[1]
    narrow = bc_proj.shape[1]
    blocks = length // BLOCK
    tp = lax.axis_size("tp")
    chips = lax.axis_size("seq") // 2
    total_blocks = batch * blocks
    half = STATE // 2
    groups = chips // batch

    hbm = pl.BlockSpec(memory_space=pltpu.HBM)
    vmem = pl.BlockSpec(memory_space=pltpu.VMEM)
    dma = pltpu.SemaphoreType.DMA
    gated, scale = pl.pallas_call(
        mixer_kernel,
        out_shape=(
            jax.ShapeDtypeStruct((batch, length, width), F32),
            jax.ShapeDtypeStruct((total_blocks, LANES), F32),
        ),
        in_specs=[hbm] * 10,
        out_specs=[vmem, vmem],
        scratch_shapes=[
            pltpu.VMEM((LANES, model_width), BF16),
            pltpu.VMEM((model_width, 2 * LANES), BF16),
            pltpu.VMEM((heads, model_width), BF16),
            pltpu.VMEM((CONV, width), F32),
            pltpu.VMEM((CONV, 2 * STATE), F32),
            pltpu.VMEM((LANES, LANES), F32),
            pltpu.VMEM((2 * STATE, LANES), F32),
            pltpu.VMEM((1, heads), F32),
            pltpu.VMEM((1, heads), F32),
            pltpu.VMEM((1, LANES), F32),
            pltpu.VMEM((1, LANES), F32),
            pltpu.VMEM((width // LANES, LANES), F32),
            pltpu.VMEM((2 * LANES, width), BF16),
            pltpu.VMEM((batch, PAD + length, model_width), BF16),
            pltpu.VMEM((model_width, 2 * width - LANES), BF16),
            pltpu.VMEM((batch, LANES + length, LANES), F32),
            pltpu.VMEM((batch, narrow, LANES + length), F32),
            pltpu.VMEM((total_blocks, BLOCK, 2 * LANES), BF16),
            pltpu.VMEM((total_blocks, BLOCK, 2 * LANES), BF16),
            pltpu.VMEM((2 * total_blocks, width), F32),
            pltpu.VMEM((8, LANES), F32),
            pltpu.VMEM((8, LANES), F32),
            pltpu.VMEM((8, LANES), F32),
            pltpu.VMEM((chips, 8, LANES), F32),
            pltpu.VMEM((tp, narrow, batch * (blocks - blocks // 2) * BLOCK), BF16),
            pltpu.VMEM((tp, narrow, batch * (blocks // 2 - 1) * BLOCK), BF16),
            pltpu.VMEM((tp, narrow, batch * BLOCK), BF16),
            pltpu.VMEM((batch, PAD + length, width), F32),
            pltpu.VMEM((batch, length, width), F32),
            pltpu.VMEM((total_blocks, BLOCK, STATE + BLOCK), BF16),
            pltpu.VMEM((total_blocks, STATE + BLOCK, width), BF16),
            pltpu.VMEM((batch, length, width), F32),
            pltpu.VMEM((batch, STATE, width), BF16),
            pltpu.VMEM((batch, STATE, width), BF16),
            pltpu.VMEM((chips, half // groups, width), BF16),
            pltpu.VMEM((chips, half // groups, width), BF16),
            pltpu.VMEM((chips, half // groups, width), BF16),
            pltpu.VMEM((chips, half // groups, width), BF16),
            pltpu.VMEM((chips, half // groups, width), BF16),
            pltpu.VMEM((batch, STATE, width), BF16),
            pltpu.VMEM((total_blocks, LANES), F32),
            pltpu.VMEM((tp, total_blocks, LANES), F32),
            dma((2 * batch + 3,)),
            dma((7,)),
            dma((2,)),
            dma((2,)),
            dma((1,)),
            dma((1,)),
            dma((3,)),
            dma((tp,)),
            dma((tp,)),
            dma((tp,)),
            dma((4,)),
            dma((1,)),
            dma((1,)),
            dma((1,)),
            dma((1,)),
            dma((2,)),
            dma((1,)),
            dma((1,)),
        ],
        compiler_params=pltpu.CompilerParams(
            vmem_limit_bytes=48 << 20, collective_id=0, has_side_effects=True
        ),
        name="mixer",
    )(*(pltpu.with_memory_space_constraint(x, pltpu.HBM) for x in (
        hidden_in, value_proj, gate_proj, bc_proj.T, step_proj.T, value_conv, bc_conv,
        step_bias.reshape(1, heads), log_rate.reshape(1, heads),
        norm_gain.reshape(width // LANES, LANES),
    )))

    return pl.pallas_call(
        norm_kernel,
        out_shape=jax.ShapeDtypeStruct((batch, length, width), BF16),
        in_specs=[vmem, vmem],
        out_specs=hbm,
        scratch_shapes=[pltpu.VMEM((batch, length, width), BF16), dma((total_blocks,))],
        compiler_params=pltpu.CompilerParams(vmem_limit_bytes=8 << 20),
        name="norm",
    )(gated, scale)


def solution(mesh):
    return jax.shard_map(
        per_device,
        mesh=mesh,
        in_specs=(
            P(None, "seq", None),
            P(None, "tp"),
            P(None, "tp"),
            P(None, "tp"),
            P(None, "tp"),
            P(None, "tp"),
            P(),
            P("tp"),
            P("tp"),
            P("tp"),
        ),
        out_specs=P(None, "seq", "tp"),
        check_vma=False,
    )
```

```python
import jax
import jax.numpy as jnp
from jax import lax
from jax.experimental import pallas as pl
from jax.experimental.pallas import tpu as pltpu
from jax.sharding import PartitionSpec as P

DI = 5120
HEAD_DIM = 64
STATE = 128
CONV = 4
BLOCK = 128
LANES = 128
PAD = 16
HALO = 8
TILE = 256
SIDE = 4
GREETED = (1, 2, 6, 7)
MESH = pl.DeviceIdType.MESH

epsilon = 1e-05
F32 = jnp.float32
BF16 = jnp.bfloat16


def silu(x):
    halved = 0.5 * x
    return halved + halved * jnp.tanh(halved)


def halves(x):
    high = x.astype(BF16)
    low = (x - high.astype(F32)).astype(BF16)
    return jnp.concatenate([high, low], axis=1)


def thirds(x):
    terms = []
    for _ in range(3):
        terms.append(x.astype(BF16))
        x = x - terms[-1].astype(F32)
    return jnp.concatenate(terms, axis=0)


def mixer_kernel(
    hidden_ref, value_ref, gate_ref, bc_in, step_in, conv_in, bc_conv_in,
    bias_in, rate_in, gain_in,
    gated_ref, scale_ref,
    small_ref, first_weights, step_cols, conv_ref, bc_taps, bc_square, bc_conv_ref,
    bias_small, rate_small, bias_ref, rate_ref, gain_ref, expand_ref, rows, weights, small_pre, bc_wide, fin, fout, ends, logs, pair_logs, chip_logs,
    all_logs, far, near, first_slots, pre, gates, left, right, other,
    local, pair, sent, got, prefix, owned, owned_pair, entering, sums, others,
    greet_sem, load_sem, small_sem, halo_sem, log_sem, log_send, log_recv, ring_send,
    far_recv, near_recv, first_recv, pair_sem, out_send, out_recv, back_send, back_recv,
    swap_sem, sum_send, sum_recv,
):
    batch, length, _ = hidden_ref.shape
    width = value_ref.shape[1]
    blocks = length // BLOCK
    total_blocks = batch * blocks
    narrow = bc_in.shape[0]
    me = lax.axis_index("tp")
    ring = lax.axis_size("tp")
    place = lax.axis_index("seq")
    devices = lax.axis_size("seq")
    chips = devices // 2
    core = lax.rem(place, 2)
    chip = place // 2
    partner = place + 1 - 2 * core
    after = lax.rem(place + 1, devices)
    before = lax.rem(place + devices - 1, devices)
    half = STATE // 2
    mine = pl.ds(pl.multiple_of(core * half, half), half)
    theirs_at = pl.ds(pl.multiple_of(half - core * half, half), half)

    across = SIDE
    along = chips // SIDE

    def chip_at(move):
        dy, dx = move
        return (
            lax.rem(chip // across + dy, along) * across
            + lax.rem(lax.rem(chip, across) + dx, across)
        )

    def hops(away, count):
        return min(away, count - away)

    moves = sorted(
        [(dy, dx) for dy in range(along) for dx in range(across) if dy or dx],
        key=lambda move: -(hops(move[0], along) + hops(move[1], across)),
    )
    turns = sorted(range(1, lax.axis_size("tp")), key=lambda away: -hops(away, lax.axis_size("tp")))

    def wait_bytes(ref, count, semaphore):
        part = ref.at[pl.ds(0, count)]
        pltpu.make_async_copy(part, part, semaphore).wait()

    def tp_at(away):
        return lax.rem(me + away, ring)

    def remote(source, target, send, recv, **device):
        return pltpu.make_async_remote_copy(
            src_ref=source, dst_ref=target, send_sem=send, recv_sem=recv,
            device_id=device, device_id_type=MESH,
        )

    little = [
        pltpu.make_async_copy(source, target, small_sem.at[i])
        for i, (source, target) in enumerate((
            (bc_in, small_ref.at[pl.ds(narrow, narrow)]), (step_in, step_cols),
            (bc_conv_in, bc_taps), (bias_in, bias_small), (rate_in, rate_small),
            (conv_in, conv_ref), (gain_in, gain_ref),
        ))
    ]
    for load in little:
        load.start()
    chunk = length // 2
    loads = []
    for b in range(batch):
        for part in range(2):
            loads.append(pltpu.make_async_copy(
                hidden_ref.at[b, pl.ds(part * chunk, chunk)],
                rows.at[b, pl.ds(PAD + part * chunk, chunk)], load_sem.at[2 * b + part],
            ))
    body = width - LANES
    gate_load = pltpu.make_async_copy(
        gate_ref, weights.at[:, pl.ds(body, width)], load_sem.at[2 * batch]
    )
    value_load = pltpu.make_async_copy(
        value_ref.at[:, pl.ds(0, body)], weights.at[:, pl.ds(0, body)],
        load_sem.at[2 * batch + 1],
    )
    tail_load = pltpu.make_async_copy(
        value_ref.at[:, pl.ds(body, LANES)], first_weights.at[:, pl.ds(LANES, LANES)],
        load_sem.at[2 * batch + 2],
    )
    tail_load.start()
    order = [2 * b + part for part in (1, 0) for b in range(batch)]
    for i in order:
        loads[i].start()

    barrier = pltpu.get_barrier_semaphore()
    for device in (after, before, partner):
        pl.semaphore_signal(barrier, inc=1, device_id={"seq": device}, device_id_type=MESH)
    for away in GREETED:
        pl.semaphore_signal(
            barrier, inc=1, device_id={"tp": tp_at(away)}, device_id_type=MESH
        )
    def greet(semaphore):
        for move in ((0, 1), (0, across - 1), (1, 0), (along - 1, 0)):
            pl.semaphore_signal(
                semaphore, inc=1, device_id={"seq": 2 * chip_at(move) + core},
                device_id_type=MESH,
            )

    greet(barrier)

    def greet_round(index):
        if index > 0:
            pl.semaphore_wait(greet_sem.at[index - 1], 4)
        if index < across // 2 + along // 2 - 1:
            greet(greet_sem.at[index])

    for b in range(batch):
        rows[b, 0:HALO, :] = jnp.zeros((HALO, rows.shape[2]), BF16)
        small_pre[b, 0:LANES, :] = jnp.zeros((LANES, LANES), F32)
    heads = step_cols.shape[0]
    small_ref[0:narrow, :] = jnp.zeros((narrow, small_ref.shape[1]), BF16)
    small_ref[2 * narrow :, :] = jnp.zeros((LANES - 2 * narrow, small_ref.shape[1]), BF16)
    bias_ref[...] = jnp.zeros_like(bias_ref)
    rate_ref[...] = jnp.zeros_like(rate_ref)
    bc_square[...] = jnp.zeros_like(bc_square)
    lane = lax.broadcasted_iota(jnp.int32, expand_ref.shape, 1) // HEAD_DIM
    owner = lax.rem(lax.broadcasted_iota(jnp.int32, expand_ref.shape, 0), LANES)
    expand_ref[...] = jnp.where(lane == owner, 1.0, 0.0).astype(BF16)
    for load in little[:2]:
        load.wait()
    small_ref[0:heads, :] = step_cols[...]

    for at in range(0, small_ref.shape[1], LANES):
        first_weights[at : at + LANES, :LANES] = jnp.transpose(small_ref[:, at : at + LANES])

    def first_products(product, b, small_at, value_at):
        small_pre[b, small_at, :] = product[:, :LANES]
        pre[b, value_at, body:] = product[:, LANES:].astype(BF16).astype(F32)

    tail_load.wait()

    def first_tile(part):
        for b in range(batch):
            loads[2 * b + part].wait()
        start = part * chunk
        for b in range(batch):
            product = jnp.dot(
                rows[b, PAD + start : PAD + start + chunk, :], first_weights[...],
                preferred_element_type=F32,
            )
            first_products(
                product, b, slice(LANES + start, LANES + start + chunk),
                slice(PAD + start, PAD + start + chunk),
            )

    first_tile(1)
    pl.semaphore_wait(barrier, 3 + len(GREETED) + 4)
    greet_round(0)
    halo = remote(
        rows.at[:, pl.ds(PAD + length - HALO, HALO)], rows.at[:, pl.ds(PAD - HALO, HALO)],
        halo_sem.at[0], halo_sem.at[1], seq=after,
    )
    @pl.when(place < devices - 1)
    def _():
        halo.start()

    value_load.start()
    first_tile(0)
    for load in little[2:]:
        load.wait()
    bias_ref[:, 0:heads] = bias_small[...]
    rate_ref[:, 0:heads] = jnp.exp(rate_small[...])
    for part in range(2):
        cut = slice(part * LANES, (part + 1) * LANES)
        bc_square[0:CONV, :] = bc_taps[:, cut]
        bc_conv_ref[cut, :] = jnp.transpose(bc_square[...])
    taps = bc_conv_ref[pl.ds(pl.multiple_of(me * narrow, narrow), narrow), :]

    def bc_conv(x):
        total = taps[:, CONV - 1 : CONV] * x
        for k in range(1, CONV):
            total = total + taps[:, CONV - 1 - k : CONV - k] * pltpu.roll(x, k, 1)
        return silu(total).astype(BF16)

    def transpose_bc(b, piece):
        at = slice(piece * LANES, (piece + 1) * LANES)
        flipped = jnp.transpose(small_pre[b, at, :])[narrow : 2 * narrow, :]
        bc_wide[b, :, at] = flipped.astype(BF16).astype(F32)

    chunks = (
        (far, far_recv, blocks // 2, blocks, 1),
        (near, near_recv, 1, blocks // 2, -1),
        (first_slots, first_recv, 0, 1, -1),
    )
    b_way = jnp.where(jnp.logical_and(me >= 2, me < 2 + ring // 2), 1, -1)

    def convolve(which):
        slots, _, low, high, _ = chunks[which]
        size = (high - low) * BLOCK
        for b in range(batch):
            done = bc_conv(bc_wide[b, :, low * LANES : (high + 1) * LANES])
            slots[me, :, b * size : (b + 1) * size] = done[:, LANES:]

    def ring_copy(which, source, target):
        slots, recv = chunks[which][:2]
        return remote(
            slots.at[source], slots.at[source], ring_send.at[which], recv.at[source], tp=target
        )

    def ring_own(which, steps):
        for away in (steps, ring - steps):
            ring_copy(which, me, tp_at(away)).start()

    def ring_relay(which, way):
        source = tp_at(ring - 2 * way)
        ring_copy(which, source, tp_at(1)).wait_recv()

        @pl.when(way == chunks[which][4])
        def _():
            ring_copy(which, source, tp_at(ring + 2 * way)).start()

        ring_copy(which, source, tp_at(ring + way)).start()

    def ring_finish(which, first, way):
        passed = tp_at(ring - 2 * way)
        for source in range(first, first + ring // 2):
            @pl.when(jnp.logical_and(me != source, passed != source))
            def _():
                ring_copy(which, source, tp_at(1)).wait_recv()

    def ring_sent(which):
        wait_bytes(chunks[which][0], ring - 1, ring_send.at[which])

    for b in range(batch):
        for piece in range(1, 1 + length // LANES):
            transpose_bc(b, piece)
    for which in range(2):
        convolve(which)
        ring_own(which, 2)
    for which in range(2):
        ring_own(which, 1)

    greet_round(1)

    row = lax.broadcasted_iota(jnp.int32, (BLOCK, BLOCK), 0)
    col = lax.broadcasted_iota(jnp.int32, (BLOCK, BLOCK), 1)
    triangle = jnp.where(row >= col, 1.0, 0.0).astype(BF16)
    triangle = jnp.concatenate([triangle] * 3, axis=1)
    ms, mos, totals = [], [], []
    for b in range(batch):
        offset = jnp.zeros((1, LANES), F32)
        for k in range(blocks):
            step_pre = small_pre[b, LANES + k * BLOCK : LANES + (k + 1) * BLOCK, :] + bias_ref[...]
            steps = jnp.maximum(step_pre, 0.0) + jnp.log1p(jnp.exp(-jnp.abs(step_pre)))
            cumulative = jnp.dot(
                triangle, thirds(-steps * rate_ref[...]), preferred_element_type=F32
            )
            last = cumulative[BLOCK - 1 : BLOCK, :]
            mid = 0.5 * last
            fin[b * blocks + k] = halves(jnp.exp(mid - cumulative) * steps)
            fout[b * blocks + k] = halves(jnp.exp(cumulative - mid))
            ms.append(mid)
            mos.append(mid + offset)
            offset = offset + last
        totals.append(offset)
    table = jnp.exp(jnp.concatenate(ms + mos, axis=0))
    ends[...] = jnp.dot(halves(table), expand_ref[...], preferred_element_type=F32)
    logs[...] = jnp.concatenate(totals + [jnp.zeros((8 - batch, LANES), F32)], axis=0)
    pair_log = remote(logs, pair_logs, log_sem.at[0], log_sem.at[1], seq=partner)
    pair_log.start()

    @pl.when(place < devices - 1)
    def _():
        halo.wait_send()

    @pl.when(place > 0)
    def _():
        halo.wait_recv()

    @pl.when(place == 0)
    def _():
        for b in range(batch):
            rows[b, 0:PAD, :] = jnp.zeros((PAD, rows.shape[2]), BF16)

    product = jnp.dot(
        jnp.concatenate([rows[b, 0:PAD, :] for b in range(batch)], axis=0), first_weights[...],
        preferred_element_type=F32,
    )
    for b in range(batch):
        first_products(
            product[b * PAD : (b + 1) * PAD], b, slice(LANES - PAD, LANES), slice(0, PAD)
        )
        transpose_bc(b, 0)
    convolve(2)
    ring_own(2, 2)
    ring_own(2, 1)
    greet_round(2)

    def gate_part(b, product):
        return silu(product.astype(BF16).astype(F32))

    def tile_of(start, size):
        cut = slice(start, start + size)
        for b in range(batch):
            if start >= body:
                product = jnp.dot(
                    rows[b, PAD : PAD + length, :], weights[:, cut], preferred_element_type=F32
                )
                gates[b, :, start - body : start - body + size] = gate_part(b, product)
            else:
                product = jnp.dot(rows[b], weights[:, cut], preferred_element_type=F32)
                pre[b, :, cut] = product.astype(BF16).astype(F32)

    value_tiles = [(at, TILE) for at in range(0, body, TILE)]
    gate_tiles = [
        (at, min(TILE, body + width - at)) for at in range(body, body + width, TILE)
    ]
    gate_load.start()
    value_load.wait()
    tile_of(*value_tiles[0])

    greet_round(3)
    pair_log.wait()
    chip_logs[...] = logs[...] + pair_logs[...]
    all_logs[chip] = logs[...] + pair_logs[...]
    for move in moves:
        remote(
            chip_logs, all_logs.at[chip], log_send.at[0], log_recv.at[0],
            seq=2 * chip_at(move) + core,
        ).start()
    def values_of(g, low, high):
        b, k = divmod(g, blocks)
        base = PAD + k * BLOCK - HALO
        wide = jnp.dot(fin[g], expand_ref[:, low:high], preferred_element_type=F32)
        for start in range(low, high, LANES):
            cut = slice(start, start + LANES)
            window = pre[b, base : base + HALO + BLOCK, cut]
            x = conv_ref[0:1, cut] * window
            for tap in range(1, CONV):
                x = pltpu.roll(x, 1, 0) + conv_ref[tap : tap + 1, cut] * window
            right[g, STATE:, cut] = (
                silu(x[HALO:]) * wide[:, start - low : start - low + LANES]
            ).astype(BF16)

    for which in range(2):
        ring_relay(which, b_way)
    for g in range(total_blocks):
        values_of(g, 0, TILE)
        values_of(g, body, width)
        if g == total_blocks // 2 - 1:
            ring_relay(2, b_way)
    for start, size in value_tiles[1:]:
        tile_of(start, size)
    for g in range(total_blocks):
        values_of(g, TILE, body)
    for which in range(3):
        ring_finish(which, 0, b_way)

    def bc_block(b, k, first):
        slots, _, low, high, _ = next(c for c in chunks if c[2] <= k < c[3])
        at = (b * (high - low) + k - low) * BLOCK
        return slots[first : first + ring // 2, :, at : at + BLOCK].reshape(STATE, BLOCK)

    for b in range(batch):
        held = jnp.zeros((STATE, width), F32)
        for k in range(blocks):
            g = b * blocks + k
            e = ends[g : g + 1, :]
            ahead = e * held
            right[g, :STATE, :] = ahead.astype(BF16)
            added = jnp.dot(
                bc_block(b, k, 0), right[g, STATE:, :], preferred_element_type=F32
            )
            held = e * (ahead + added)
        local[b] = held.astype(BF16)

    def pair_copy(at, index):
        return remote(
            local.at[:, at], pair.at[:, at], pair_sem.at[index], pair_sem.at[index + 1],
            seq=partner,
        )

    pair_copy(theirs_at, 0).start()
    pair_copy(mine, 2).start()
    for which in range(3):
        ring_relay(which, -b_way)
    wait_bytes(all_logs, chips - 1, log_send.at[0])
    wait_bytes(all_logs, chips - 1, log_recv.at[0])
    own_end = jnp.exp(logs[...])
    pair_end = jnp.exp(pair_logs[...])
    wide_ends = jnp.dot(
        halves(jnp.concatenate([own_end, pair_end], axis=0)), expand_ref[...],
        preferred_element_type=F32,
    )
    low = chip < chips // batch
    spans = jnp.concatenate(
        [jnp.where(low, all_logs[i, 0:1, :], all_logs[i, 1:2, :]) for i in range(chips)], axis=0
    )
    spans = jnp.dot(halves(jnp.exp(spans)), expand_ref[...], preferred_element_type=F32)

    pair_copy(theirs_at, 0).wait()
    groups = chips // batch
    for b in range(batch):
        own = local[b, mine, :].astype(F32)
        theirs = pair[b, mine, :].astype(F32)
        first = jnp.where(core == 0, own, theirs)
        second = jnp.where(core == 0, theirs, own)
        later = jnp.where(core == 0, wide_ends[8 + b : 9 + b, :], wide_ends[b : b + 1, :])
        both = (later * first + second).reshape(groups, half // groups, width)
        sent[b * groups : (b + 1) * groups] = both.astype(BF16)
    got[chip] = sent[chip]
    for move in moves:
        peer = chip_at(move)
        remote(
            sent.at[peer], got.at[chip], out_send.at[0], out_recv.at[0], seq=2 * peer + core
        ).start()
    gate_load.wait()
    for start, size in gate_tiles[:2]:
        tile_of(start, size)

    wait_bytes(got, chips - 1, out_send.at[0])
    wait_bytes(got, chips - 1, out_recv.at[0])
    running = jnp.zeros((half // groups, width), F32)
    for i in range(chips):
        prefix[i] = running.astype(BF16)
        if i + 1 < chips:
            running = spans[i : i + 1, :] * running + got[i].astype(F32)
    owned[chip] = prefix[chip]
    for move in moves:
        peer = chip_at(move)
        remote(
            prefix.at[peer], owned.at[chip], back_send.at[0], back_recv.at[0],
            seq=2 * peer + core,
        ).start()

    for start, size in gate_tiles[2:]:
        tile_of(start, size)
    for which in range(3):
        ring_finish(which, ring // 2, -b_way)
    for g in range(total_blocks):
        b, k = divmod(g, blocks)
        b_flat = bc_block(b, k, 0)
        c_rows = jnp.transpose(bc_block(b, k, ring // 2).astype(F32)).astype(BF16)
        scores = jnp.dot(c_rows, b_flat, preferred_element_type=F32)
        left[g, :, :STATE] = c_rows
        left[g, :, STATE:] = jnp.where(row >= col, scores, 0.0).astype(BF16)
    for g in range(total_blocks):
        b, k = divmod(g, blocks)
        at = slice(k * BLOCK, (k + 1) * BLOCK)
        wide = jnp.dot(fout[g], expand_ref[...], preferred_element_type=F32)
        y = jnp.dot(left[g], right[g], preferred_element_type=F32)
        weighted = wide * gates[b, at, :]
        gated_ref[b, at, :] = y * weighted
        other[b, at, :] = weighted * ends[total_blocks + g : total_blocks + g + 1, :]
    for which in range(3):
        ring_sent(which)
    wait_bytes(owned, chips - 1, back_send.at[0])
    wait_bytes(owned, chips - 1, back_recv.at[0])
    swap = remote(owned, owned_pair, swap_sem.at[0], swap_sem.at[1], seq=partner)
    swap.start()
    pair_copy(mine, 2).wait()
    swap.wait()

    for b in range(batch):
        at = slice(b * groups, (b + 1) * groups)
        own = owned[at].astype(F32).reshape(half, width)
        theirs = owned_pair[at].astype(F32).reshape(half, width)
        span = wide_ends[8 + b : 9 + b, :]
        for c in range(2):
            cut = slice(c * half, (c + 1) * half)
            full = jnp.where(core == c, own, theirs)
            moved = span * full + pair[b, cut, :].astype(F32)
            entering[b, cut, :] = jnp.where(core == 0, full, moved).astype(BF16)

    for b in range(batch):
        for k in range(blocks):
            g = b * blocks + k
            at = slice(k * BLOCK, (k + 1) * BLOCK)
            extra = jnp.dot(left[g, :, :STATE], entering[b], preferred_element_type=F32)
            total = jnp.zeros((BLOCK, LANES), F32)
            for start in range(0, width, LANES):
                cut = slice(start, start + LANES)
                gated = gated_ref[b, at, cut] + other[b, at, cut] * extra[:, cut]
                gated_ref[b, at, cut] = gated * gain_ref[start // LANES : start // LANES + 1, :]
                total = total + gated * gated
            sums[g : g + 1, :] = jnp.sum(jnp.transpose(total), axis=0, keepdims=True)

    for away in turns:
        remote(sums, others.at[me], sum_send.at[0], sum_recv.at[0], tp=tp_at(away)).start()
    others[me] = sums[...]
    wait_bytes(others, ring - 1, sum_send.at[0])
    wait_bytes(others, ring - 1, sum_recv.at[0])
    whole_sq = others[0]
    for k in range(1, ring):
        whole_sq = whole_sq + others[k]
    scale_ref[...] = lax.rsqrt(whole_sq / DI + epsilon)


def norm_kernel(gated_ref, scale_ref, out_ref, done, sems):
    batch, length, width = gated_ref.shape
    copies = []
    for b in range(batch):
        for k in range(length // BLOCK):
            g = b * (length // BLOCK) + k
            at = slice(k * BLOCK, (k + 1) * BLOCK)
            column = jnp.transpose(jnp.broadcast_to(scale_ref[g : g + 1, :], (BLOCK, LANES)))
            for start in range(0, width, LANES):
                cut = slice(start, start + LANES)
                done[b, at, cut] = (gated_ref[b, at, cut] * column).astype(BF16)
            copies.append(pltpu.make_async_copy(
                done.at[b, pl.ds(k * BLOCK, BLOCK)], out_ref.at[b, pl.ds(k * BLOCK, BLOCK)],
                sems.at[g],
            ))
            copies[-1].start()
    for copy in copies:
        copy.wait()


def per_device(
    hidden_in, gate_proj, value_proj, bc_proj, step_proj,
    value_conv, bc_conv, step_bias, log_rate, norm_gain,
):
    batch, length, model_width = hidden_in.shape
    heads = step_proj.shape[1]
    width = value_proj.shape[1]
    narrow = bc_proj.shape[1]
    blocks = length // BLOCK
    tp = lax.axis_size("tp")
    chips = lax.axis_size("seq") // 2
    total_blocks = batch * blocks
    half = STATE // 2
    groups = chips // batch

    hbm = pl.BlockSpec(memory_space=pltpu.HBM)
    vmem = pl.BlockSpec(memory_space=pltpu.VMEM)
    dma = pltpu.SemaphoreType.DMA
    gated, scale = pl.pallas_call(
        mixer_kernel,
        out_shape=(
            jax.ShapeDtypeStruct((batch, length, width), F32),
            jax.ShapeDtypeStruct((total_blocks, LANES), F32),
        ),
        in_specs=[hbm] * 10,
        out_specs=[vmem, vmem],
        scratch_shapes=[
            pltpu.VMEM((LANES, model_width), BF16),
            pltpu.VMEM((model_width, 2 * LANES), BF16),
            pltpu.VMEM((heads, model_width), BF16),
            pltpu.VMEM((CONV, width), F32),
            pltpu.VMEM((CONV, 2 * STATE), F32),
            pltpu.VMEM((LANES, LANES), F32),
            pltpu.VMEM((2 * STATE, LANES), F32),
            pltpu.VMEM((1, heads), F32),
            pltpu.VMEM((1, heads), F32),
            pltpu.VMEM((1, LANES), F32),
            pltpu.VMEM((1, LANES), F32),
            pltpu.VMEM((width // LANES, LANES), F32),
            pltpu.VMEM((2 * LANES, width), BF16),
            pltpu.VMEM((batch, PAD + length, model_width), BF16),
            pltpu.VMEM((model_width, 2 * width - LANES), BF16),
            pltpu.VMEM((batch, LANES + length, LANES), F32),
            pltpu.VMEM((batch, narrow, LANES + length), F32),
            pltpu.VMEM((total_blocks, BLOCK, 2 * LANES), BF16),
            pltpu.VMEM((total_blocks, BLOCK, 2 * LANES), BF16),
            pltpu.VMEM((2 * total_blocks, width), F32),
            pltpu.VMEM((8, LANES), F32),
            pltpu.VMEM((8, LANES), F32),
            pltpu.VMEM((8, LANES), F32),
            pltpu.VMEM((chips, 8, LANES), F32),
            pltpu.VMEM((tp, narrow, batch * (blocks - blocks // 2) * BLOCK), BF16),
            pltpu.VMEM((tp, narrow, batch * (blocks // 2 - 1) * BLOCK), BF16),
            pltpu.VMEM((tp, narrow, batch * BLOCK), BF16),
            pltpu.VMEM((batch, PAD + length, width), F32),
            pltpu.VMEM((batch, length, width), F32),
            pltpu.VMEM((total_blocks, BLOCK, STATE + BLOCK), BF16),
            pltpu.VMEM((total_blocks, STATE + BLOCK, width), BF16),
            pltpu.VMEM((batch, length, width), F32),
            pltpu.VMEM((batch, STATE, width), BF16),
            pltpu.VMEM((batch, STATE, width), BF16),
            pltpu.VMEM((chips, half // groups, width), BF16),
            pltpu.VMEM((chips, half // groups, width), BF16),
            pltpu.VMEM((chips, half // groups, width), BF16),
            pltpu.VMEM((chips, half // groups, width), BF16),
            pltpu.VMEM((chips, half // groups, width), BF16),
            pltpu.VMEM((batch, STATE, width), BF16),
            pltpu.VMEM((total_blocks, LANES), F32),
            pltpu.VMEM((tp, total_blocks, LANES), F32),
            pltpu.SemaphoreType.REGULAR((SIDE // 2 + chips // SIDE // 2 - 1,)),
            dma((2 * batch + 3,)),
            dma((7,)),
            dma((2,)),
            dma((2,)),
            dma((1,)),
            dma((1,)),
            dma((3,)),
            dma((tp,)),
            dma((tp,)),
            dma((tp,)),
            dma((4,)),
            dma((1,)),
            dma((1,)),
            dma((1,)),
            dma((1,)),
            dma((2,)),
            dma((1,)),
            dma((1,)),
        ],
        compiler_params=pltpu.CompilerParams(
            vmem_limit_bytes=48 << 20, collective_id=0, has_side_effects=True
        ),
        name="mixer",
    )(*(pltpu.with_memory_space_constraint(x, pltpu.HBM) for x in (
        hidden_in, value_proj, gate_proj, bc_proj.T, step_proj.T, value_conv, bc_conv,
        step_bias.reshape(1, heads), log_rate.reshape(1, heads),
        norm_gain.reshape(width // LANES, LANES),
    )))

    return pl.pallas_call(
        norm_kernel,
        out_shape=jax.ShapeDtypeStruct((batch, length, width), BF16),
        in_specs=[vmem, vmem],
        out_specs=hbm,
        scratch_shapes=[pltpu.VMEM((batch, length, width), BF16), dma((total_blocks,))],
        compiler_params=pltpu.CompilerParams(vmem_limit_bytes=8 << 20),
        name="norm",
    )(gated, scale)


def solution(mesh):
    return jax.shard_map(
        per_device,
        mesh=mesh,
        in_specs=(
            P(None, "seq", None),
            P(None, "tp"),
            P(None, "tp"),
            P(None, "tp"),
            P(None, "tp"),
            P(None, "tp"),
            P(),
            P("tp"),
            P("tp"),
            P("tp"),
        ),
        out_specs=P(None, "seq", "tp"),
        check_vma=False,
    )
```

```python
import jax
import jax.numpy as jnp
from jax import lax
from jax.experimental import pallas as pl
from jax.experimental.pallas import tpu as pltpu
from jax.sharding import PartitionSpec as P

DI = 5120
HEAD_DIM = 64
STATE = 128
CONV = 4
BLOCK = 128
LANES = 128
PAD = 16
HALO = 8
TILE = 256
SIDE = 4
GREETED = (1, 2, 6, 7)
MESH = pl.DeviceIdType.MESH

epsilon = 1e-05
F32 = jnp.float32
BF16 = jnp.bfloat16


def silu(x):
    halved = 0.5 * x
    return halved + halved * jnp.tanh(halved)


def halves(x):
    high = x.astype(BF16)
    low = (x - high.astype(F32)).astype(BF16)
    return jnp.concatenate([high, low], axis=1)


def thirds(x):
    terms = []
    for _ in range(3):
        terms.append(x.astype(BF16))
        x = x - terms[-1].astype(F32)
    return jnp.concatenate(terms, axis=0)


def mixer_kernel(
    hidden_ref, value_ref, gate_ref, bc_in, step_in, conv_in, bc_conv_in,
    bias_in, rate_in, gain_in,
    gated_ref, scale_ref,
    small_ref, first_weights, step_cols, conv_ref, bc_taps, bc_square, bc_conv_ref,
    bias_small, rate_small, bias_ref, rate_ref, gain_ref, expand_ref, rows, weights, small_pre, bc_wide, fin, fout, ends, logs, pair_logs, chip_logs,
    all_logs, far, near, first_slots, pre, gates, left, right, other,
    local, pair, sent, got, prefix, owned, owned_pair, entering, sums, others,
    greet_sem, load_sem, small_sem, halo_sem, log_sem, log_send, log_recv, ring_send,
    far_recv, near_recv, first_recv, pair_sem, out_send, out_recv, back_send, back_recv,
    swap_sem, sum_send, sum_recv,
):
    batch, length, _ = hidden_ref.shape
    width = value_ref.shape[1]
    blocks = length // BLOCK
    total_blocks = batch * blocks
    narrow = bc_in.shape[0]
    me = lax.axis_index("tp")
    ring = lax.axis_size("tp")
    place = lax.axis_index("seq")
    devices = lax.axis_size("seq")
    chips = devices // 2
    core = lax.rem(place, 2)
    chip = place // 2
    partner = place + 1 - 2 * core
    after = lax.rem(place + 1, devices)
    before = lax.rem(place + devices - 1, devices)
    half = STATE // 2
    mine = pl.ds(pl.multiple_of(core * half, half), half)
    theirs_at = pl.ds(pl.multiple_of(half - core * half, half), half)

    across = SIDE
    along = chips // SIDE

    def chip_at(move):
        dy, dx = move
        return (
            lax.rem(chip // across + dy, along) * across
            + lax.rem(lax.rem(chip, across) + dx, across)
        )

    def hops(away, count):
        return min(away, count - away)

    moves = sorted(
        [(dy, dx) for dy in range(along) for dx in range(across) if dy or dx],
        key=lambda move: -(hops(move[0], along) + hops(move[1], across)),
    )
    turns = sorted(range(1, lax.axis_size("tp")), key=lambda away: -hops(away, lax.axis_size("tp")))

    def wait_bytes(ref, count, semaphore):
        part = ref.at[pl.ds(0, count)]
        pltpu.make_async_copy(part, part, semaphore).wait()

    def tp_at(away):
        return lax.rem(me + away, ring)

    def remote(source, target, send, recv, **device):
        return pltpu.make_async_remote_copy(
            src_ref=source, dst_ref=target, send_sem=send, recv_sem=recv,
            device_id=device, device_id_type=MESH,
        )

    little = [
        pltpu.make_async_copy(source, target, small_sem.at[i])
        for i, (source, target) in enumerate((
            (bc_in, small_ref.at[pl.ds(narrow, narrow)]), (step_in, step_cols),
            (bc_conv_in, bc_taps), (bias_in, bias_small), (rate_in, rate_small),
            (conv_in, conv_ref), (gain_in, gain_ref),
        ))
    ]
    for load in little:
        load.start()
    chunk = length // 2
    loads = []
    for b in range(batch):
        for part in range(2):
            loads.append(pltpu.make_async_copy(
                hidden_ref.at[b, pl.ds(part * chunk, chunk)],
                rows.at[b, pl.ds(PAD + part * chunk, chunk)], load_sem.at[2 * b + part],
            ))
    body = width - LANES
    gate_load = pltpu.make_async_copy(
        gate_ref, weights.at[:, pl.ds(body, width)], load_sem.at[2 * batch]
    )
    value_load = pltpu.make_async_copy(
        value_ref.at[:, pl.ds(0, body)], weights.at[:, pl.ds(0, body)],
        load_sem.at[2 * batch + 1],
    )
    tail_load = pltpu.make_async_copy(
        value_ref.at[:, pl.ds(body, LANES)], first_weights.at[:, pl.ds(LANES, LANES)],
        load_sem.at[2 * batch + 2],
    )
    tail_load.start()
    order = [2 * b + part for part in (1, 0) for b in range(batch)]
    for i in order:
        loads[i].start()

    barrier = pltpu.get_barrier_semaphore()
    for device in (after, before, partner):
        pl.semaphore_signal(barrier, inc=1, device_id={"seq": device}, device_id_type=MESH)
    for away in GREETED:
        pl.semaphore_signal(
            barrier, inc=1, device_id={"tp": tp_at(away)}, device_id_type=MESH
        )
    def greet(semaphore):
        for move in ((0, 1), (0, across - 1), (1, 0), (along - 1, 0)):
            pl.semaphore_signal(
                semaphore, inc=1, device_id={"seq": 2 * chip_at(move) + core},
                device_id_type=MESH,
            )

    greet(barrier)

    def greet_round(index):
        if index > 0:
            pl.semaphore_wait(greet_sem.at[index - 1], 4)
        if index < across // 2 + along // 2 - 1:
            greet(greet_sem.at[index])

    for b in range(batch):
        rows[b, 0:HALO, :] = jnp.zeros((HALO, rows.shape[2]), BF16)
        small_pre[b, 0 : LANES - HALO, :] = jnp.zeros((LANES - HALO, LANES), F32)
    heads = step_cols.shape[0]
    small_ref[0:narrow, :] = jnp.zeros((narrow, small_ref.shape[1]), BF16)
    small_ref[2 * narrow :, :] = jnp.zeros((LANES - 2 * narrow, small_ref.shape[1]), BF16)
    bias_ref[...] = jnp.zeros_like(bias_ref)
    rate_ref[...] = jnp.zeros_like(rate_ref)
    bc_square[...] = jnp.zeros_like(bc_square)
    lane = lax.broadcasted_iota(jnp.int32, expand_ref.shape, 1) // HEAD_DIM
    owner = lax.rem(lax.broadcasted_iota(jnp.int32, expand_ref.shape, 0), LANES)
    expand_ref[...] = jnp.where(lane == owner, 1.0, 0.0).astype(BF16)
    for load in little[:2]:
        load.wait()
    small_ref[0:heads, :] = step_cols[...]

    for at in range(0, small_ref.shape[1], LANES):
        first_weights[at : at + LANES, :LANES] = jnp.transpose(small_ref[:, at : at + LANES])

    tail_load.wait()

    def first_tile(part):
        start = part * chunk
        for b in range(batch):
            product = jnp.dot(
                rows[b, PAD + start : PAD + start + chunk, :], first_weights[...],
                preferred_element_type=F32,
            )
            small_pre[b, LANES + start : LANES + start + chunk, :] = product[:, :LANES]
            pre[b, PAD + start : PAD + start + chunk, body:] = (
                product[:, LANES:].astype(BF16).astype(F32)
            )

    for b in range(batch):
        loads[2 * b + 1].wait()
    halo = remote(
        rows.at[:, pl.ds(PAD + length - HALO, HALO)], rows.at[:, pl.ds(PAD - HALO, HALO)],
        halo_sem.at[0], halo_sem.at[1], seq=after,
    )

    small_halo = remote(
        small_pre.at[:, pl.ds(LANES + length - HALO, HALO)],
        small_pre.at[:, pl.ds(LANES - HALO, HALO)],
        halo_sem.at[2], halo_sem.at[3], seq=after,
    )
    tail_halo = remote(
        pre.at[:, pl.ds(PAD + length - HALO, HALO), pl.ds(body, LANES)],
        pre.at[:, pl.ds(PAD - HALO, HALO), pl.ds(body, LANES)],
        halo_sem.at[4], halo_sem.at[5], seq=after,
    )

    def send_halo(copies, now=True):
        @pl.when(jnp.logical_and(place < devices - 1, now))
        def _():
            for copy in copies:
                copy.start()

    def wait_halo(copy):
        @pl.when(place < devices - 1)
        def _():
            copy.wait_send()

        @pl.when(place > 0)
        def _():
            copy.wait_recv()

    def enter(now, copies):
        @pl.when(now)
        def _():
            pl.semaphore_wait(barrier, 7 + len(GREETED))
            send_halo(copies)

    enter(me >= ring // 2, [halo])
    first_tile(1)
    send_halo([small_halo, tail_halo], me >= ring // 2)
    value_load.start()
    for b in range(batch):
        loads[2 * b].wait()
    first_tile(0)
    enter(me == ring // 2 - 1, [small_halo, tail_halo, halo])
    for load in little[2:]:
        load.wait()
    bias_ref[:, 0:heads] = bias_small[...]
    rate_ref[:, 0:heads] = jnp.exp(rate_small[...])
    for part in range(2):
        cut = slice(part * LANES, (part + 1) * LANES)
        bc_square[0:CONV, :] = bc_taps[:, cut]
        bc_conv_ref[cut, :] = jnp.transpose(bc_square[...])
    taps = bc_conv_ref[pl.ds(pl.multiple_of(me * narrow, narrow), narrow), :]

    def bc_conv(x):
        total = taps[:, CONV - 1 : CONV] * x
        for k in range(1, CONV):
            total = total + taps[:, CONV - 1 - k : CONV - k] * pltpu.roll(x, k, 1)
        return silu(total).astype(BF16)

    def transpose_bc(b, piece):
        at = slice(piece * LANES, (piece + 1) * LANES)
        flipped = jnp.transpose(small_pre[b, at, :])[narrow : 2 * narrow, :]
        bc_wide[b, :, at] = flipped.astype(BF16).astype(F32)

    chunks = (
        (far, far_recv, blocks // 2, blocks),
        (near, near_recv, 1, blocks // 2),
        (first_slots, first_recv, 0, 1),
    )
    b_way = jnp.where(jnp.logical_and(me >= 2, me < 2 + ring // 2), 1, -1)

    def convolve(which):
        slots, _, low, high = chunks[which]
        size = (high - low) * BLOCK
        for b in range(batch):
            done = bc_conv(bc_wide[b, :, low * LANES : (high + 1) * LANES])
            slots[me, :, b * size : (b + 1) * size] = done[:, LANES:]

    def ring_copy(which, source, target):
        slots, recv = chunks[which][:2]
        return remote(
            slots.at[source], slots.at[source], ring_send.at[which], recv.at[source], tp=target
        )

    def ring_own(which, steps):
        for away in (steps, ring - steps):
            ring_copy(which, me, tp_at(away)).start()

    def ring_relay(which, way):
        source = tp_at(ring - 2 * way)
        ring_copy(which, source, tp_at(1)).wait_recv()

        last_way = jnp.where(lax.rem(source, 2) == 0, 1, -1)

        @pl.when(way == last_way)
        def _():
            ring_copy(which, source, tp_at(ring + 2 * way)).start()

        ring_copy(which, source, tp_at(ring + way)).start()

    def ring_finish(which, first, way):
        passed = tp_at(ring - 2 * way)
        for source in range(first, first + ring // 2):
            @pl.when(jnp.logical_and(me != source, passed != source))
            def _():
                ring_copy(which, source, tp_at(1)).wait_recv()

    def ring_sent(which):
        wait_bytes(chunks[which][0], ring - 1, ring_send.at[which])

    for b in range(batch):
        for piece in range(1, 1 + length // LANES):
            transpose_bc(b, piece)
    for which in range(2):
        convolve(which)
    enter(me < ring // 2 - 1, [small_halo, tail_halo, halo])
    greet_round(0)
    for which in range(2):
        ring_own(which, 2)

    row = lax.broadcasted_iota(jnp.int32, (BLOCK, BLOCK), 0)
    col = lax.broadcasted_iota(jnp.int32, (BLOCK, BLOCK), 1)
    triangle = jnp.where(row >= col, 1.0, 0.0).astype(BF16)
    triangle = jnp.concatenate([triangle] * 3, axis=1)
    ms, mos, totals = [], [], []
    for b in range(batch):
        offset = jnp.zeros((1, LANES), F32)
        for k in range(blocks):
            step_pre = small_pre[b, LANES + k * BLOCK : LANES + (k + 1) * BLOCK, :] + bias_ref[...]
            steps = jnp.maximum(step_pre, 0.0) + jnp.log1p(jnp.exp(-jnp.abs(step_pre)))
            cumulative = jnp.dot(
                triangle, thirds(-steps * rate_ref[...]), preferred_element_type=F32
            )
            last = cumulative[BLOCK - 1 : BLOCK, :]
            mid = 0.5 * last
            fin[b * blocks + k] = halves(jnp.exp(mid - cumulative) * steps)
            fout[b * blocks + k] = halves(jnp.exp(cumulative - mid))
            ms.append(mid)
            mos.append(mid + offset)
            offset = offset + last
        totals.append(offset)
    table = jnp.exp(jnp.concatenate(ms + mos, axis=0))
    ends[...] = jnp.dot(halves(table), expand_ref[...], preferred_element_type=F32)
    logs[...] = jnp.concatenate(totals + [jnp.zeros((8 - batch, LANES), F32)], axis=0)
    pair_log = remote(logs, pair_logs, log_sem.at[0], log_sem.at[1], seq=partner)
    pair_log.start()

    wait_halo(small_halo)

    @pl.when(place == 0)
    def _():
        for b in range(batch):
            rows[b, 0:PAD, :] = jnp.zeros((PAD, rows.shape[2]), BF16)
            small_pre[b, LANES - HALO : LANES, :] = jnp.zeros((HALO, LANES), F32)
            pre[b, PAD - HALO : PAD, body:] = jnp.zeros((HALO, LANES), F32)

    for b in range(batch):
        transpose_bc(b, 0)
    convolve(2)
    ring_own(2, 2)
    for which in range(3):
        ring_own(which, 1)
    greet_round(1)

    def gate_part(b, product):
        return silu(product.astype(BF16).astype(F32))

    def tile_of(start, size):
        cut = slice(start, start + size)
        for b in range(batch):
            if start >= body:
                product = jnp.dot(
                    rows[b, PAD : PAD + length, :], weights[:, cut], preferred_element_type=F32
                )
                gates[b, :, start - body : start - body + size] = gate_part(b, product)
            else:
                product = jnp.dot(rows[b], weights[:, cut], preferred_element_type=F32)
                pre[b, :, cut] = product.astype(BF16).astype(F32)

    value_tiles = [(at, TILE) for at in range(0, body, TILE)]
    gate_tiles = [
        (at, min(TILE, body + width - at)) for at in range(body, body + width, TILE)
    ]
    gate_load.start()
    value_load.wait()
    wait_halo(halo)
    tile_of(*value_tiles[0])
    wait_halo(tail_halo)


    def values_of(g, low, high):
        b, k = divmod(g, blocks)
        base = PAD + k * BLOCK - HALO
        wide = jnp.dot(fin[g], expand_ref[:, low:high], preferred_element_type=F32)
        for start in range(low, high, LANES):
            cut = slice(start, start + LANES)
            window = pre[b, base : base + HALO + BLOCK, cut]
            x = conv_ref[0:1, cut] * window
            for tap in range(1, CONV):
                x = pltpu.roll(x, 1, 0) + conv_ref[tap : tap + 1, cut] * window
            right[g, STATE:, cut] = (
                silu(x[HALO:]) * wide[:, start - low : start - low + LANES]
            ).astype(BF16)

    for which in range(2):
        ring_relay(which, b_way)
    greet_round(2)
    for g in range(total_blocks):
        values_of(g, 0, TILE)
        values_of(g, body, width)
        if g == total_blocks // 2 - 1:
            ring_relay(2, b_way)
    for start, size in value_tiles[1:]:
        tile_of(start, size)
    for g in range(total_blocks):
        values_of(g, TILE, body)
    greet_round(3)
    pair_log.wait()
    chip_logs[...] = logs[...] + pair_logs[...]
    all_logs[chip] = logs[...] + pair_logs[...]
    for move in moves:
        remote(
            chip_logs, all_logs.at[chip], log_send.at[0], log_recv.at[0],
            seq=2 * chip_at(move) + core,
        ).start()
    for which in range(3):
        ring_finish(which, 0, b_way)

    def bc_block(b, k, first):
        slots, _, low, high = next(c for c in chunks if c[2] <= k < c[3])
        at = (b * (high - low) + k - low) * BLOCK
        return slots[first : first + ring // 2, :, at : at + BLOCK].reshape(STATE, BLOCK)

    for b in range(batch):
        held = jnp.zeros((STATE, width), F32)
        for k in range(blocks):
            g = b * blocks + k
            e = ends[g : g + 1, :]
            ahead = e * held
            right[g, :STATE, :] = ahead.astype(BF16)
            added = jnp.dot(
                bc_block(b, k, 0), right[g, STATE:, :], preferred_element_type=F32
            )
            held = e * (ahead + added)
        local[b] = held.astype(BF16)

    def pair_copy(at, index):
        return remote(
            local.at[:, at], pair.at[:, at], pair_sem.at[index], pair_sem.at[index + 1],
            seq=partner,
        )

    pair_copy(theirs_at, 0).start()
    pair_copy(mine, 2).start()
    for which in range(3):
        ring_relay(which, -b_way)
    own_end = jnp.exp(logs[...])
    pair_end = jnp.exp(pair_logs[...])
    wide_ends = jnp.dot(
        halves(jnp.concatenate([own_end, pair_end], axis=0)), expand_ref[...],
        preferred_element_type=F32,
    )
    pair_copy(theirs_at, 0).wait()
    groups = chips // batch
    for b in range(batch):
        own = local[b, mine, :].astype(F32)
        theirs = pair[b, mine, :].astype(F32)
        first = jnp.where(core == 0, own, theirs)
        second = jnp.where(core == 0, theirs, own)
        later = jnp.where(core == 0, wide_ends[8 + b : 9 + b, :], wide_ends[b : b + 1, :])
        both = (later * first + second).reshape(groups, half // groups, width)
        sent[b * groups : (b + 1) * groups] = both.astype(BF16)
    got[chip] = sent[chip]
    for move in moves:
        peer = chip_at(move)
        remote(
            sent.at[peer], got.at[chip], out_send.at[0], out_recv.at[0], seq=2 * peer + core
        ).start()
    gate_load.wait()
    for start, size in gate_tiles[:2]:
        tile_of(start, size)

    wait_bytes(all_logs, chips - 1, log_send.at[0])
    wait_bytes(all_logs, chips - 1, log_recv.at[0])
    low = chip < chips // batch
    spans = jnp.concatenate(
        [jnp.where(low, all_logs[i, 0:1, :], all_logs[i, 1:2, :]) for i in range(chips)], axis=0
    )
    spans = jnp.dot(halves(jnp.exp(spans)), expand_ref[...], preferred_element_type=F32)
    wait_bytes(got, chips - 1, out_send.at[0])
    wait_bytes(got, chips - 1, out_recv.at[0])
    running = jnp.zeros((half // groups, width), F32)
    for i in range(chips):
        prefix[i] = running.astype(BF16)
        if i + 1 < chips:
            running = spans[i : i + 1, :] * running + got[i].astype(F32)
    owned[chip] = prefix[chip]
    for move in moves:
        peer = chip_at(move)
        remote(
            prefix.at[peer], owned.at[chip], back_send.at[0], back_recv.at[0],
            seq=2 * peer + core,
        ).start()

    for start, size in gate_tiles[2:]:
        tile_of(start, size)
    for which in range(3):
        ring_finish(which, ring // 2, -b_way)
    for g in range(total_blocks):
        b, k = divmod(g, blocks)
        b_flat = bc_block(b, k, 0)
        c_rows = jnp.transpose(bc_block(b, k, ring // 2).astype(F32)).astype(BF16)
        scores = jnp.dot(c_rows, b_flat, preferred_element_type=F32)
        left[g, :, :STATE] = c_rows
        left[g, :, STATE:] = jnp.where(row >= col, scores, 0.0).astype(BF16)
    for g in range(total_blocks):
        b, k = divmod(g, blocks)
        at = slice(k * BLOCK, (k + 1) * BLOCK)
        wide = jnp.dot(fout[g], expand_ref[...], preferred_element_type=F32)
        y = jnp.dot(left[g], right[g], preferred_element_type=F32)
        weighted = wide * gates[b, at, :]
        gated_ref[b, at, :] = y * weighted
        other[b, at, :] = weighted * ends[total_blocks + g : total_blocks + g + 1, :]
    for which in range(3):
        ring_sent(which)
    wait_bytes(owned, chips - 1, back_send.at[0])
    wait_bytes(owned, chips - 1, back_recv.at[0])
    swap = remote(owned, owned_pair, swap_sem.at[0], swap_sem.at[1], seq=partner)
    swap.start()
    pair_copy(mine, 2).wait()
    swap.wait()

    for b in range(batch):
        at = slice(b * groups, (b + 1) * groups)
        own = owned[at].astype(F32).reshape(half, width)
        theirs = owned_pair[at].astype(F32).reshape(half, width)
        span = wide_ends[8 + b : 9 + b, :]
        for c in range(2):
            cut = slice(c * half, (c + 1) * half)
            full = jnp.where(core == c, own, theirs)
            moved = span * full + pair[b, cut, :].astype(F32)
            entering[b, cut, :] = jnp.where(core == 0, full, moved).astype(BF16)

    for b in range(batch):
        for k in range(blocks):
            g = b * blocks + k
            at = slice(k * BLOCK, (k + 1) * BLOCK)
            extra = jnp.dot(left[g, :, :STATE], entering[b], preferred_element_type=F32)
            total = jnp.zeros((BLOCK, LANES), F32)
            for start in range(0, width, LANES):
                cut = slice(start, start + LANES)
                gated = gated_ref[b, at, cut] + other[b, at, cut] * extra[:, cut]
                gated_ref[b, at, cut] = gated * gain_ref[start // LANES : start // LANES + 1, :]
                total = total + gated * gated
            sums[g : g + 1, :] = jnp.sum(jnp.transpose(total), axis=0, keepdims=True)

    for away in turns:
        remote(sums, others.at[me], sum_send.at[0], sum_recv.at[0], tp=tp_at(away)).start()
    others[me] = sums[...]
    wait_bytes(others, ring - 1, sum_send.at[0])
    wait_bytes(others, ring - 1, sum_recv.at[0])
    whole_sq = others[0]
    for k in range(1, ring):
        whole_sq = whole_sq + others[k]
    scale_ref[...] = lax.rsqrt(whole_sq / DI + epsilon)


def norm_kernel(gated_ref, scale_ref, out_ref, done, sems):
    batch, length, width = gated_ref.shape
    copies = []
    for b in range(batch):
        for k in range(length // BLOCK):
            g = b * (length // BLOCK) + k
            at = slice(k * BLOCK, (k + 1) * BLOCK)
            column = jnp.transpose(jnp.broadcast_to(scale_ref[g : g + 1, :], (BLOCK, LANES)))
            for start in range(0, width, LANES):
                cut = slice(start, start + LANES)
                done[b, at, cut] = (gated_ref[b, at, cut] * column).astype(BF16)
            copies.append(pltpu.make_async_copy(
                done.at[b, pl.ds(k * BLOCK, BLOCK)], out_ref.at[b, pl.ds(k * BLOCK, BLOCK)],
                sems.at[g],
            ))
            copies[-1].start()
    for copy in copies:
        copy.wait()


def per_device(
    hidden_in, gate_proj, value_proj, bc_proj, step_proj,
    value_conv, bc_conv, step_bias, log_rate, norm_gain,
):
    batch, length, model_width = hidden_in.shape
    heads = step_proj.shape[1]
    width = value_proj.shape[1]
    narrow = bc_proj.shape[1]
    blocks = length // BLOCK
    tp = lax.axis_size("tp")
    chips = lax.axis_size("seq") // 2
    total_blocks = batch * blocks
    half = STATE // 2
    groups = chips // batch

    hbm = pl.BlockSpec(memory_space=pltpu.HBM)
    vmem = pl.BlockSpec(memory_space=pltpu.VMEM)
    dma = pltpu.SemaphoreType.DMA
    gated, scale = pl.pallas_call(
        mixer_kernel,
        out_shape=(
            jax.ShapeDtypeStruct((batch, length, width), F32),
            jax.ShapeDtypeStruct((total_blocks, LANES), F32),
        ),
        in_specs=[hbm] * 10,
        out_specs=[vmem, vmem],
        scratch_shapes=[
            pltpu.VMEM((LANES, model_width), BF16),
            pltpu.VMEM((model_width, 2 * LANES), BF16),
            pltpu.VMEM((heads, model_width), BF16),
            pltpu.VMEM((CONV, width), F32),
            pltpu.VMEM((CONV, 2 * STATE), F32),
            pltpu.VMEM((LANES, LANES), F32),
            pltpu.VMEM((2 * STATE, LANES), F32),
            pltpu.VMEM((1, heads), F32),
            pltpu.VMEM((1, heads), F32),
            pltpu.VMEM((1, LANES), F32),
            pltpu.VMEM((1, LANES), F32),
            pltpu.VMEM((width // LANES, LANES), F32),
            pltpu.VMEM((2 * LANES, width), BF16),
            pltpu.VMEM((batch, PAD + length, model_width), BF16),
            pltpu.VMEM((model_width, 2 * width - LANES), BF16),
            pltpu.VMEM((batch, LANES + length, LANES), F32),
            pltpu.VMEM((batch, narrow, LANES + length), F32),
            pltpu.VMEM((total_blocks, BLOCK, 2 * LANES), BF16),
            pltpu.VMEM((total_blocks, BLOCK, 2 * LANES), BF16),
            pltpu.VMEM((2 * total_blocks, width), F32),
            pltpu.VMEM((8, LANES), F32),
            pltpu.VMEM((8, LANES), F32),
            pltpu.VMEM((8, LANES), F32),
            pltpu.VMEM((chips, 8, LANES), F32),
            pltpu.VMEM((tp, narrow, batch * (blocks - blocks // 2) * BLOCK), BF16),
            pltpu.VMEM((tp, narrow, batch * (blocks // 2 - 1) * BLOCK), BF16),
            pltpu.VMEM((tp, narrow, batch * BLOCK), BF16),
            pltpu.VMEM((batch, PAD + length, width), F32),
            pltpu.VMEM((batch, length, width), F32),
            pltpu.VMEM((total_blocks, BLOCK, STATE + BLOCK), BF16),
            pltpu.VMEM((total_blocks, STATE + BLOCK, width), BF16),
            pltpu.VMEM((batch, length, width), F32),
            pltpu.VMEM((batch, STATE, width), BF16),
            pltpu.VMEM((batch, STATE, width), BF16),
            pltpu.VMEM((chips, half // groups, width), BF16),
            pltpu.VMEM((chips, half // groups, width), BF16),
            pltpu.VMEM((chips, half // groups, width), BF16),
            pltpu.VMEM((chips, half // groups, width), BF16),
            pltpu.VMEM((chips, half // groups, width), BF16),
            pltpu.VMEM((batch, STATE, width), BF16),
            pltpu.VMEM((total_blocks, LANES), F32),
            pltpu.VMEM((tp, total_blocks, LANES), F32),
            pltpu.SemaphoreType.REGULAR((SIDE // 2 + chips // SIDE // 2 - 1,)),
            dma((2 * batch + 3,)),
            dma((7,)),
            dma((6,)),
            dma((2,)),
            dma((1,)),
            dma((1,)),
            dma((3,)),
            dma((tp,)),
            dma((tp,)),
            dma((tp,)),
            dma((4,)),
            dma((1,)),
            dma((1,)),
            dma((1,)),
            dma((1,)),
            dma((2,)),
            dma((1,)),
            dma((1,)),
        ],
        compiler_params=pltpu.CompilerParams(
            vmem_limit_bytes=48 << 20, collective_id=0, has_side_effects=True
        ),
        name="mixer",
    )(*(pltpu.with_memory_space_constraint(x, pltpu.HBM) for x in (
        hidden_in, value_proj, gate_proj, bc_proj.T, step_proj.T, value_conv, bc_conv,
        step_bias.reshape(1, heads), log_rate.reshape(1, heads),
        norm_gain.reshape(width // LANES, LANES),
    )))

    return pl.pallas_call(
        norm_kernel,
        out_shape=jax.ShapeDtypeStruct((batch, length, width), BF16),
        in_specs=[vmem, vmem],
        out_specs=hbm,
        scratch_shapes=[pltpu.VMEM((batch, length, width), BF16), dma((total_blocks,))],
        compiler_params=pltpu.CompilerParams(vmem_limit_bytes=8 << 20),
        name="norm",
    )(gated, scale)


def solution(mesh):
    return jax.shard_map(
        per_device,
        mesh=mesh,
        in_specs=(
            P(None, "seq", None),
            P(None, "tp"),
            P(None, "tp"),
            P(None, "tp"),
            P(None, "tp"),
            P(None, "tp"),
            P(),
            P("tp"),
            P("tp"),
            P("tp"),
        ),
        out_specs=P(None, "seq", "tp"),
        check_vma=False,
    )
```

```python
import jax
import jax.numpy as jnp
from jax import lax
from jax.experimental import pallas as pl
from jax.experimental.pallas import tpu as pltpu
from jax.sharding import PartitionSpec as P

DI = 5120
HEAD_DIM = 64
STATE = 128
CONV = 4
BLOCK = 128
LANES = 128
PAD = 16
HALO = 8
TILE = 256
SIDE = 4
GREETED = (1, 2, 6, 7)
MESH = pl.DeviceIdType.MESH

epsilon = 1e-05
F32 = jnp.float32
BF16 = jnp.bfloat16


def silu(x):
    halved = 0.5 * x
    return halved + halved * jnp.tanh(halved)


def halves(x):
    high = x.astype(BF16)
    low = (x - high.astype(F32)).astype(BF16)
    return jnp.concatenate([high, low], axis=1)


def thirds(x):
    terms = []
    for _ in range(3):
        terms.append(x.astype(BF16))
        x = x - terms[-1].astype(F32)
    return jnp.concatenate(terms, axis=0)


def mixer_kernel(
    hidden_ref, value_ref, gate_ref, bc_in, step_in, conv_in, bc_conv_in,
    bias_in, rate_in, gain_in,
    gated_ref, scale_ref,
    small_ref, first_weights, step_cols, conv_ref, bc_taps, bc_square, bc_conv_ref,
    bias_small, rate_small, bias_ref, rate_ref, gain_ref, expand_ref, rows, weights, small_pre, bc_wide, fin, fout, ends, logs, pair_logs, chip_logs,
    all_logs, far, near, first_slots, pre, gates, left, right, other,
    local, pair, sent, got, prefix, owned, owned_pair, entering, sums, others,
    greet_sem, load_sem, small_sem, halo_sem, log_sem, log_send, log_recv, ring_send,
    far_recv, near_recv, first_recv, pair_sem, out_send, out_recv, back_send, back_recv,
    swap_sem, sum_send, sum_recv,
):
    batch, length, _ = hidden_ref.shape
    width = value_ref.shape[1]
    blocks = length // BLOCK
    total_blocks = batch * blocks
    narrow = bc_in.shape[0]
    me = lax.axis_index("tp")
    ring = lax.axis_size("tp")
    place = lax.axis_index("seq")
    devices = lax.axis_size("seq")
    chips = devices // 2
    core = lax.rem(place, 2)
    chip = place // 2
    partner = place + 1 - 2 * core
    after = lax.rem(place + 1, devices)
    before = lax.rem(place + devices - 1, devices)
    half = STATE // 2
    mine = pl.ds(pl.multiple_of(core * half, half), half)
    theirs_at = pl.ds(pl.multiple_of(half - core * half, half), half)

    across = SIDE
    along = chips // SIDE

    def chip_at(move):
        dy, dx = move
        return (
            lax.rem(chip // across + dy, along) * across
            + lax.rem(lax.rem(chip, across) + dx, across)
        )

    def hops(away, count):
        return min(away, count - away)

    moves = sorted(
        [(dy, dx) for dy in range(along) for dx in range(across) if dy or dx],
        key=lambda move: -(hops(move[0], along) + hops(move[1], across)),
    )
    turns = sorted(range(1, lax.axis_size("tp")), key=lambda away: -hops(away, lax.axis_size("tp")))

    def wait_bytes(ref, count, semaphore):
        part = ref.at[pl.ds(0, count)]
        pltpu.make_async_copy(part, part, semaphore).wait()

    def tp_at(away):
        return lax.rem(me + away, ring)

    def remote(source, target, send, recv, **device):
        return pltpu.make_async_remote_copy(
            src_ref=source, dst_ref=target, send_sem=send, recv_sem=recv,
            device_id=device, device_id_type=MESH,
        )

    little = [
        pltpu.make_async_copy(source, target, small_sem.at[i])
        for i, (source, target) in enumerate((
            (bc_in, small_ref.at[pl.ds(narrow, narrow)]), (step_in, step_cols),
            (bc_conv_in, bc_taps), (bias_in, bias_small), (rate_in, rate_small),
            (conv_in, conv_ref), (gain_in, gain_ref),
        ))
    ]
    for load in little:
        load.start()
    chunk = length // 2
    loads = []
    for b in range(batch):
        for part in range(2):
            loads.append(pltpu.make_async_copy(
                hidden_ref.at[b, pl.ds(part * chunk, chunk)],
                rows.at[b, pl.ds(PAD + part * chunk, chunk)], load_sem.at[2 * b + part],
            ))
    body = width - LANES
    gate_load = pltpu.make_async_copy(
        gate_ref, weights.at[:, pl.ds(body, width)], load_sem.at[2 * batch]
    )
    value_load = pltpu.make_async_copy(
        value_ref.at[:, pl.ds(0, body)], weights.at[:, pl.ds(0, body)],
        load_sem.at[2 * batch + 1],
    )
    tail_load = pltpu.make_async_copy(
        value_ref.at[:, pl.ds(body, LANES)], first_weights.at[:, pl.ds(LANES, LANES)],
        load_sem.at[2 * batch + 2],
    )
    tail_load.start()
    order = [2 * b + part for part in (1, 0) for b in range(batch)]
    for i in order:
        loads[i].start()

    barrier = pltpu.get_barrier_semaphore()
    for device in (after, before, partner):
        pl.semaphore_signal(barrier, inc=1, device_id={"seq": device}, device_id_type=MESH)
    for away in GREETED:
        pl.semaphore_signal(
            barrier, inc=1, device_id={"tp": tp_at(away)}, device_id_type=MESH
        )
    def greet(semaphore):
        for move in ((0, 1), (0, across - 1), (1, 0), (along - 1, 0)):
            pl.semaphore_signal(
                semaphore, inc=1, device_id={"seq": 2 * chip_at(move) + core},
                device_id_type=MESH,
            )

    greet(barrier)

    def greet_round(index):
        if index > 0:
            pl.semaphore_wait(greet_sem.at[index - 1], 4)
        if index < across // 2 + along // 2 - 1:
            greet(greet_sem.at[index])

    for b in range(batch):
        rows[b, 0:HALO, :] = jnp.zeros((HALO, rows.shape[2]), BF16)
        small_pre[b, 0 : LANES - HALO, :] = jnp.zeros((LANES - HALO, LANES), F32)
    heads = step_cols.shape[0]
    small_ref[0:narrow, :] = jnp.zeros((narrow, small_ref.shape[1]), BF16)
    small_ref[2 * narrow :, :] = jnp.zeros((LANES - 2 * narrow, small_ref.shape[1]), BF16)
    bias_ref[...] = jnp.zeros_like(bias_ref)
    rate_ref[...] = jnp.zeros_like(rate_ref)
    bc_square[...] = jnp.zeros_like(bc_square)
    lane = lax.broadcasted_iota(jnp.int32, expand_ref.shape, 1) // HEAD_DIM
    owner = lax.rem(lax.broadcasted_iota(jnp.int32, expand_ref.shape, 0), LANES)
    expand_ref[...] = jnp.where(lane == owner, 1.0, 0.0).astype(BF16)
    for load in little[:2]:
        load.wait()
    small_ref[0:heads, :] = step_cols[...]

    for at in range(0, small_ref.shape[1], LANES):
        first_weights[at : at + LANES, :LANES] = jnp.transpose(small_ref[:, at : at + LANES])

    tail_load.wait()

    def first_tile(part):
        start = part * chunk
        for b in range(batch):
            product = jnp.dot(
                rows[b, PAD + start : PAD + start + chunk, :], first_weights[...],
                preferred_element_type=F32,
            )
            small_pre[b, LANES + start : LANES + start + chunk, :] = product[:, :LANES]
            pre[b, PAD + start : PAD + start + chunk, body:] = (
                product[:, LANES:].astype(BF16).astype(F32)
            )

    for b in range(batch):
        loads[2 * b + 1].wait()
    halo = remote(
        rows.at[:, pl.ds(PAD + length - HALO, HALO)], rows.at[:, pl.ds(PAD - HALO, HALO)],
        halo_sem.at[0], halo_sem.at[1], seq=after,
    )

    small_halo = remote(
        small_pre.at[:, pl.ds(LANES + length - HALO, HALO)],
        small_pre.at[:, pl.ds(LANES - HALO, HALO)],
        halo_sem.at[2], halo_sem.at[3], seq=after,
    )
    tail_halo = remote(
        pre.at[:, pl.ds(PAD + length - HALO, HALO), pl.ds(body, LANES)],
        pre.at[:, pl.ds(PAD - HALO, HALO), pl.ds(body, LANES)],
        halo_sem.at[4], halo_sem.at[5], seq=after,
    )

    def send_halo(copies, now=True):
        @pl.when(jnp.logical_and(place < devices - 1, now))
        def _():
            for copy in copies:
                copy.start()

    def wait_halo(copy):
        @pl.when(place < devices - 1)
        def _():
            copy.wait_send()

        @pl.when(place > 0)
        def _():
            copy.wait_recv()

    def enter(now, copies):
        @pl.when(now)
        def _():
            pl.semaphore_wait(barrier, 7 + len(GREETED))
            send_halo(copies)

    enter(me >= ring // 2, [halo])
    first_tile(1)
    send_halo([small_halo, tail_halo], me >= ring // 2)
    value_load.start()
    for b in range(batch):
        loads[2 * b].wait()
    first_tile(0)
    enter(me == ring // 2 - 1, [small_halo, tail_halo, halo])
    for load in little[2:]:
        load.wait()
    bias_ref[:, 0:heads] = bias_small[...]
    rate_ref[:, 0:heads] = jnp.exp(rate_small[...])
    for part in range(2):
        cut = slice(part * LANES, (part + 1) * LANES)
        bc_square[0:CONV, :] = bc_taps[:, cut]
        bc_conv_ref[cut, :] = jnp.transpose(bc_square[...])
    taps = bc_conv_ref[pl.ds(pl.multiple_of(me * narrow, narrow), narrow), :]

    def bc_conv(x):
        total = taps[:, CONV - 1 : CONV] * x
        for k in range(1, CONV):
            total = total + taps[:, CONV - 1 - k : CONV - k] * pltpu.roll(x, k, 1)
        return silu(total).astype(BF16)

    def transpose_bc(b, piece):
        at = slice(piece * LANES, (piece + 1) * LANES)
        flipped = jnp.transpose(small_pre[b, at, :])[narrow : 2 * narrow, :]
        bc_wide[b, :, at] = flipped.astype(BF16).astype(F32)

    chunks = (
        (far, far_recv, blocks // 2, blocks),
        (near, near_recv, 1, blocks // 2),
        (first_slots, first_recv, 0, 1),
    )
    b_way = jnp.where(jnp.logical_and(me >= 2, me < 2 + ring // 2), 1, -1)

    def convolve(which):
        slots, _, low, high = chunks[which]
        size = (high - low) * BLOCK
        for b in range(batch):
            done = bc_conv(bc_wide[b, :, low * LANES : (high + 1) * LANES])
            slots[me, :, b * size : (b + 1) * size] = done[:, LANES:]

    def ring_copy(which, source, target):
        slots, recv = chunks[which][:2]
        return remote(
            slots.at[source], slots.at[source], ring_send.at[which], recv.at[source], tp=target
        )

    def ring_own(which, steps):
        for away in (steps, ring - steps):
            ring_copy(which, me, tp_at(away)).start()

    def ring_relay(which, way):
        source = tp_at(ring - 2 * way)
        ring_copy(which, source, tp_at(1)).wait_recv()

        if chunks[which][2] == 0:
            clockwise = lax.rem(source, ring // 2) < ring // 4
        else:
            clockwise = lax.rem(source, 2) == 0
        last_way = jnp.where(clockwise, 1, -1)

        @pl.when(way == last_way)
        def _():
            ring_copy(which, source, tp_at(ring + 2 * way)).start()

        ring_copy(which, source, tp_at(ring + way)).start()

    def ring_finish(which, first, way):
        passed = tp_at(ring - 2 * way)
        for source in range(first, first + ring // 2):
            @pl.when(jnp.logical_and(me != source, passed != source))
            def _():
                ring_copy(which, source, tp_at(1)).wait_recv()

    def ring_sent(which):
        wait_bytes(chunks[which][0], ring - 1, ring_send.at[which])

    for b in range(batch):
        for piece in range(1, 1 + length // LANES):
            transpose_bc(b, piece)
    for which in range(2):
        convolve(which)
    enter(me < ring // 2 - 1, [small_halo, tail_halo, halo])
    greet_round(0)
    for which in range(2):
        ring_own(which, 2)

    row = lax.broadcasted_iota(jnp.int32, (BLOCK, BLOCK), 0)
    col = lax.broadcasted_iota(jnp.int32, (BLOCK, BLOCK), 1)
    triangle = jnp.where(row >= col, 1.0, 0.0).astype(BF16)
    triangle = jnp.concatenate([triangle] * 3, axis=1)
    ms, mos, totals = [], [], []
    for b in range(batch):
        offset = jnp.zeros((1, LANES), F32)
        for k in range(blocks):
            step_pre = small_pre[b, LANES + k * BLOCK : LANES + (k + 1) * BLOCK, :] + bias_ref[...]
            steps = jnp.maximum(step_pre, 0.0) + jnp.log1p(jnp.exp(-jnp.abs(step_pre)))
            cumulative = jnp.dot(
                triangle, thirds(-steps * rate_ref[...]), preferred_element_type=F32
            )
            last = cumulative[BLOCK - 1 : BLOCK, :]
            mid = 0.5 * last
            fin[b * blocks + k] = halves(jnp.exp(mid - cumulative) * steps)
            fout[b * blocks + k] = halves(jnp.exp(cumulative - mid))
            ms.append(mid)
            mos.append(mid + offset)
            offset = offset + last
        totals.append(offset)
    table = jnp.exp(jnp.concatenate(ms + mos, axis=0))
    ends[...] = jnp.dot(halves(table), expand_ref[...], preferred_element_type=F32)
    logs[...] = jnp.concatenate(totals + [jnp.zeros((8 - batch, LANES), F32)], axis=0)
    pair_log = remote(logs, pair_logs, log_sem.at[0], log_sem.at[1], seq=partner)
    pair_log.start()

    wait_halo(small_halo)

    @pl.when(place == 0)
    def _():
        for b in range(batch):
            rows[b, 0:PAD, :] = jnp.zeros((PAD, rows.shape[2]), BF16)
            small_pre[b, LANES - HALO : LANES, :] = jnp.zeros((HALO, LANES), F32)
            pre[b, PAD - HALO : PAD, body:] = jnp.zeros((HALO, LANES), F32)

    for b in range(batch):
        transpose_bc(b, 0)
    convolve(2)
    ring_own(2, 2)
    for which in range(3):
        ring_own(which, 1)
    greet_round(1)

    def gate_part(b, product):
        return silu(product.astype(BF16).astype(F32))

    def tile_of(start, size):
        cut = slice(start, start + size)
        for b in range(batch):
            if start >= body:
                product = jnp.dot(
                    rows[b, PAD : PAD + length, :], weights[:, cut], preferred_element_type=F32
                )
                gates[b, :, start - body : start - body + size] = gate_part(b, product)
            else:
                product = jnp.dot(rows[b], weights[:, cut], preferred_element_type=F32)
                pre[b, :, cut] = product.astype(BF16).astype(F32)

    value_tiles = [(at, TILE) for at in range(0, body, TILE)]
    gate_tiles = [
        (at, min(TILE, body + width - at)) for at in range(body, body + width, TILE)
    ]
    gate_load.start()
    value_load.wait()
    wait_halo(halo)
    ring_relay(0, b_way)
    tile_of(*value_tiles[0])
    wait_halo(tail_halo)


    def values_of(g, low, high):
        b, k = divmod(g, blocks)
        base = PAD + k * BLOCK - HALO
        wide = jnp.dot(fin[g], expand_ref[:, low:high], preferred_element_type=F32)
        for start in range(low, high, LANES):
            cut = slice(start, start + LANES)
            window = pre[b, base : base + HALO + BLOCK, cut]
            x = conv_ref[0:1, cut] * window
            for tap in range(1, CONV):
                x = pltpu.roll(x, 1, 0) + conv_ref[tap : tap + 1, cut] * window
            right[g, STATE:, cut] = (
                silu(x[HALO:]) * wide[:, start - low : start - low + LANES]
            ).astype(BF16)

    ring_relay(1, b_way)
    for g in range(total_blocks):
        values_of(g, 0, TILE)
        values_of(g, body, width)
        if g == total_blocks // 2 - 1:
            ring_relay(2, b_way)
            greet_round(2)
    for start, size in value_tiles[1:]:
        tile_of(start, size)
    for g in range(total_blocks):
        values_of(g, TILE, body)
    greet_round(3)
    pair_log.wait()
    chip_logs[...] = logs[...] + pair_logs[...]
    all_logs[chip] = logs[...] + pair_logs[...]
    for move in moves:
        remote(
            chip_logs, all_logs.at[chip], log_send.at[0], log_recv.at[0],
            seq=2 * chip_at(move) + core,
        ).start()
    for which in range(3):
        ring_finish(which, 0, b_way)

    def bc_block(b, k, first):
        slots, _, low, high = next(c for c in chunks if c[2] <= k < c[3])
        at = (b * (high - low) + k - low) * BLOCK
        return slots[first : first + ring // 2, :, at : at + BLOCK].reshape(STATE, BLOCK)

    for b in range(batch):
        held = jnp.zeros((STATE, width), F32)
        for k in range(blocks):
            g = b * blocks + k
            e = ends[g : g + 1, :]
            ahead = e * held
            right[g, :STATE, :] = ahead.astype(BF16)
            added = jnp.dot(
                bc_block(b, k, 0), right[g, STATE:, :], preferred_element_type=F32
            )
            held = e * (ahead + added)
        local[b] = held.astype(BF16)

    def pair_copy(at, index):
        return remote(
            local.at[:, at], pair.at[:, at], pair_sem.at[index], pair_sem.at[index + 1],
            seq=partner,
        )

    pair_copy(theirs_at, 0).start()
    pair_copy(mine, 2).start()
    for which in range(3):
        ring_relay(which, -b_way)
    own_end = jnp.exp(logs[...])
    pair_end = jnp.exp(pair_logs[...])
    wide_ends = jnp.dot(
        halves(jnp.concatenate([own_end, pair_end], axis=0)), expand_ref[...],
        preferred_element_type=F32,
    )
    pair_copy(theirs_at, 0).wait()
    groups = chips // batch
    for b in range(batch):
        own = local[b, mine, :].astype(F32)
        theirs = pair[b, mine, :].astype(F32)
        first = jnp.where(core == 0, own, theirs)
        second = jnp.where(core == 0, theirs, own)
        later = jnp.where(core == 0, wide_ends[8 + b : 9 + b, :], wide_ends[b : b + 1, :])
        both = (later * first + second).reshape(groups, half // groups, width)
        sent[b * groups : (b + 1) * groups] = both.astype(BF16)
    got[chip] = sent[chip]
    for move in moves:
        peer = chip_at(move)
        remote(
            sent.at[peer], got.at[chip], out_send.at[0], out_recv.at[0], seq=2 * peer + core
        ).start()
    gate_load.wait()
    for start, size in gate_tiles[:2]:
        tile_of(start, size)

    wait_bytes(all_logs, chips - 1, log_send.at[0])
    wait_bytes(all_logs, chips - 1, log_recv.at[0])
    low = chip < chips // batch
    spans = jnp.concatenate(
        [jnp.where(low, all_logs[i, 0:1, :], all_logs[i, 1:2, :]) for i in range(chips)], axis=0
    )
    spans = jnp.dot(halves(jnp.exp(spans)), expand_ref[...], preferred_element_type=F32)
    wait_bytes(got, chips - 1, out_send.at[0])
    wait_bytes(got, chips - 1, out_recv.at[0])
    running = jnp.zeros((half // groups, width), F32)
    for i in range(chips):
        prefix[i] = running.astype(BF16)
        if i + 1 < chips:
            running = spans[i : i + 1, :] * running + got[i].astype(F32)
    owned[chip] = prefix[chip]
    for move in moves:
        peer = chip_at(move)
        remote(
            prefix.at[peer], owned.at[chip], back_send.at[0], back_recv.at[0],
            seq=2 * peer + core,
        ).start()

    for start, size in gate_tiles[2:]:
        tile_of(start, size)
    for which in range(3):
        ring_finish(which, ring // 2, -b_way)
    for g in range(total_blocks):
        b, k = divmod(g, blocks)
        b_flat = bc_block(b, k, 0)
        c_rows = jnp.transpose(bc_block(b, k, ring // 2).astype(F32)).astype(BF16)
        scores = jnp.dot(c_rows, b_flat, preferred_element_type=F32)
        left[g, :, :STATE] = c_rows
        left[g, :, STATE:] = jnp.where(row >= col, scores, 0.0).astype(BF16)
    for g in range(total_blocks):
        b, k = divmod(g, blocks)
        at = slice(k * BLOCK, (k + 1) * BLOCK)
        wide = jnp.dot(fout[g], expand_ref[...], preferred_element_type=F32)
        y = jnp.dot(left[g], right[g], preferred_element_type=F32)
        weighted = wide * gates[b, at, :]
        gated_ref[b, at, :] = y * weighted
        other[b, at, :] = weighted * ends[total_blocks + g : total_blocks + g + 1, :]
    for which in range(3):
        ring_sent(which)
    wait_bytes(owned, chips - 1, back_send.at[0])
    wait_bytes(owned, chips - 1, back_recv.at[0])
    swap = remote(owned, owned_pair, swap_sem.at[0], swap_sem.at[1], seq=partner)
    swap.start()
    pair_copy(mine, 2).wait()
    swap.wait()

    for b in range(batch):
        at = slice(b * groups, (b + 1) * groups)
        own = owned[at].astype(F32).reshape(half, width)
        theirs = owned_pair[at].astype(F32).reshape(half, width)
        span = wide_ends[8 + b : 9 + b, :]
        for c in range(2):
            cut = slice(c * half, (c + 1) * half)
            full = jnp.where(core == c, own, theirs)
            moved = span * full + pair[b, cut, :].astype(F32)
            entering[b, cut, :] = jnp.where(core == 0, full, moved).astype(BF16)

    for b in range(batch):
        for k in range(blocks):
            g = b * blocks + k
            at = slice(k * BLOCK, (k + 1) * BLOCK)
            extra = jnp.dot(left[g, :, :STATE], entering[b], preferred_element_type=F32)
            total = jnp.zeros((BLOCK, LANES), F32)
            for start in range(0, width, LANES):
                cut = slice(start, start + LANES)
                gated = gated_ref[b, at, cut] + other[b, at, cut] * extra[:, cut]
                gated_ref[b, at, cut] = gated * gain_ref[start // LANES : start // LANES + 1, :]
                total = total + gated * gated
            sums[g : g + 1, :] = jnp.sum(jnp.transpose(total), axis=0, keepdims=True)

    for away in turns:
        remote(sums, others.at[me], sum_send.at[0], sum_recv.at[0], tp=tp_at(away)).start()
    others[me] = sums[...]
    wait_bytes(others, ring - 1, sum_send.at[0])
    wait_bytes(others, ring - 1, sum_recv.at[0])
    whole_sq = others[0]
    for k in range(1, ring):
        whole_sq = whole_sq + others[k]
    scale_ref[...] = lax.rsqrt(whole_sq / DI + epsilon)


def norm_kernel(gated_ref, scale_ref, out_ref, done, sems):
    batch, length, width = gated_ref.shape
    copies = []
    for b in range(batch):
        for k in range(length // BLOCK):
            g = b * (length // BLOCK) + k
            at = slice(k * BLOCK, (k + 1) * BLOCK)
            column = jnp.transpose(jnp.broadcast_to(scale_ref[g : g + 1, :], (BLOCK, LANES)))
            for start in range(0, width, LANES):
                cut = slice(start, start + LANES)
                done[b, at, cut] = (gated_ref[b, at, cut] * column).astype(BF16)
            copies.append(pltpu.make_async_copy(
                done.at[b, pl.ds(k * BLOCK, BLOCK)], out_ref.at[b, pl.ds(k * BLOCK, BLOCK)],
                sems.at[g],
            ))
            copies[-1].start()
    for copy in copies:
        copy.wait()


def per_device(
    hidden_in, gate_proj, value_proj, bc_proj, step_proj,
    value_conv, bc_conv, step_bias, log_rate, norm_gain,
):
    batch, length, model_width = hidden_in.shape
    heads = step_proj.shape[1]
    width = value_proj.shape[1]
    narrow = bc_proj.shape[1]
    blocks = length // BLOCK
    tp = lax.axis_size("tp")
    chips = lax.axis_size("seq") // 2
    total_blocks = batch * blocks
    half = STATE // 2
    groups = chips // batch

    hbm = pl.BlockSpec(memory_space=pltpu.HBM)
    vmem = pl.BlockSpec(memory_space=pltpu.VMEM)
    dma = pltpu.SemaphoreType.DMA
    gated, scale = pl.pallas_call(
        mixer_kernel,
        out_shape=(
            jax.ShapeDtypeStruct((batch, length, width), F32),
            jax.ShapeDtypeStruct((total_blocks, LANES), F32),
        ),
        in_specs=[hbm] * 10,
        out_specs=[vmem, vmem],
        scratch_shapes=[
            pltpu.VMEM((LANES, model_width), BF16),
            pltpu.VMEM((model_width, 2 * LANES), BF16),
            pltpu.VMEM((heads, model_width), BF16),
            pltpu.VMEM((CONV, width), F32),
            pltpu.VMEM((CONV, 2 * STATE), F32),
            pltpu.VMEM((LANES, LANES), F32),
            pltpu.VMEM((2 * STATE, LANES), F32),
            pltpu.VMEM((1, heads), F32),
            pltpu.VMEM((1, heads), F32),
            pltpu.VMEM((1, LANES), F32),
            pltpu.VMEM((1, LANES), F32),
            pltpu.VMEM((width // LANES, LANES), F32),
            pltpu.VMEM((2 * LANES, width), BF16),
            pltpu.VMEM((batch, PAD + length, model_width), BF16),
            pltpu.VMEM((model_width, 2 * width - LANES), BF16),
            pltpu.VMEM((batch, LANES + length, LANES), F32),
            pltpu.VMEM((batch, narrow, LANES + length), F32),
            pltpu.VMEM((total_blocks, BLOCK, 2 * LANES), BF16),
            pltpu.VMEM((total_blocks, BLOCK, 2 * LANES), BF16),
            pltpu.VMEM((2 * total_blocks, width), F32),
            pltpu.VMEM((8, LANES), F32),
            pltpu.VMEM((8, LANES), F32),
            pltpu.VMEM((8, LANES), F32),
            pltpu.VMEM((chips, 8, LANES), F32),
            pltpu.VMEM((tp, narrow, batch * (blocks - blocks // 2) * BLOCK), BF16),
            pltpu.VMEM((tp, narrow, batch * (blocks // 2 - 1) * BLOCK), BF16),
            pltpu.VMEM((tp, narrow, batch * BLOCK), BF16),
            pltpu.VMEM((batch, PAD + length, width), F32),
            pltpu.VMEM((batch, length, width), F32),
            pltpu.VMEM((total_blocks, BLOCK, STATE + BLOCK), BF16),
            pltpu.VMEM((total_blocks, STATE + BLOCK, width), BF16),
            pltpu.VMEM((batch, length, width), F32),
            pltpu.VMEM((batch, STATE, width), BF16),
            pltpu.VMEM((batch, STATE, width), BF16),
            pltpu.VMEM((chips, half // groups, width), BF16),
            pltpu.VMEM((chips, half // groups, width), BF16),
            pltpu.VMEM((chips, half // groups, width), BF16),
            pltpu.VMEM((chips, half // groups, width), BF16),
            pltpu.VMEM((chips, half // groups, width), BF16),
            pltpu.VMEM((batch, STATE, width), BF16),
            pltpu.VMEM((total_blocks, LANES), F32),
            pltpu.VMEM((tp, total_blocks, LANES), F32),
            pltpu.SemaphoreType.REGULAR((SIDE // 2 + chips // SIDE // 2 - 1,)),
            dma((2 * batch + 3,)),
            dma((7,)),
            dma((6,)),
            dma((2,)),
            dma((1,)),
            dma((1,)),
            dma((3,)),
            dma((tp,)),
            dma((tp,)),
            dma((tp,)),
            dma((4,)),
            dma((1,)),
            dma((1,)),
            dma((1,)),
            dma((1,)),
            dma((2,)),
            dma((1,)),
            dma((1,)),
        ],
        compiler_params=pltpu.CompilerParams(
            vmem_limit_bytes=48 << 20, collective_id=0, has_side_effects=True
        ),
        name="mixer",
    )(*(pltpu.with_memory_space_constraint(x, pltpu.HBM) for x in (
        hidden_in, value_proj, gate_proj, bc_proj.T, step_proj.T, value_conv, bc_conv,
        step_bias.reshape(1, heads), log_rate.reshape(1, heads),
        norm_gain.reshape(width // LANES, LANES),
    )))

    return pl.pallas_call(
        norm_kernel,
        out_shape=jax.ShapeDtypeStruct((batch, length, width), BF16),
        in_specs=[vmem, vmem],
        out_specs=hbm,
        scratch_shapes=[pltpu.VMEM((batch, length, width), BF16), dma((total_blocks,))],
        compiler_params=pltpu.CompilerParams(vmem_limit_bytes=8 << 20),
        name="norm",
    )(gated, scale)


def solution(mesh):
    return jax.shard_map(
        per_device,
        mesh=mesh,
        in_specs=(
            P(None, "seq", None),
            P(None, "tp"),
            P(None, "tp"),
            P(None, "tp"),
            P(None, "tp"),
            P(None, "tp"),
            P(),
            P("tp"),
            P("tp"),
            P("tp"),
        ),
        out_specs=P(None, "seq", "tp"),
        check_vma=False,
    )
```

```python
import jax
import jax.numpy as jnp
from jax import lax
from jax.experimental import pallas as pl
from jax.experimental.pallas import tpu as pltpu
from jax.sharding import PartitionSpec as P

DI = 5120
HEAD_DIM = 64
STATE = 128
CONV = 4
BLOCK = 128
LANES = 128
PAD = 16
HALO = 8
TILE = 256
SIDE = 4
GREETED = (1, 2, 6, 7)
MESH = pl.DeviceIdType.MESH

epsilon = 1e-05
F32 = jnp.float32
BF16 = jnp.bfloat16


def silu(x):
    halved = 0.5 * x
    return halved + halved * jnp.tanh(halved)


def halves(x):
    high = x.astype(BF16)
    low = (x - high.astype(F32)).astype(BF16)
    return jnp.concatenate([high, low], axis=1)


def thirds(x):
    terms = []
    for _ in range(3):
        terms.append(x.astype(BF16))
        x = x - terms[-1].astype(F32)
    return jnp.concatenate(terms, axis=0)


def mixer_kernel(
    hidden_ref, value_ref, gate_ref, bc_in, step_in, conv_in, bc_conv_in,
    bias_in, rate_in, gain_in,
    gated_ref, scale_ref,
    small_ref, first_weights, step_cols, conv_ref, bc_taps, bc_square, bc_conv_ref,
    bias_small, rate_small, bias_ref, rate_ref, gain_ref, expand_ref, rows, weights, small_pre, bc_wide, fin, fout, ends, logs, pair_logs, chip_logs,
    all_logs, far, near, first_slots, pre, gates, left, right, other,
    local, pair, sent, got, prefix, owned, owned_pair, entering, sums, others,
    greet_sem, load_sem, small_sem, halo_sem, log_sem, log_send, log_recv, ring_send,
    far_recv, near_recv, first_recv, pair_sem, out_send, out_recv, back_send, back_recv,
    swap_sem, sum_send, sum_recv,
):
    batch, length, _ = hidden_ref.shape
    width = value_ref.shape[1]
    blocks = length // BLOCK
    total_blocks = batch * blocks
    narrow = bc_in.shape[0]
    me = lax.axis_index("tp")
    ring = lax.axis_size("tp")
    place = lax.axis_index("seq")
    devices = lax.axis_size("seq")
    chips = devices // 2
    core = lax.rem(place, 2)
    chip = place // 2
    partner = place + 1 - 2 * core
    after = lax.rem(place + 1, devices)
    before = lax.rem(place + devices - 1, devices)
    half = STATE // 2
    mine = pl.ds(pl.multiple_of(core * half, half), half)
    theirs_at = pl.ds(pl.multiple_of(half - core * half, half), half)

    across = SIDE
    along = chips // SIDE

    def chip_at(move):
        dy, dx = move
        return (
            lax.rem(chip // across + dy, along) * across
            + lax.rem(lax.rem(chip, across) + dx, across)
        )

    def hops(away, count):
        return min(away, count - away)

    moves = sorted(
        [(dy, dx) for dy in range(along) for dx in range(across) if dy or dx],
        key=lambda move: -(hops(move[0], along) + hops(move[1], across)),
    )
    turns = sorted(range(1, lax.axis_size("tp")), key=lambda away: -hops(away, lax.axis_size("tp")))

    def wait_bytes(ref, count, semaphore):
        part = ref.at[pl.ds(0, count)]
        pltpu.make_async_copy(part, part, semaphore).wait()

    def tp_at(away):
        return lax.rem(me + away, ring)

    def remote(source, target, send, recv, **device):
        return pltpu.make_async_remote_copy(
            src_ref=source, dst_ref=target, send_sem=send, recv_sem=recv,
            device_id=device, device_id_type=MESH,
        )

    little = [
        pltpu.make_async_copy(source, target, small_sem.at[i])
        for i, (source, target) in enumerate((
            (bc_in, small_ref.at[pl.ds(narrow, narrow)]), (step_in, step_cols),
            (bc_conv_in, bc_taps), (bias_in, bias_small), (rate_in, rate_small),
            (conv_in, conv_ref), (gain_in, gain_ref),
        ))
    ]
    for load in little:
        load.start()
    chunk = length // 2
    loads = []
    for b in range(batch):
        for part in range(2):
            loads.append(pltpu.make_async_copy(
                hidden_ref.at[b, pl.ds(part * chunk, chunk)],
                rows.at[b, pl.ds(PAD + part * chunk, chunk)], load_sem.at[2 * b + part],
            ))
    body = width - LANES
    gate_load = pltpu.make_async_copy(
        gate_ref, weights.at[:, pl.ds(body, width)], load_sem.at[2 * batch]
    )
    value_load = pltpu.make_async_copy(
        value_ref.at[:, pl.ds(0, body)], weights.at[:, pl.ds(0, body)],
        load_sem.at[2 * batch + 1],
    )
    tail_load = pltpu.make_async_copy(
        value_ref.at[:, pl.ds(body, LANES)], first_weights.at[:, pl.ds(LANES, LANES)],
        load_sem.at[2 * batch + 2],
    )
    tail_load.start()
    order = [2 * b + part for part in (1, 0) for b in range(batch)]
    for i in order:
        loads[i].start()

    barrier = pltpu.get_barrier_semaphore()
    for device in (after, before, partner):
        pl.semaphore_signal(barrier, inc=1, device_id={"seq": device}, device_id_type=MESH)
    for away in GREETED:
        pl.semaphore_signal(
            barrier, inc=1, device_id={"tp": tp_at(away)}, device_id_type=MESH
        )
    def greet(semaphore):
        for move in ((0, 1), (0, across - 1), (1, 0), (along - 1, 0)):
            pl.semaphore_signal(
                semaphore, inc=1, device_id={"seq": 2 * chip_at(move) + core},
                device_id_type=MESH,
            )

    greet(barrier)

    def greet_round(index):
        if index > 0:
            pl.semaphore_wait(greet_sem.at[index - 1], 4)
        if index < across // 2 + along // 2 - 1:
            greet(greet_sem.at[index])

    for b in range(batch):
        rows[b, 0:HALO, :] = jnp.zeros((HALO, rows.shape[2]), BF16)
        small_pre[b, 0 : LANES - HALO, :] = jnp.zeros((LANES - HALO, LANES), F32)
    heads = step_cols.shape[0]
    small_ref[0:narrow, :] = jnp.zeros((narrow, small_ref.shape[1]), BF16)
    small_ref[2 * narrow :, :] = jnp.zeros((LANES - 2 * narrow, small_ref.shape[1]), BF16)
    bias_ref[...] = jnp.zeros_like(bias_ref)
    rate_ref[...] = jnp.zeros_like(rate_ref)
    bc_square[...] = jnp.zeros_like(bc_square)
    lane = lax.broadcasted_iota(jnp.int32, expand_ref.shape, 1) // HEAD_DIM
    owner = lax.rem(lax.broadcasted_iota(jnp.int32, expand_ref.shape, 0), LANES)
    expand_ref[...] = jnp.where(lane == owner, 1.0, 0.0).astype(BF16)
    for load in little[:2]:
        load.wait()
    small_ref[0:heads, :] = step_cols[...]

    for at in range(0, small_ref.shape[1], LANES):
        first_weights[at : at + LANES, :LANES] = jnp.transpose(small_ref[:, at : at + LANES])

    tail_load.wait()

    def first_tile(part):
        start = part * chunk
        for b in range(batch):
            product = jnp.dot(
                rows[b, PAD + start : PAD + start + chunk, :], first_weights[...],
                preferred_element_type=F32,
            )
            small_pre[b, LANES + start : LANES + start + chunk, :] = product[:, :LANES]
            pre[b, PAD + start : PAD + start + chunk, body:] = (
                product[:, LANES:].astype(BF16).astype(F32)
            )

    for b in range(batch):
        loads[2 * b + 1].wait()
    halo = remote(
        rows.at[:, pl.ds(PAD + length - HALO, HALO)], rows.at[:, pl.ds(PAD - HALO, HALO)],
        halo_sem.at[0], halo_sem.at[1], seq=after,
    )

    small_halo = remote(
        small_pre.at[:, pl.ds(LANES + length - HALO, HALO)],
        small_pre.at[:, pl.ds(LANES - HALO, HALO)],
        halo_sem.at[2], halo_sem.at[3], seq=after,
    )
    tail_halo = remote(
        pre.at[:, pl.ds(PAD + length - HALO, HALO), pl.ds(body, LANES)],
        pre.at[:, pl.ds(PAD - HALO, HALO), pl.ds(body, LANES)],
        halo_sem.at[4], halo_sem.at[5], seq=after,
    )

    def send_halo(copies, now=True):
        @pl.when(jnp.logical_and(place < devices - 1, now))
        def _():
            for copy in copies:
                copy.start()

    def wait_halo(copy):
        @pl.when(place < devices - 1)
        def _():
            copy.wait_send()

        @pl.when(place > 0)
        def _():
            copy.wait_recv()

    def enter(now, copies):
        @pl.when(now)
        def _():
            pl.semaphore_wait(barrier, 7 + len(GREETED))
            send_halo(copies)

    enter(me >= ring // 2, [halo])
    first_tile(1)
    send_halo([small_halo, tail_halo], me >= ring // 2)
    value_load.start()
    for b in range(batch):
        loads[2 * b].wait()
    first_tile(0)
    enter(me == ring // 2 - 1, [small_halo, tail_halo, halo])
    for load in little[2:]:
        load.wait()
    bias_ref[:, 0:heads] = bias_small[...]
    rate_ref[:, 0:heads] = jnp.exp(rate_small[...])
    for part in range(2):
        cut = slice(part * LANES, (part + 1) * LANES)
        bc_square[0:CONV, :] = bc_taps[:, cut]
        bc_conv_ref[cut, :] = jnp.transpose(bc_square[...])
    taps = bc_conv_ref[pl.ds(pl.multiple_of(me * narrow, narrow), narrow), :]

    def bc_conv(x):
        total = taps[:, CONV - 1 : CONV] * x
        for k in range(1, CONV):
            total = total + taps[:, CONV - 1 - k : CONV - k] * pltpu.roll(x, k, 1)
        return silu(total).astype(BF16)

    def transpose_bc(b, piece):
        at = slice(piece * LANES, (piece + 1) * LANES)
        flipped = jnp.transpose(small_pre[b, at, :])[narrow : 2 * narrow, :]
        bc_wide[b, :, at] = flipped.astype(BF16).astype(F32)

    chunks = (
        (far, far_recv, blocks // 2, blocks),
        (near, near_recv, 1, blocks // 2),
        (first_slots, first_recv, 0, 1),
    )
    b_way = jnp.where(jnp.logical_and(me >= 2, me < 2 + ring // 2), 1, -1)

    def convolve(which):
        slots, _, low, high = chunks[which]
        size = (high - low) * BLOCK
        for b in range(batch):
            done = bc_conv(bc_wide[b, :, low * LANES : (high + 1) * LANES])
            slots[me, :, b * size : (b + 1) * size] = done[:, LANES:]

    def ring_copy(which, source, target):
        slots, recv = chunks[which][:2]
        return remote(
            slots.at[source], slots.at[source], ring_send.at[which], recv.at[source], tp=target
        )

    def ring_own(which, steps):
        for away in (steps, ring - steps):
            ring_copy(which, me, tp_at(away)).start()

    def ring_relay(which, way):
        source = tp_at(ring - 2 * way)
        ring_copy(which, source, tp_at(1)).wait_recv()

        last_way = jnp.where(lax.rem(source, 2) == 0, 1, -1)

        @pl.when(way == last_way)
        def _():
            ring_copy(which, source, tp_at(ring + 2 * way)).start()

        ring_copy(which, source, tp_at(ring + way)).start()

    def ring_finish(which, first, way):
        passed = tp_at(ring - 2 * way)
        for source in range(first, first + ring // 2):
            @pl.when(jnp.logical_and(me != source, passed != source))
            def _():
                ring_copy(which, source, tp_at(1)).wait_recv()

    def ring_sent(which):
        wait_bytes(chunks[which][0], ring - 1, ring_send.at[which])

    for b in range(batch):
        for piece in range(1, 1 + length // LANES):
            transpose_bc(b, piece)
    for which in range(2):
        convolve(which)
    enter(me < ring // 2 - 1, [small_halo, tail_halo, halo])
    greet_round(0)
    for which in range(2):
        ring_own(which, 2)

    row = lax.broadcasted_iota(jnp.int32, (BLOCK, BLOCK), 0)
    col = lax.broadcasted_iota(jnp.int32, (BLOCK, BLOCK), 1)
    triangle = jnp.where(row >= col, 1.0, 0.0).astype(BF16)
    triangle = jnp.concatenate([triangle] * 3, axis=1)
    ms, mos, totals = [], [], []
    for b in range(batch):
        offset = jnp.zeros((1, LANES), F32)
        for k in range(blocks):
            step_pre = small_pre[b, LANES + k * BLOCK : LANES + (k + 1) * BLOCK, :] + bias_ref[...]
            steps = jnp.maximum(step_pre, 0.0) + jnp.log1p(jnp.exp(-jnp.abs(step_pre)))
            cumulative = jnp.dot(
                triangle, thirds(-steps * rate_ref[...]), preferred_element_type=F32
            )
            last = cumulative[BLOCK - 1 : BLOCK, :]
            mid = 0.5 * last
            fin[b * blocks + k] = halves(jnp.exp(mid - cumulative) * steps)
            fout[b * blocks + k] = halves(jnp.exp(cumulative - mid))
            ms.append(mid)
            mos.append(mid + offset)
            offset = offset + last
        totals.append(offset)
    table = jnp.exp(jnp.concatenate(ms + mos, axis=0))
    ends[...] = jnp.dot(halves(table), expand_ref[...], preferred_element_type=F32)
    logs[...] = jnp.concatenate(totals + [jnp.zeros((8 - batch, LANES), F32)], axis=0)
    pair_log = remote(logs, pair_logs, log_sem.at[0], log_sem.at[1], seq=partner)
    pair_log.start()

    wait_halo(small_halo)

    @pl.when(place == 0)
    def _():
        for b in range(batch):
            rows[b, 0:PAD, :] = jnp.zeros((PAD, rows.shape[2]), BF16)
            small_pre[b, LANES - HALO : LANES, :] = jnp.zeros((HALO, LANES), F32)
            pre[b, PAD - HALO : PAD, body:] = jnp.zeros((HALO, LANES), F32)

    for b in range(batch):
        transpose_bc(b, 0)
    convolve(2)
    ring_own(2, 2)
    for which in range(3):
        ring_own(which, 1)
    greet_round(1)

    def gate_part(b, product):
        return silu(product.astype(BF16).astype(F32))

    def tile_of(start, size):
        cut = slice(start, start + size)
        for b in range(batch):
            if start >= body:
                product = jnp.dot(
                    rows[b, PAD : PAD + length, :], weights[:, cut], preferred_element_type=F32
                )
                gates[b, :, start - body : start - body + size] = gate_part(b, product)
            else:
                product = jnp.dot(rows[b], weights[:, cut], preferred_element_type=F32)
                pre[b, :, cut] = product.astype(BF16).astype(F32)

    value_tiles = [(at, TILE) for at in range(0, body, TILE)]
    gate_tiles = [
        (at, min(TILE, body + width - at)) for at in range(body, body + width, TILE)
    ]
    gate_load.start()
    value_load.wait()
    wait_halo(halo)
    tile_of(*value_tiles[0])
    wait_halo(tail_halo)


    def values_of(g, low, high):
        b, k = divmod(g, blocks)
        base = PAD + k * BLOCK - HALO
        wide = jnp.dot(fin[g], expand_ref[:, low:high], preferred_element_type=F32)
        for start in range(low, high, LANES):
            cut = slice(start, start + LANES)
            window = pre[b, base : base + HALO + BLOCK, cut]
            x = conv_ref[0:1, cut] * window
            for tap in range(1, CONV):
                x = pltpu.roll(x, 1, 0) + conv_ref[tap : tap + 1, cut] * window
            right[g, STATE:, cut] = (
                silu(x[HALO:]) * wide[:, start - low : start - low + LANES]
            ).astype(BF16)

    for which in range(2):
        ring_relay(which, b_way)
    for g in range(total_blocks):
        values_of(g, 0, TILE)
        values_of(g, body, width)
        if g == total_blocks // 2 - 1:
            ring_relay(2, b_way)
            greet_round(2)
    for start, size in value_tiles[1:]:
        tile_of(start, size)
    for g in range(total_blocks):
        values_of(g, TILE, body)
    greet_round(3)
    pair_log.wait()
    chip_logs[...] = logs[...] + pair_logs[...]
    all_logs[chip] = logs[...] + pair_logs[...]
    for move in moves:
        remote(
            chip_logs, all_logs.at[chip], log_send.at[0], log_recv.at[0],
            seq=2 * chip_at(move) + core,
        ).start()
    for which in range(3):
        ring_finish(which, 0, b_way)

    def bc_block(b, k, first):
        slots, _, low, high = next(c for c in chunks if c[2] <= k < c[3])
        at = (b * (high - low) + k - low) * BLOCK
        return slots[first : first + ring // 2, :, at : at + BLOCK].reshape(STATE, BLOCK)

    for b in range(batch):
        held = jnp.zeros((STATE, width), F32)
        for k in range(blocks):
            g = b * blocks + k
            e = ends[g : g + 1, :]
            ahead = e * held
            right[g, :STATE, :] = ahead.astype(BF16)
            added = jnp.dot(
                bc_block(b, k, 0), right[g, STATE:, :], preferred_element_type=F32
            )
            held = e * (ahead + added)
        local[b] = held.astype(BF16)

    def pair_copy(at, index):
        return remote(
            local.at[:, at], pair.at[:, at], pair_sem.at[index], pair_sem.at[index + 1],
            seq=partner,
        )

    pair_copy(theirs_at, 0).start()
    pair_copy(mine, 2).start()
    for which in range(3):
        ring_relay(which, -b_way)
    own_end = jnp.exp(logs[...])
    pair_end = jnp.exp(pair_logs[...])
    wide_ends = jnp.dot(
        halves(jnp.concatenate([own_end, pair_end], axis=0)), expand_ref[...],
        preferred_element_type=F32,
    )
    pair_copy(theirs_at, 0).wait()
    groups = chips // batch
    for b in range(batch):
        own = local[b, mine, :].astype(F32)
        theirs = pair[b, mine, :].astype(F32)
        first = jnp.where(core == 0, own, theirs)
        second = jnp.where(core == 0, theirs, own)
        later = jnp.where(core == 0, wide_ends[8 + b : 9 + b, :], wide_ends[b : b + 1, :])
        both = (later * first + second).reshape(groups, half // groups, width)
        sent[b * groups : (b + 1) * groups] = both.astype(BF16)
    got[chip] = sent[chip]
    for move in moves:
        peer = chip_at(move)
        remote(
            sent.at[peer], got.at[chip], out_send.at[0], out_recv.at[0], seq=2 * peer + core
        ).start()
    gate_load.wait()
    for start, size in gate_tiles[:2]:
        tile_of(start, size)

    wait_bytes(all_logs, chips - 1, log_send.at[0])
    wait_bytes(all_logs, chips - 1, log_recv.at[0])
    low = chip < chips // batch
    spans = jnp.concatenate(
        [jnp.where(low, all_logs[i, 0:1, :], all_logs[i, 1:2, :]) for i in range(chips)], axis=0
    )
    spans = jnp.dot(halves(jnp.exp(spans)), expand_ref[...], preferred_element_type=F32)
    wait_bytes(got, chips - 1, out_send.at[0])
    wait_bytes(got, chips - 1, out_recv.at[0])
    running = jnp.zeros((half // groups, width), F32)
    for i in range(chips):
        prefix[i] = running.astype(BF16)
        if i + 1 < chips:
            running = spans[i : i + 1, :] * running + got[i].astype(F32)
    owned[chip] = prefix[chip]
    for move in moves:
        peer = chip_at(move)
        remote(
            prefix.at[peer], owned.at[chip], back_send.at[0], back_recv.at[0],
            seq=2 * peer + core,
        ).start()

    for start, size in gate_tiles[2:]:
        tile_of(start, size)
    for which in range(3):
        ring_finish(which, ring // 2, -b_way)
    for g in range(total_blocks):
        b, k = divmod(g, blocks)
        b_flat = bc_block(b, k, 0)
        c_rows = jnp.transpose(bc_block(b, k, ring // 2).astype(F32)).astype(BF16)
        scores = jnp.dot(c_rows, b_flat, preferred_element_type=F32)
        left[g, :, :STATE] = c_rows
        left[g, :, STATE:] = jnp.where(row >= col, scores, 0.0).astype(BF16)
    for g in range(total_blocks):
        b, k = divmod(g, blocks)
        at = slice(k * BLOCK, (k + 1) * BLOCK)
        wide = jnp.dot(fout[g], expand_ref[...], preferred_element_type=F32)
        y = jnp.dot(left[g], right[g], preferred_element_type=F32)
        weighted = wide * gates[b, at, :]
        gated_ref[b, at, :] = y * weighted
        other[b, at, :] = weighted * ends[total_blocks + g : total_blocks + g + 1, :]
    for which in range(3):
        ring_sent(which)
    wait_bytes(owned, chips - 1, back_send.at[0])
    wait_bytes(owned, chips - 1, back_recv.at[0])
    swap = remote(owned, owned_pair, swap_sem.at[0], swap_sem.at[1], seq=partner)
    swap.start()
    pair_copy(mine, 2).wait()
    swap.wait()

    for b in range(batch):
        at = slice(b * groups, (b + 1) * groups)
        own = owned[at].astype(F32).reshape(half, width)
        theirs = owned_pair[at].astype(F32).reshape(half, width)
        span = wide_ends[8 + b : 9 + b, :]
        for c in range(2):
            cut = slice(c * half, (c + 1) * half)
            full = jnp.where(core == c, own, theirs)
            moved = span * full + pair[b, cut, :].astype(F32)
            entering[b, cut, :] = jnp.where(core == 0, full, moved).astype(BF16)

    for b in range(batch):
        for k in range(blocks):
            g = b * blocks + k
            at = slice(k * BLOCK, (k + 1) * BLOCK)
            extra = jnp.dot(left[g, :, :STATE], entering[b], preferred_element_type=F32)
            total = jnp.zeros((BLOCK, LANES), F32)
            for start in range(0, width, LANES):
                cut = slice(start, start + LANES)
                gated = gated_ref[b, at, cut] + other[b, at, cut] * extra[:, cut]
                gated_ref[b, at, cut] = gated * gain_ref[start // LANES : start // LANES + 1, :]
                total = total + gated * gated
            sums[g : g + 1, :] = jnp.sum(jnp.transpose(total), axis=0, keepdims=True)

    for away in turns:
        remote(sums, others.at[me], sum_send.at[0], sum_recv.at[0], tp=tp_at(away)).start()
    others[me] = sums[...]
    wait_bytes(others, ring - 1, sum_send.at[0])
    wait_bytes(others, ring - 1, sum_recv.at[0])
    whole_sq = others[0]
    for k in range(1, ring):
        whole_sq = whole_sq + others[k]
    scale_ref[...] = lax.rsqrt(whole_sq / DI + epsilon)


def norm_kernel(gated_ref, scale_ref, out_ref, done, sems):
    batch, length, width = gated_ref.shape
    copies = []
    for b in range(batch):
        for k in range(length // BLOCK):
            g = b * (length // BLOCK) + k
            at = slice(k * BLOCK, (k + 1) * BLOCK)
            column = jnp.transpose(jnp.broadcast_to(scale_ref[g : g + 1, :], (BLOCK, LANES)))
            for start in range(0, width, LANES):
                cut = slice(start, start + LANES)
                done[b, at, cut] = (gated_ref[b, at, cut] * column).astype(BF16)
            copies.append(pltpu.make_async_copy(
                done.at[b, pl.ds(k * BLOCK, BLOCK)], out_ref.at[b, pl.ds(k * BLOCK, BLOCK)],
                sems.at[g],
            ))
            copies[-1].start()
    for copy in copies:
        copy.wait()


def per_device(
    hidden_in, gate_proj, value_proj, bc_proj, step_proj,
    value_conv, bc_conv, step_bias, log_rate, norm_gain,
):
    batch, length, model_width = hidden_in.shape
    heads = step_proj.shape[1]
    width = value_proj.shape[1]
    narrow = bc_proj.shape[1]
    blocks = length // BLOCK
    tp = lax.axis_size("tp")
    chips = lax.axis_size("seq") // 2
    total_blocks = batch * blocks
    half = STATE // 2
    groups = chips // batch

    hbm = pl.BlockSpec(memory_space=pltpu.HBM)
    vmem = pl.BlockSpec(memory_space=pltpu.VMEM)
    dma = pltpu.SemaphoreType.DMA
    gated, scale = pl.pallas_call(
        mixer_kernel,
        out_shape=(
            jax.ShapeDtypeStruct((batch, length, width), F32),
            jax.ShapeDtypeStruct((total_blocks, LANES), F32),
        ),
        in_specs=[hbm] * 10,
        out_specs=[vmem, vmem],
        scratch_shapes=[
            pltpu.VMEM((LANES, model_width), BF16),
            pltpu.VMEM((model_width, 2 * LANES), BF16),
            pltpu.VMEM((heads, model_width), BF16),
            pltpu.VMEM((CONV, width), F32),
            pltpu.VMEM((CONV, 2 * STATE), F32),
            pltpu.VMEM((LANES, LANES), F32),
            pltpu.VMEM((2 * STATE, LANES), F32),
            pltpu.VMEM((1, heads), F32),
            pltpu.VMEM((1, heads), F32),
            pltpu.VMEM((1, LANES), F32),
            pltpu.VMEM((1, LANES), F32),
            pltpu.VMEM((width // LANES, LANES), F32),
            pltpu.VMEM((2 * LANES, width), BF16),
            pltpu.VMEM((batch, PAD + length, model_width), BF16),
            pltpu.VMEM((model_width, 2 * width - LANES), BF16),
            pltpu.VMEM((batch, LANES + length, LANES), F32),
            pltpu.VMEM((batch, narrow, LANES + length), F32),
            pltpu.VMEM((total_blocks, BLOCK, 2 * LANES), BF16),
            pltpu.VMEM((total_blocks, BLOCK, 2 * LANES), BF16),
            pltpu.VMEM((2 * total_blocks, width), F32),
            pltpu.VMEM((8, LANES), F32),
            pltpu.VMEM((8, LANES), F32),
            pltpu.VMEM((8, LANES), F32),
            pltpu.VMEM((chips, 8, LANES), F32),
            pltpu.VMEM((tp, narrow, batch * (blocks - blocks // 2) * BLOCK), BF16),
            pltpu.VMEM((tp, narrow, batch * (blocks // 2 - 1) * BLOCK), BF16),
            pltpu.VMEM((tp, narrow, batch * BLOCK), BF16),
            pltpu.VMEM((batch, PAD + length, width), F32),
            pltpu.VMEM((batch, length, width), F32),
            pltpu.VMEM((total_blocks, BLOCK, STATE + BLOCK), BF16),
            pltpu.VMEM((total_blocks, STATE + BLOCK, width), BF16),
            pltpu.VMEM((batch, length, width), F32),
            pltpu.VMEM((batch, STATE, width), BF16),
            pltpu.VMEM((batch, STATE, width), BF16),
            pltpu.VMEM((chips, half // groups, width), BF16),
            pltpu.VMEM((chips, half // groups, width), BF16),
            pltpu.VMEM((chips, half // groups, width), BF16),
            pltpu.VMEM((chips, half // groups, width), BF16),
            pltpu.VMEM((chips, half // groups, width), BF16),
            pltpu.VMEM((batch, STATE, width), BF16),
            pltpu.VMEM((total_blocks, LANES), F32),
            pltpu.VMEM((tp, total_blocks, LANES), F32),
            pltpu.SemaphoreType.REGULAR((SIDE // 2 + chips // SIDE // 2 - 1,)),
            dma((2 * batch + 3,)),
            dma((7,)),
            dma((6,)),
            dma((2,)),
            dma((1,)),
            dma((1,)),
            dma((3,)),
            dma((tp,)),
            dma((tp,)),
            dma((tp,)),
            dma((4,)),
            dma((1,)),
            dma((1,)),
            dma((1,)),
            dma((1,)),
            dma((2,)),
            dma((1,)),
            dma((1,)),
        ],
        compiler_params=pltpu.CompilerParams(
            vmem_limit_bytes=48 << 20, collective_id=0, has_side_effects=True
        ),
        name="mixer",
    )(*(pltpu.with_memory_space_constraint(x, pltpu.HBM) for x in (
        hidden_in, value_proj, gate_proj, bc_proj.T, step_proj.T, value_conv, bc_conv,
        step_bias.reshape(1, heads), log_rate.reshape(1, heads),
        norm_gain.reshape(width // LANES, LANES),
    )))

    return pl.pallas_call(
        norm_kernel,
        out_shape=jax.ShapeDtypeStruct((batch, length, width), BF16),
        in_specs=[vmem, vmem],
        out_specs=hbm,
        scratch_shapes=[pltpu.VMEM((batch, length, width), BF16), dma((total_blocks,))],
        compiler_params=pltpu.CompilerParams(vmem_limit_bytes=8 << 20),
        name="norm",
    )(gated, scale)


def solution(mesh):
    return jax.shard_map(
        per_device,
        mesh=mesh,
        in_specs=(
            P(None, "seq", None),
            P(None, "tp"),
            P(None, "tp"),
            P(None, "tp"),
            P(None, "tp"),
            P(None, "tp"),
            P(),
            P("tp"),
            P("tp"),
            P("tp"),
        ),
        out_specs=P(None, "seq", "tp"),
        check_vma=False,
    )
```
